128 devices in a mesh: wide: 16 (over y, z), narrow: 8 (over x, core).
Axes of the slice: x: 4, y: 4, z: 4, core: 2. Of those that a mesh axis runs over, the one named last changes fastest.
Arguments:
- fine_in: bfloat16 [32, 64, 128, 80], P(None, 'narrow', 'wide'), may hold values from -6 to 6
- voxel_mask: int32 [64, 128, 80], P('narrow', 'wide'), may hold values from 0 to 1, as said below
- timestep: int32 [1], replicated, may hold values from 0 to 999
- w_enc: bfloat16 [27, 32, 32], replicated, may hold values from -0.21875 to 0.21875
- b_enc: float32 [32], replicated, may hold values from -3 to 3
- w_down: bfloat16 [128, 256], replicated, may hold values from -0.375 to 0.375
- w_time: bfloat16 [128, 256], replicated, may hold values from -0.5 to 0.5
- w_coarse: bfloat16 [27, 128, 128], replicated, may hold values from -0.109375 to 0.109375
- b_coarse: float32 [128], replicated, may hold values from -3 to 3
- w_up: bfloat16 [32, 128], replicated, may hold values from -0.5 to 0.5
- w_dec: bfloat16 [27, 32, 64], replicated, may hold values from -0.15625 to 0.15625
- b_dec: float32 [32], replicated, may hold values from -3 to 3
Outputs:
- denoised: bfloat16 [32, 64, 128, 80], P(None, 'narrow', 'wide')
The draws below stay inside these ranges and needn't reach their ends.
Inputs may be any that keep to these rules, and one draw needn't show every extreme that they name: `voxel_mask`: each device's tile of 8 x 8 x 80 voxels consists of aligned 8 x 8 x 8 blocks; a block is active when it holds a 1. Two tiles with the same narrow index whose wide indices differ by 8 hold at most 10 active blocks together, and some such pair holds exactly 10.
All inputs are finite; a program needn't handle non-finite values.
Results may differ from the reference program's by a relative error of at most 0.0044.
Values may be sent and summed in bfloat16 or wider, within the bound.
No kernel may reach another device: no remote copies, remote signals or barrier semaphores. Data moves between devices by JAX's collectives and lax.ppermute only.
A program may use at most 64 MiB of HBM per device.

```python
import math
import jax
import jax.numpy as jnp
from jax import lax

C = 32
CC = 128
TE = 128
TX = 8
TY = 8
Z = 80
NX = 64
NY = 128


def draw_voxel_mask(key, part):
    tiles_x = NX // TX
    tiles_y = NY // TY
    half_y = tiles_y // 2
    blocks_x = TX // 8
    blocks_y = TY // 8
    blocks_z = Z // 8
    per_tile = blocks_x * blocks_y * blocks_z
    keys = jax.random.split(jax.random.fold_in(key, 17), 7)
    heavy = jax.random.randint(keys[0], (tiles_x, half_y), 3 * per_tile // 4, per_tile + 1)
    chosen = jax.random.randint(keys[1], (), 0, tiles_x * half_y)
    places = jnp.arange(tiles_x * half_y, dtype=jnp.int32).reshape(tiles_x, half_y)
    heavy = jnp.where(places == chosen, per_tile, heavy)
    light = jax.random.randint(keys[2], (tiles_x, half_y), 0, per_tile - heavy + 1)
    sides = jax.random.randint(keys[3], (tiles_x, half_y), 0, 2)
    lower = jnp.where(sides == 0, heavy, light)
    upper = jnp.where(sides == 0, light, heavy)
    counts = jnp.concatenate([lower, upper], axis=1)
    scores = jax.random.randint(keys[4], (tiles_x, tiles_y, per_tile), 0, 1 << 20) * per_tile + jnp.arange(per_tile, dtype=jnp.int32)
    ranks = jnp.argsort(jnp.argsort(scores, axis=-1), axis=-1)
    active = (ranks < counts[..., None]).astype(jnp.int32)
    voxels = jax.random.randint(keys[5], (tiles_x, tiles_y, per_tile, 512), 0, 2)
    forced = jax.random.randint(keys[6], (tiles_x, tiles_y, per_tile), 0, 512)
    voxels = jnp.where(jnp.arange(512, dtype=jnp.int32) == forced[..., None], 1, voxels)
    filled = active[..., None] * voxels
    filled = filled.reshape(tiles_x, tiles_y, blocks_x, blocks_y, blocks_z, 8, 8, 8)
    filled = jnp.transpose(filled, (0, 2, 5, 1, 3, 6, 4, 7))
    return filled.reshape(NX, NY, Z).astype(jnp.int32)


def level_of(rng, dims, pieces, smallest, high):
    def one(axis_at, parts):
        steps = jax.random.uniform(jax.random.fold_in(jax.random.fold_in(rng, 6), axis_at), (parts,), jnp.float32, smallest / len(pieces), high / len(pieces))
        return jnp.repeat(jnp.exp(steps), dims[axis_at] // parts).reshape((-1,) + (1,) * (len(dims) - axis_at - 1))

    gain = one(*pieces[0])
    for cut in pieces[1:]:
        gain = gain * one(*cut)
    return gain


def bell_draw(own_key, shape, width, reach, pieces=(), kind=jnp.bfloat16):
    array = jax.random.normal(own_key, shape, jnp.float32) * width
    if len(pieces) > 0:
        array = level_of(own_key, shape, pieces, -0.22, 0.18) * array
    return jnp.clip(array, min=-reach, max=reach).astype(kind)


def setup_inputs(seed: int = 0) -> dict:
    seeds = jax.random.split(jax.random.key(seed), 13)
    return {
        "fine_in": bell_draw(seeds[0], (C, NX, NY, Z), 1.0, 6.0, ((1, 8), (2, 16))),
        "voxel_mask": draw_voxel_mask(jax.random.fold_in(seeds[12], 71), 0),
        "timestep": jax.random.randint(seeds[2], (1,), 0, 1000).astype(jnp.int32),
        "w_enc": bell_draw(seeds[3], (27, C, C), (27 * C) ** -0.5, 0.21875),
        "b_enc": bell_draw(seeds[4], (C,), 0.5, 3.0, (), jnp.float32),
        "w_down": bell_draw(seeds[5], (CC, 8 * C), (8 * C) ** -0.5, 0.375),
        "w_time": bell_draw(seeds[6], (TE, 2 * CC), TE ** -0.5, 0.5),
        "w_coarse": bell_draw(seeds[7], (27, CC, CC), (27 * CC) ** -0.5, 0.109375),
        "b_coarse": bell_draw(seeds[8], (CC,), 0.5, 3.0, (), jnp.float32),
        "w_up": bell_draw(seeds[9], (C, CC), CC ** -0.5, 0.5),
        "w_dec": bell_draw(seeds[10], (27, C, 2 * C), (54 * C) ** -0.5, 0.15625),
        "b_dec": bell_draw(seeds[11], (C,), 0.5, 3.0, (), jnp.float32),
    }


LAYOUT = ("NCDHW", "OIDHW", "NCDHW")


def cube_weight(weight):
    out_ch = weight.shape[1]
    in_ch = weight.shape[2]
    return jnp.transpose(weight.reshape(3, 3, 3, out_ch, in_ch), (3, 4, 0, 1, 2))


def conv_scene(field_in, weight):
    size_x = field_in.shape[1]
    size_y = field_in.shape[2]
    size_z = field_in.shape[3]
    kernel = cube_weight(weight).astype(jnp.float32)
    padded = jnp.pad(field_in, ((0, 0), (1, 1), (1, 1), (1, 1)))

    def slab_conv(offset):
        window = lax.dynamic_slice_in_dim(padded, offset, 10, 1).astype(jnp.float32)
        result = lax.conv_general_dilated(window[None], kernel, (1, 1, 1), "VALID", dimension_numbers=LAYOUT, precision=lax.Precision.HIGHEST, preferred_element_type=jnp.float32)
        return result[0]

    offsets = jnp.arange(size_x // 8, dtype=jnp.int32) * 8
    stacked = lax.map(slab_conv, offsets)
    return jnp.moveaxis(stacked, 0, 1).reshape(weight.shape[1], size_x, size_y, size_z)


def time_features(timestep, embed_width):
    halves = embed_width // 2
    freqs = jnp.exp(-math.log(10000.0) * jnp.arange(halves, dtype=jnp.float32) / halves)
    angles = timestep[0].astype(jnp.float32) * freqs
    return jnp.concatenate([jnp.sin(angles), jnp.cos(angles)]).astype(jnp.bfloat16)


def pool_children(field_in):
    chans = field_in.shape[0]
    half_x = field_in.shape[1] // 2
    half_y = field_in.shape[2] // 2
    half_z = field_in.shape[3] // 2
    grouped = field_in.reshape(chans, half_x, 2, half_y, 2, half_z, 2)
    return jnp.transpose(grouped, (2, 4, 6, 0, 1, 3, 5)).reshape(8 * chans, half_x, half_y, half_z)


def coarse_mask(mask_in):
    half_x = mask_in.shape[0] // 2
    half_y = mask_in.shape[1] // 2
    half_z = mask_in.shape[2] // 2
    return jnp.max(mask_in.reshape(half_x, 2, half_y, 2, half_z, 2), axis=(1, 3, 5)) > 0


def upsample(field_in):
    return jnp.repeat(jnp.repeat(jnp.repeat(field_in, 2, axis=1), 2, axis=2), 2, axis=3)


def reference(fine_in, voxel_mask, timestep, w_enc, b_enc, w_down, w_time, w_coarse, b_coarse, w_up, w_dec, b_dec):
    active = voxel_mask[None] > 0
    masked = jnp.where(active, fine_in, jnp.zeros_like(fine_in))
    encoded = jnp.where(active, jax.nn.silu(conv_scene(masked, w_enc) + b_enc[:, None, None, None]), 0.0).astype(jnp.bfloat16)
    pooled = pool_children(encoded)
    coarse_on = coarse_mask(voxel_mask)[None]
    embedded = time_features(timestep, w_time.shape[0])
    film = jnp.dot(embedded[None], w_time, preferred_element_type=jnp.float32)[0]
    chans = w_down.shape[0]
    gains = 1.0 + film[:chans]
    shifts = film[chans:]
    lifted = jnp.dot(w_down, pooled.reshape(pooled.shape[0], -1), preferred_element_type=jnp.float32)
    lifted = lifted.reshape((chans,) + pooled.shape[1:])
    coarse_in = jnp.where(coarse_on, jax.nn.silu(lifted * gains[:, None, None, None] + shifts[:, None, None, None]), 0.0).astype(jnp.bfloat16)
    coarse_act = jnp.where(coarse_on, jax.nn.silu(conv_scene(coarse_in, w_coarse) + b_coarse[:, None, None, None]), 0.0).astype(jnp.bfloat16)
    lifted_up = jnp.dot(w_up, coarse_act.reshape(chans, -1), preferred_element_type=jnp.float32)
    lifted_up = lifted_up.reshape((w_up.shape[0],) + coarse_act.shape[1:]).astype(jnp.bfloat16)
    joined = jnp.concatenate([encoded, upsample(lifted_up)], axis=0)
    decoded = conv_scene(joined, w_dec) + b_dec[:, None, None, None]
    return jnp.where(active, decoded, 0.0).astype(jnp.bfloat16)
```

```python
import math

import jax
import jax.numpy as jnp
from jax import lax
from jax.experimental import pallas as pl
from jax.experimental.pallas import tpu as pltpu
from jax.sharding import PartitionSpec as P

F32 = jnp.float32
BF16 = jnp.bfloat16
LANES = 128
ZC = 40
Z = 80
CH = 32
BITS = (0, 1)


def nn(a, b):
    return lax.dot_general(a, b, (((1,), (0,)), ((), ())), preferred_element_type=F32)


def nt(a, b):
    return lax.dot_general(a, b, (((1,), (1,)), ((), ())), preferred_element_type=F32)


def iota(shape, dim):
    return lax.broadcasted_iota(jnp.int32, shape, dim)


def silu(v):
    return v / (1.0 + jnp.exp(-v))


def rounded(v):
    return v.astype(BF16).astype(F32)


def pack_kernel(x_ref, m_ref, a_ref, k_ref):
    row = iota((Z, Z), 0)
    sel = (jnp.where(row < ZC, 2 * row, 2 * row - (Z - 1)) == iota((Z, Z), 1)).astype(F32).astype(BF16)
    src = iota((512, LANES), 0)
    y = src & 7
    goal = ((y >> 1) << 7) + ((src >> 8) << 6) + ((y & 1) << 5) + ((src >> 3) & 31) - iota((512, LANES), 1)
    perm = [(goal == LANES * i).astype(F32).astype(BF16) for i in range(4)]
    for cx in range(4):
        halves = []
        for a in BITS:
            x = 2 * cx + a
            tile = x_ref[:, x].astype(F32)
            tile = jnp.where(m_ref[x][None] > 0, tile, 0.0)
            halves.append(nt(sel, tile.reshape(8 * CH, Z).astype(BF16)).astype(BF16))
        both = jnp.concatenate(halves, axis=1)
        for cy in range(4):
            a_ref[cx, cy] = nn(both, perm[cy]).astype(BF16)
    mask = (m_ref[...] > 0).astype(F32).reshape(64, Z).astype(BF16)
    cols = nt(sel, mask)
    k_ref[...] = jnp.concatenate([cols[:ZC], cols[ZC:]], axis=1).astype(BF16)


def tap_of(out_bit, in_bit, far):
    if far:
        return 2 * (1 - in_bit) if out_bit != in_bit else None
    return in_bit - out_bit + 1


def placed(w_ref, taps, group):
    total = jnp.zeros((CH, LANES), F32)
    for g, tap in enumerate(taps):
        if tap is not None:
            total = jnp.where(group == g, w_ref[tap].astype(F32), total)
    return total


def block(w_ref, group, far_x, far_y, a_in, b_in, cz_in, shifted, cz_out):
    if shifted:
        tz = None
        if cz_out == 0 and cz_in == 1:
            tz = 0
        if cz_out == 1 and cz_in == 0:
            tz = 2
    else:
        tz = cz_in - cz_out + 1
    taps = []
    for a_out in BITS:
        for b_out in BITS:
            tx = tap_of(a_out, a_in, far_x)
            ty = tap_of(b_out, b_in, far_y)
            taps.append(None if tx is None or ty is None or tz is None else 9 * tx + 3 * ty + tz)
    return placed(w_ref, taps, group)


KINDS = ((0, 0), (1, 0), (0, 1), (1, 1))


def weights_kernel(we_ref, wd_ref, wl_ref, oe_ref, od_ref):
    group = iota((CH, LANES), 1) >> 5
    for w_ref, o_ref in ((we_ref, oe_ref), (wd_ref, od_ref)):
        for t, (fx, fy) in enumerate(KINDS):
            for cz in BITS:
                for a in BITS:
                    for b in BITS:
                        base = 256 * t + 128 * cz + 64 * a + 32 * b
                        for s in BITS:
                            for co in BITS:
                                v = block(w_ref, group, fx, fy, a, b, cz, s, co)
                                o_ref[base : base + CH, 256 * s + 128 * co : 256 * s + 128 * co + LANES] = v.astype(BF16)
    for t, (fx, fy) in enumerate(KINDS):
        for a in BITS:
            for b in BITS:
                base = 1024 + 128 * t + 64 * a + 32 * b
                for s in BITS:
                    for co in BITS:
                        v = block(wl_ref, group, fx, fy, a, b, 0, s, co) + block(wl_ref, group, fx, fy, a, b, 1, s, co)
                        od_ref[base : base + CH, 256 * s + 128 * co : 256 * s + 128 * co + LANES] = v.astype(BF16)


def moved(t, amount, edge):
    rows = t.shape[0]
    return jnp.where(edge, 0.0, pltpu.roll(t, amount % rows, 0))


def depth_of(rows):
    return iota((rows, LANES), 0) % ZC


def main_kernel(
    own_ref, left_ref, right_ref, kl_ref, ko_ref, kr_ref, m_ref, we_ref, be_ref, wdn_ref, gain_ref, shift_ref,
    wc_ref, bc_ref, wu_ref, wd_ref, bd_ref, out_ref, a_ref, v_ref, e_ref, c_ref, u_ref, l_ref,
):
    lane = iota((ZC, LANES), 1)
    low_a = lane < 64
    low_b = (lane & 32) == 0
    for xi in range(10):
        ref, at = (left_ref, xi) if xi < 3 else ((own_ref, xi - 3) if xi < 7 else (right_ref, xi - 7))
        for yi in range(10):
            v = ref[at, yi].astype(F32)
            for cz in BITS:
                a_ref[xi, cz, yi * ZC : (yi + 1) * ZC] = v[cz * ZC : (cz + 1) * ZC]
    la8 = iota((320, LANES), 1) < 64
    lb8 = (iota((320, LANES), 1) & 32) == 0
    for xi in range(10):
        for cz in BITS:
            v_ref[xi, cz] = jnp.where(lb8, a_ref[xi, cz, 80:400], a_ref[xi, cz, 0:320])
    z8 = depth_of(320)
    first8, last8 = z8 == 0, z8 == ZC - 1
    where_lane = iota((8, LANES), 1)
    blocks = {}
    for bx, ref in enumerate((kl_ref, ko_ref, kr_ref)):
        for by in range(3):
            k = ref[by * ZC : (by + 1) * ZC].astype(F32)
            m = jnp.maximum(k, pltpu.roll(k, LANES - 1, 1))
            m = jnp.maximum(m, pltpu.roll(m, LANES - 8, 1))
            m = jnp.maximum(m, pltpu.roll(m, LANES - 64, 1))
            blocks[bx, by] = (k, m)

    def spread(k, index):
        parts = []
        for i in range(5):
            parts.append(jnp.take_along_axis(k[8 * i : 8 * i + 8], index, axis=1, mode="promise_in_bounds"))
        return jnp.concatenate(parts, axis=0)

    def local(i):
        c = i - 3
        return (0, c + 4) if c < 0 else ((1, c) if c < 4 else (2, c - 4))

    on_of = {}
    for xi in range(1, 9):
        for cz in BITS:
            l_ref[:, 128 * cz : 128 * cz + 128] = a_ref[xi, cz, 40:360].astype(BF16)
            l_ref[:, 256 + 128 * cz : 384 + 128 * cz] = jnp.where(
                la8, a_ref[xi + 1, cz, 40:360], a_ref[xi - 1, cz, 40:360]
            ).astype(BF16)
            l_ref[:, 512 + 128 * cz : 640 + 128 * cz] = v_ref[xi, cz].astype(BF16)
            l_ref[:, 768 + 128 * cz : 896 + 128 * cz] = jnp.where(la8, v_ref[xi + 1, cz], v_ref[xi - 1, cz]).astype(BF16)
        o = nn(l_ref[:, 0:1024], we_ref[...])
        bx, lx = local(xi)
        expanded = [[], []]
        on = []
        for yi in range(1, 9):
            by, ly = local(yi)
            k, m = blocks[bx, by]
            for cz in BITS:
                index = 64 * cz + (2 * lx + (where_lane >> 6)) * 8 + 2 * ly + ((where_lane >> 5) & 1)
                expanded[cz].append(spread(k, index))
            on.append(spread(m, where_lane * 0 + (16 * lx + 2 * ly)))
        on = jnp.concatenate(on, axis=0) > 0.5
        pre = (
            o[:, 0:128] + moved(o[:, 256:384], 1, first8) + be_ref[...],
            o[:, 128:256] + moved(o[:, 384:512], -1, last8) + be_ref[...],
        )
        enc = []
        for cz in BITS:
            active = jnp.concatenate(expanded[cz], axis=0) > 0.5
            e = jnp.where(active, silu(pre[cz]), 0.0)
            enc.append(e.astype(BF16))
            if 2 <= xi <= 7:
                e_ref[xi - 2, cz] = rounded(e)[40:280]
        lifted = nn(jnp.concatenate(enc, axis=1), wdn_ref[...])
        c = jnp.where(on, silu(lifted * gain_ref[...] + shift_ref[...]), 0.0)
        c_ref[xi - 1] = rounded(c)
        on_of[xi] = on[40:280]
    z6 = depth_of(240)
    first6, last6 = z6 == 0, z6 == ZC - 1
    pairs = [(dx, dy) for dx in range(3) for dy in range(3)]
    for xo in range(6):
        p = None
        for i in range(0, 9, 2):
            some = pairs[i : i + 2]
            lhs = [c_ref[xo + dx, dy * ZC : dy * ZC + 240].astype(BF16) for dx, dy in some]
            rhs = [wc_ref[9 * dx + 3 * dy : 9 * dx + 3 * dy + 3].reshape(384, 128) for dx, dy in some]
            lhs = jnp.concatenate(lhs, axis=1) if len(lhs) > 1 else lhs[0]
            rhs = jnp.concatenate(rhs, axis=1) if len(rhs) > 1 else rhs[0]
            q = nt(lhs, rhs)
            p = q if p is None else p + q
        s = p[:, 128:256] + moved(p[:, 0:128], 1, first6) + moved(p[:, 256:384], -1, last6) + bc_ref[...]
        act = jnp.where(on_of[xo + 2], silu(s), 0.0).astype(BF16)
        u_ref[xo] = rounded(nn(act, wu_ref[...]))
    z4 = depth_of(160)
    first4, last4 = z4 == 0, z4 == ZC - 1
    la4 = iota((160, LANES), 1) < 64
    lb4 = (iota((160, LANES), 1) & 32) == 0

    def spans(load):
        mid = [load(i)[40:200] for i in range(3)]
        side = [jnp.where(lb4, load(i)[80:240], load(i)[0:160]) for i in range(3)]
        return mid[1], jnp.where(la4, mid[2], mid[0]), side[1], jnp.where(la4, side[2], side[0])

    row = iota((LANES, Z), 0)
    back = (jnp.where(row < ZC, 2 * row, 2 * row - (Z - 1)) == iota((LANES, Z), 1)).astype(F32).astype(BF16)
    src = iota((512, LANES), 0)
    goal = (((src >> 6) & 1) << 8) + ((src & 31) << 3) + ((src >> 7) << 1) + ((src >> 5) & 1) - iota((512, LANES), 1)
    perm = jnp.concatenate([(goal == LANES * i).astype(F32).astype(BF16) for i in range(4)], axis=1)
    for xo in range(4):
        for cz in BITS:
            for t, v in enumerate(spans(lambda i: e_ref[xo + i, cz])):
                l_ref[0:160, 256 * t + 128 * cz : 256 * t + 128 * cz + 128] = v.astype(BF16)
        for t, v in enumerate(spans(lambda i: u_ref[xo + i])):
            l_ref[0:160, 1024 + 128 * t : 1152 + 128 * t] = v.astype(BF16)
        o = nn(l_ref[0:160, :], wd_ref[...])
        d0 = (o[:, 0:128] + moved(o[:, 256:384], 1, first4) + bd_ref[...])
        d1 = (o[:, 128:256] + moved(o[:, 384:512], -1, last4) + bd_ref[...])
        d = [jnp.concatenate([v[ZC * y : ZC * y + ZC] for y in range(4)], axis=1) for v in (d0, d1)]
        d = jnp.concatenate(d + [jnp.zeros((LANES - Z, 512), F32)], axis=0).astype(BF16)
        d = nn(d, perm)
        for a in BITS:
            t = jnp.transpose(d[:, 256 * a : 256 * a + 256]).astype(BF16)
            t = nn(t, back).reshape(CH, 8, Z)
            x = 2 * xo + a
            out_ref[:, x] = jnp.where(m_ref[x][None] > 0, t, 0.0).astype(BF16)


def vmem(n):
    return [pl.BlockSpec(memory_space=pltpu.VMEM)] * n


def shifted(value, axis, step):
    peers = lax.axis_size(axis)
    return lax.ppermute(value, axis, [(i, i + step) for i in range(peers) if 0 <= i + step < peers])


def time_features(timestep, embed_width):
    halves = embed_width // 2
    freqs = jnp.exp(-math.log(10000.0) * jnp.arange(halves, dtype=F32) / halves)
    angles = timestep[0].astype(F32) * freqs
    return jnp.concatenate([jnp.sin(angles), jnp.cos(angles)]).astype(BF16)


def tiled_taps(w):
    return jnp.tile(jnp.transpose(w, (0, 2, 1)), (1, 1, 4))


def on_device(
    fine_in, voxel_mask, timestep, w_enc, b_enc, w_down, w_time, w_coarse, b_coarse, w_up, w_dec, b_dec
):
    big = pltpu.CompilerParams(vmem_limit_bytes=60 * 1024 * 1024)
    tile, mask = pl.pallas_call(
        pack_kernel,
        out_shape=[jax.ShapeDtypeStruct((4, 4, Z, LANES), BF16), jax.ShapeDtypeStruct((ZC, LANES), BF16)],
        in_specs=vmem(2),
        out_specs=vmem(2),
        compiler_params=big,
        cost_estimate=pl.CostEstimate(flops=10**9, bytes_accessed=10**6, transcendentals=0),
        name="pack",
    )(fine_in, voxel_mask)

    def joined(part, masks):
        return jnp.concatenate([part.reshape(-1, LANES), masks], axis=0)

    low = shifted(joined(tile[:, 1:4], mask), "wide", 1)
    high = shifted(joined(tile[:, 0:3], mask), "wide", -1)
    rows = 12 * Z
    wide = jnp.concatenate(
        [low[:rows].reshape(4, 3, Z, LANES), tile, high[:rows].reshape(4, 3, Z, LANES)], axis=1
    )
    masks = jnp.concatenate([low[rows:], mask, high[rows:]], axis=0)
    left = shifted(joined(wide[1:4], masks), "narrow", 1)
    right = shifted(joined(wide[0:3], masks), "narrow", -1)
    rows = 30 * Z

    embedded = time_features(timestep, w_time.shape[0])
    film = jnp.dot(embedded[None], w_time, preferred_element_type=F32)
    chans = w_down.shape[0]
    gains = 1.0 + film[:, :chans]
    shifts = film[:, chans:]

    enc_w, dec_w = pl.pallas_call(
        weights_kernel,
        out_shape=[jax.ShapeDtypeStruct((1024, 512), BF16), jax.ShapeDtypeStruct((1536, 512), BF16)],
        in_specs=vmem(3),
        out_specs=vmem(2),
        compiler_params=big,
        cost_estimate=pl.CostEstimate(flops=2 * 10**9, bytes_accessed=10**6, transcendentals=0),
        name="weights",
    )(tiled_taps(w_enc), tiled_taps(w_dec[:, :, :CH]), tiled_taps(w_dec[:, :, CH:]))
    down_w = jnp.transpose(w_down.reshape(chans, 2, 2, 2, CH), (3, 1, 2, 4, 0)).reshape(8 * CH, chans)
    up_w = jnp.tile(jnp.transpose(w_up), (1, 4))

    def four(bias):
        return jnp.tile(bias, 4)[None]

    return pl.pallas_call(
        main_kernel,
        out_shape=jax.ShapeDtypeStruct(fine_in.shape, BF16),
        in_specs=vmem(17),
        out_specs=vmem(1)[0],
        scratch_shapes=[
            pltpu.VMEM((10, 2, 400, LANES), F32),
            pltpu.VMEM((10, 2, 320, LANES), F32),
            pltpu.VMEM((6, 2, 240, LANES), F32),
            pltpu.VMEM((8, 320, LANES), F32),
            pltpu.VMEM((6, 240, LANES), F32),
            pltpu.VMEM((320, 1536), BF16),
        ],
        compiler_params=big,
        cost_estimate=pl.CostEstimate(flops=8 * 10**9, bytes_accessed=10**6, transcendentals=0),
        name="network",
    )(
        wide,
        left[:rows].reshape(3, 10, Z, LANES),
        right[:rows].reshape(3, 10, Z, LANES),
        left[rows:],
        masks,
        right[rows:],
        voxel_mask,
        enc_w,
        four(b_enc),
        down_w,
        gains,
        shifts,
        w_coarse,
        b_coarse[None],
        up_w,
        dec_w,
        four(b_dec),
    )


def solution(mesh):
    field = P(None, "narrow", "wide", None)
    return jax.shard_map(
        on_device,
        mesh=mesh,
        in_specs=(field, P("narrow", "wide", None)) + (P(),) * 10,
        out_specs=field,
        check_vma=False,
    )
```

```python
import math

import jax
import jax.numpy as jnp
from jax import lax
from jax.experimental import pallas as pl
from jax.experimental.pallas import tpu as pltpu
from jax.sharding import PartitionSpec as P

F32 = jnp.float32
BF16 = jnp.bfloat16
LANES = 128
ZC = 40
Z = 80
CH = 32
BITS = (0, 1)


def nn(a, b):
    return lax.dot_general(a, b, (((1,), (0,)), ((), ())), preferred_element_type=F32)


def nt(a, b):
    return lax.dot_general(a, b, (((1,), (1,)), ((), ())), preferred_element_type=F32)


def iota(shape, dim):
    return lax.broadcasted_iota(jnp.int32, shape, dim)


def silu(v):
    return v / (1.0 + jnp.exp(-v))


def rounded(v):
    return v.astype(BF16).astype(F32)


UNIT = Z
OWN = 16 * UNIT
SIDE = 12 * UNIT
EDGE = 30 * UNIT


def unpick(rows, cols):
    row = iota((rows, cols), 0)
    return (jnp.where(row < ZC, 2 * row, 2 * row - (Z - 1)) == iota((rows, cols), 1)).astype(F32).astype(BF16)


def pack_kernel(x_ref, m_ref, own_ref, up_ref, dn_ref):
    sel = unpick(Z, Z)
    src = iota((512, LANES), 0)
    y = src & 7
    goal = ((y >> 1) << 7) + ((src >> 8) << 6) + ((y & 1) << 5) + ((src >> 3) & 31) - iota((512, LANES), 1)
    perm = [(goal == LANES * i).astype(F32).astype(BF16) for i in range(4)]
    for cx in range(4):
        halves = []
        for a in BITS:
            x = 2 * cx + a
            tile = x_ref[:, x].astype(F32)
            tile = jnp.where(m_ref[x][None] > 0, tile, 0.0)
            halves.append(nt(sel, tile.reshape(8 * CH, Z).astype(BF16)).astype(BF16))
        both = jnp.concatenate(halves, axis=1)
        for cy in range(4):
            column = nn(both, perm[cy]).astype(BF16)
            at = (4 * cx + cy) * UNIT
            own_ref[at : at + UNIT] = column
            if cy > 0:
                at = (3 * cx + cy - 1) * UNIT
                up_ref[at : at + UNIT] = column
            if cy < 3:
                at = (3 * cx + cy) * UNIT
                dn_ref[at : at + UNIT] = column
    mask = (m_ref[...] > 0).astype(F32).reshape(64, Z).astype(BF16)
    cols = nt(sel, mask)
    cols = jnp.concatenate([cols[:ZC], cols[ZC:]], axis=1).astype(BF16)
    own_ref[OWN : OWN + ZC] = cols
    up_ref[SIDE : SIDE + ZC] = cols
    dn_ref[SIDE : SIDE + ZC] = cols


def mid_kernel(base_ref, own_ref, low_ref, high_ref, far_ref, near_ref):
    for ref, first in ((far_ref, base_ref[0]), (near_ref, 1 - base_ref[0])):
        for i in range(3):
            x = first + i
            at = 10 * i * UNIT
            ref[at : at + 3 * UNIT] = low_ref[pl.ds(pl.multiple_of(x * 3 * UNIT, 3 * UNIT), 3 * UNIT)]
            ref[at + 3 * UNIT : at + 7 * UNIT] = own_ref[pl.ds(pl.multiple_of(x * 4 * UNIT, 4 * UNIT), 4 * UNIT)]
            ref[at + 7 * UNIT : at + 10 * UNIT] = high_ref[pl.ds(pl.multiple_of(x * 3 * UNIT, 3 * UNIT), 3 * UNIT)]
        masks = [low_ref[SIDE : SIDE + ZC], own_ref[OWN : OWN + ZC], high_ref[SIDE : SIDE + ZC]]
        masks = jnp.concatenate([m.astype(F32) for m in masks], axis=0).astype(BF16)
        ref[EDGE : EDGE + 3 * ZC] = masks


def tap_of(out_bit, in_bit, far):
    if far:
        return 2 * (1 - in_bit) if out_bit != in_bit else None
    return in_bit - out_bit + 1


def placed(w_ref, rows, taps, group):
    total = jnp.zeros((CH, LANES), F32)
    for g, tap in enumerate(taps):
        if tap is not None:
            total = jnp.where(group == g, w_ref[rows : rows + CH, LANES * tap : LANES * tap + LANES], total)
    return total


def block(w_ref, rows, group, far_x, far_y, a_in, b_in, cz_in, shifted, cz_out):
    if shifted:
        tz = None
        if cz_out == 0 and cz_in == 1:
            tz = 0
        if cz_out == 1 and cz_in == 0:
            tz = 2
    else:
        tz = cz_in - cz_out + 1
    taps = []
    for a_out in BITS:
        for b_out in BITS:
            tx = tap_of(a_out, a_in, far_x)
            ty = tap_of(b_out, b_in, far_y)
            taps.append(None if tx is None or ty is None or tz is None else 9 * tx + 3 * ty + tz)
    return placed(w_ref, rows, taps, group)


KINDS = ((0, 0), (1, 0), (0, 1), (1, 1))


def weights_kernel(we_ref, wd_ref, wn_ref, oe_ref, od_ref, on_ref, re_ref, rd_ref, te_ref, td_ref):
    for tap in range(27):
        for g in range(4):
            at = LANES * tap + CH * g
            re_ref[at : at + CH] = we_ref[tap]
            rd_ref[at : at + CH] = wd_ref[tap]
    one = (iota((CH, CH), 0) == iota((CH, CH), 1)).astype(F32).astype(BF16)
    te_ref[...] = nt(one, re_ref[...])
    one = (iota((2 * CH, 2 * CH), 0) == iota((2 * CH, 2 * CH), 1)).astype(F32).astype(BF16)
    td_ref[...] = nt(one, rd_ref[...])
    group = iota((CH, LANES), 1) >> 5
    for w_ref, o_ref in ((te_ref, oe_ref), (td_ref, od_ref)):
        for t, (fx, fy) in enumerate(KINDS):
            for cz in BITS:
                for a in BITS:
                    for b in BITS:
                        base = 256 * t + 128 * cz + 64 * a + 32 * b
                        for s in BITS:
                            for co in BITS:
                                v = block(w_ref, 0, group, fx, fy, a, b, cz, s, co)
                                o_ref[base : base + CH, 256 * s + 128 * co : 256 * s + 128 * co + LANES] = v.astype(BF16)
    for t, (fx, fy) in enumerate(KINDS):
        for a in BITS:
            for b in BITS:
                base = 1024 + 128 * t + 64 * a + 32 * b
                for s in BITS:
                    for co in BITS:
                        v = block(td_ref, CH, group, fx, fy, a, b, 0, s, co)
                        v = v + block(td_ref, CH, group, fx, fy, a, b, 1, s, co)
                        od_ref[base : base + CH, 256 * s + 128 * co : 256 * s + 128 * co + LANES] = v.astype(BF16)
    k = iota((8 * CH, LANES), 0)
    goal = (((k >> 5) & 1) << 7) + ((k >> 6) << 5) + (k & 31) - iota((8 * CH, LANES), 1)
    perm = jnp.concatenate([(goal == LANES * i).astype(F32).astype(BF16) for i in BITS], axis=1)
    on_ref[...] = nn(wn_ref[...], perm).astype(BF16)


def moved(t, amount, edge):
    rows = t.shape[0]
    return jnp.where(edge, 0.0, pltpu.roll(t, amount % rows, 0))


def depth_of(rows):
    return iota((rows, LANES), 0) % ZC


def quad(bias):
    return jnp.concatenate([bias] * 4, axis=1)


def load_own(own_ref, low_ref, high_ref, a_ref, planes):
    for x in planes:
        for yi in range(10):
            if yi < 3:
                v = low_ref[(3 * x + yi) * UNIT : (3 * x + yi + 1) * UNIT]
            elif yi < 7:
                v = own_ref[(4 * x + yi - 3) * UNIT : (4 * x + yi - 2) * UNIT]
            else:
                v = high_ref[(3 * x + yi - 7) * UNIT : (3 * x + yi - 6) * UNIT]
            v = v.astype(F32)
            for cz in BITS:
                a_ref[3 + x, cz, yi * ZC : (yi + 1) * ZC] = v[cz * ZC : (cz + 1) * ZC]


def load_side(ref, start, a_ref):
    for i in range(3):
        for yi in range(10):
            v = ref[(10 * i + yi) * UNIT : (10 * i + yi + 1) * UNIT].astype(F32)
            for cz in BITS:
                a_ref[start + i, cz, yi * ZC : (yi + 1) * ZC] = v[cz * ZC : (cz + 1) * ZC]


def load_masks(at, parts, k_ref):
    for by, part in enumerate(parts):
        k = part.astype(F32)
        m = jnp.maximum(k, pltpu.roll(k, LANES - 1, 1))
        m = jnp.maximum(m, pltpu.roll(m, LANES - 8, 1))
        m = jnp.maximum(m, pltpu.roll(m, LANES - 64, 1))
        k_ref[0, at, by] = k
        k_ref[1, at, by] = m


def spread(k, index):
    parts = [jnp.take_along_axis(k[8 * i : 8 * i + 8], index, axis=1, mode="promise_in_bounds") for i in range(5)]
    return jnp.concatenate(parts, axis=0)


def local(i):
    return (i + 1) >> 2, (i + 1) & 3


def side_select(a_ref, v_ref, x):
    low_b = (iota((320, LANES), 1) & 32) == 0
    for cz in BITS:
        v_ref[x, cz] = jnp.where(low_b, a_ref[x, cz, 80:400], a_ref[x, cz, 0:320])


def encode(xi, a_ref, v_ref, k_ref, l_ref, e_ref, c_ref, o_ref, we_ref, be, wn_ref, gain, shift):
    low_a = iota((320, LANES), 1) < 64
    z8 = depth_of(320)
    first, last = z8 == 0, z8 == ZC - 1
    lane = iota((8, LANES), 1)
    lane_at = 8 * (lane >> 6) + ((lane >> 5) & 1)
    for cz in BITS:
        l_ref[:, 128 * cz : 128 * cz + 128] = a_ref[xi, cz, 40:360].astype(BF16)
        l_ref[:, 256 + 128 * cz : 384 + 128 * cz] = jnp.where(
            low_a, a_ref[xi + 1, cz, 40:360], a_ref[xi - 1, cz, 40:360]
        ).astype(BF16)
        l_ref[:, 512 + 128 * cz : 640 + 128 * cz] = v_ref[xi, cz].astype(BF16)
        l_ref[:, 768 + 128 * cz : 896 + 128 * cz] = jnp.where(low_a, v_ref[xi + 1, cz], v_ref[xi - 1, cz]).astype(BF16)
    o = nn(l_ref[:, 0:1024], we_ref[...])
    bx, lx = local(xi)
    expanded = [[], []]
    on = []
    for yi in range(1, 9):
        by, ly = local(yi)
        k = k_ref[0, bx, by]
        for cz in BITS:
            expanded[cz].append(spread(k, lane_at + (64 * cz + 2 * ly + 16 * lx)))
        on.append(spread(k_ref[1, bx, by], lane * 0 + (2 * ly + 16 * lx)))
    on = jnp.concatenate(on, axis=0)
    pre = (
        o[:, 0:128] + moved(o[:, 256:384], 1, first) + be,
        o[:, 128:256] + moved(o[:, 384:512], -1, last) + be,
    )
    enc = []
    for cz in BITS:
        active = jnp.concatenate(expanded[cz], axis=0) > 0.5
        e = jnp.where(active, silu(pre[cz]), 0.0)
        enc.append(e.astype(BF16))
        e_ref[xi - 1, cz] = rounded(e)[40:280]
    lifted = nt(jnp.concatenate(enc, axis=1), wn_ref[...])
    c = jnp.where(on > 0.5, silu(lifted * gain + shift), 0.0)
    c_ref[xi - 1] = rounded(c)
    o_ref[xi - 1] = on[40:280]


PAIRS = [(dx, dy) for dx in range(3) for dy in range(3)]


def coarse(xo, c_ref, o_ref, u_ref, wc_ref, bc, wu_ref):
    z6 = depth_of(240)
    first, last = z6 == 0, z6 == ZC - 1
    p = None
    for i in range(0, 9, 2):
        some = PAIRS[i : i + 2]
        lhs = [c_ref[xo + dx, dy * ZC : dy * ZC + 240].astype(BF16) for dx, dy in some]
        rhs = [wc_ref[9 * dx + 3 * dy : 9 * dx + 3 * dy + 3].reshape(384, 128) for dx, dy in some]
        lhs = jnp.concatenate(lhs, axis=1) if len(lhs) > 1 else lhs[0]
        rhs = jnp.concatenate(rhs, axis=1) if len(rhs) > 1 else rhs[0]
        q = nt(lhs, rhs)
        p = q if p is None else p + q
    s = p[:, 128:256] + moved(p[:, 0:128], 1, first) + moved(p[:, 256:384], -1, last) + bc
    act = jnp.where(o_ref[xo + 1] > 0.5, silu(s), 0.0).astype(BF16)
    u_ref[xo] = rounded(nt(act, jnp.concatenate([wu_ref[...]] * 4, axis=0)))


def near_kernel(
    near_ref_index, own_ref, low_ref, high_ref, side_ref, we_ref, be_ref, wn_ref, gain_ref, shift_ref, wc_ref, bc_ref,
    wu_ref, e_ref, c_ref, o_ref, u_ref, a_ref, v_ref, k_ref, l_ref,
):
    even = near_ref_index[0]
    load_own(own_ref, low_ref, high_ref, a_ref, range(4))
    load_side(side_ref, 7 * even, a_ref)
    load_masks(1, (low_ref[SIDE : SIDE + ZC], own_ref[OWN : OWN + ZC], high_ref[SIDE : SIDE + ZC]), k_ref)
    masks = side_ref[EDGE : EDGE + 3 * ZC].astype(F32)
    load_masks(2 * even, [masks[ZC * i : ZC * i + ZC] for i in range(3)], k_ref)
    start = 3 * even
    for i in range(7):
        side_select(a_ref, v_ref, start + i)
    be = quad(be_ref[...])
    for i in range(5):
        encode(
            start + 1 + i, a_ref, v_ref, k_ref, l_ref, e_ref, c_ref, o_ref, we_ref, be, wn_ref, gain_ref[...], shift_ref[...]
        )
    for i in range(3):
        coarse(start + i, c_ref, o_ref, u_ref, wc_ref, bc_ref[...], wu_ref)


def far_kernel(
    near_ref_index, own_ref, low_ref, high_ref, side_ref, we_ref, be_ref, wn_ref, gain_ref, shift_ref, wc_ref, bc_ref,
    wu_ref, e1_ref, c1_ref, o1_ref, u1_ref, m_ref, wd_ref, bd_ref, out_ref, a_ref, v_ref, k_ref, l_ref, e_ref, c_ref,
    o_ref, u_ref,
):
    even = near_ref_index[0]
    odd = 1 - even
    load_own(own_ref, low_ref, high_ref, a_ref, range(4))
    load_side(side_ref, 7 * odd, a_ref)
    load_masks(1, (low_ref[SIDE : SIDE + ZC], own_ref[OWN : OWN + ZC], high_ref[SIDE : SIDE + ZC]), k_ref)
    masks = side_ref[EDGE : EDGE + 3 * ZC].astype(F32)
    load_masks(2 * odd, [masks[ZC * i : ZC * i + ZC] for i in range(3)], k_ref)
    start = 5 * odd
    for i in range(5):
        side_select(a_ref, v_ref, start + i)
    be = quad(be_ref[...])
    for i in range(5):
        e_ref[3 * even + i] = e1_ref[3 * even + i]
        c_ref[3 * even + i] = c1_ref[3 * even + i]
        o_ref[3 * even + i] = o1_ref[3 * even + i]
    for i in range(3):
        u_ref[3 * even + i] = u1_ref[3 * even + i]
    for i in range(3):
        encode(
            start + 1 + i, a_ref, v_ref, k_ref, l_ref, e_ref, c_ref, o_ref, we_ref, be, wn_ref, gain_ref[...], shift_ref[...]
        )
    for i in range(3):
        coarse(3 * odd + i, c_ref, o_ref, u_ref, wc_ref, bc_ref[...], wu_ref)
    z4 = depth_of(160)
    first4, last4 = z4 == 0, z4 == ZC - 1
    la4 = iota((160, LANES), 1) < 64
    lb4 = (iota((160, LANES), 1) & 32) == 0
    bd = quad(bd_ref[...])

    def spans(load):
        mid = [load(i)[40:200] for i in range(3)]
        side = [jnp.where(lb4, load(i)[80:240], load(i)[0:160]) for i in range(3)]
        return mid[1], jnp.where(la4, mid[2], mid[0]), side[1], jnp.where(la4, side[2], side[0])

    back = unpick(LANES, Z)
    src = iota((512, LANES), 0)
    goal = (((src >> 6) & 1) << 8) + ((src & 31) << 3) + ((src >> 7) << 1) + ((src >> 5) & 1) - iota((512, LANES), 1)
    perm = jnp.concatenate([(goal == LANES * i).astype(F32).astype(BF16) for i in range(4)], axis=1)
    for xo in range(4):
        for cz in BITS:
            for t, v in enumerate(spans(lambda i: e_ref[xo + 1 + i, cz])):
                l_ref[0:160, 256 * t + 128 * cz : 256 * t + 128 * cz + 128] = v.astype(BF16)
        for t, v in enumerate(spans(lambda i: u_ref[xo + i])):
            l_ref[0:160, 1024 + 128 * t : 1152 + 128 * t] = v.astype(BF16)
        o = nn(l_ref[0:160, :], wd_ref[...])
        d0 = o[:, 0:128] + moved(o[:, 256:384], 1, first4) + bd
        d1 = o[:, 128:256] + moved(o[:, 384:512], -1, last4) + bd
        d = [jnp.concatenate([v[ZC * y : ZC * y + ZC] for y in range(4)], axis=1) for v in (d0, d1)]
        d = jnp.concatenate(d + [jnp.zeros((LANES - Z, 512), F32)], axis=0).astype(BF16)
        d = nn(d, perm)
        for a in BITS:
            t = jnp.transpose(d[:, 256 * a : 256 * a + 256]).astype(BF16)
            t = nn(t, back).reshape(CH, 8, Z)
            x = 2 * xo + a
            out_ref[:, x] = jnp.where(m_ref[x][None] > 0, t, 0.0).astype(BF16)


def vmem(n):
    return [pl.BlockSpec(memory_space=pltpu.VMEM)] * n


def call(kernel, outs, ins, scratch, mib, flops, name, scalar=False):
    return pl.pallas_call(
        kernel,
        out_shape=outs,
        in_specs=([pl.BlockSpec(memory_space=pltpu.SMEM)] if scalar else []) + vmem(ins),
        out_specs=vmem(len(outs)),
        scratch_shapes=[pltpu.VMEM(s, d) for s, d in scratch],
        compiler_params=pltpu.CompilerParams(vmem_limit_bytes=mib << 20),
        cost_estimate=pl.CostEstimate(flops=flops, bytes_accessed=10**6, transcendentals=0),
        name=name,
    )


def rows(n):
    return jax.ShapeDtypeStruct((n, LANES), BF16)


def shifted(value, axis, step):
    peers = lax.axis_size(axis)
    return lax.ppermute(value, axis, [(i, i + step) for i in range(peers) if 0 <= i + step < peers])


def swapped(value, axis, first):
    peers = lax.axis_size(axis)
    pairs = []
    for i in range(first, peers - 1, 2):
        pairs += [(i, i + 1), (i + 1, i)]
    return lax.ppermute(value, axis, pairs)


def time_features(timestep, embed_width):
    halves = embed_width // 2
    freqs = jnp.exp(-math.log(10000.0) * jnp.arange(halves, dtype=F32) / halves)
    angles = timestep[0].astype(F32) * freqs
    return jnp.concatenate([jnp.sin(angles), jnp.cos(angles)]).astype(BF16)


def on_device(
    fine_in, voxel_mask, timestep, w_enc, b_enc, w_down, w_time, w_coarse, b_coarse, w_up, w_dec, b_dec
):
    own, up, down = call(
        pack_kernel, [rows(OWN + ZC), rows(SIDE + ZC), rows(SIDE + ZC)], 2, [], 12, 10**9, "pack"
    )(fine_in, voxel_mask)
    low = shifted(up, "wide", 1)
    high = shifted(down, "wide", -1)

    embedded = time_features(timestep, w_time.shape[0])
    film = jnp.dot(embedded[None], w_time, preferred_element_type=F32)
    chans = w_down.shape[0]
    gains = 1.0 + film[:, :chans]
    shifts = film[:, chans:]
    enc_w, dec_w, down_w = call(
        weights_kernel,
        [
            jax.ShapeDtypeStruct((1024, 512), BF16),
            jax.ShapeDtypeStruct((1536, 512), BF16),
            jax.ShapeDtypeStruct((128, 256), BF16),
        ],
        3,
        [((27 * 128, 32), BF16), ((27 * 128, 64), BF16), ((32, 27 * 128), F32), ((64, 27 * 128), F32)],
        16,
        4 * 10**9,
        "weights",
    )(w_enc, w_dec, w_down)

    odd = lax.axis_index("narrow").astype(jnp.int32) & 1
    far_base = odd[None]
    near_right = 1 - far_base
    far, near = call(
        mid_kernel, [rows(EDGE + 3 * ZC), rows(EDGE + 3 * ZC)], 3, [], 8, 10**8, "mid", scalar=True
    )(far_base, own, low, high)
    far_side = swapped(far, "narrow", 1)
    near_side = swapped(near, "narrow", 0)

    planes = [((10, 2, 400, LANES), F32), ((10, 2, 320, LANES), F32), ((2, 3, 3, ZC, LANES), F32)]
    shared = [((8, 2, 240, LANES), F32), ((8, 320, LANES), F32), ((8, 240, LANES), F32), ((6, 240, LANES), F32)]
    some = (enc_w, b_enc[None], down_w, gains, shifts, w_coarse, b_coarse[None], w_up)
    state = call(
        near_kernel,
        [jax.ShapeDtypeStruct(s, d) for s, d in shared],
        12,
        planes + [((320, 1024), BF16)],
        24,
        5 * 10**9,
        "near",
        scalar=True,
    )(near_right, own, low, high, near_side, *some)
    return call(
        far_kernel,
        [jax.ShapeDtypeStruct(fine_in.shape, BF16)],
        19,
        planes + [((320, 1536), BF16)] + shared,
        30,
        5 * 10**9,
        "far",
        scalar=True,
    )(near_right, own, low, high, far_side, *some, *state, voxel_mask, dec_w, b_dec[None])[0]


def solution(mesh):
    field = P(None, "narrow", "wide", None)
    return jax.shard_map(
        on_device,
        mesh=mesh,
        in_specs=(field, P("narrow", "wide", None)) + (P(),) * 10,
        out_specs=field,
        check_vma=False,
    )
```

```python
import math

import jax
import jax.numpy as jnp
from jax import lax
from jax.experimental import pallas as pl
from jax.experimental.pallas import tpu as pltpu
from jax.sharding import PartitionSpec as P


F32 = jnp.float32
BF16 = jnp.bfloat16
LANES = 128
ZC = 40
Z = 80
CH = 32
BITS = (0, 1)


def nn(a, b):
    return lax.dot_general(a, b, (((1,), (0,)), ((), ())), preferred_element_type=F32)


def nt(a, b):
    return lax.dot_general(a, b, (((1,), (1,)), ((), ())), preferred_element_type=F32)


def iota(shape, dim):
    return lax.broadcasted_iota(jnp.int32, shape, dim)


PAIR = 2 * ZC
OWN = 16 * PAIR
SIDE = 8 * PAIR
SIDE_MASK = SIDE + 4 * ZC
SIDE_ROWS = SIDE_MASK + ZC
PLANE = 9 * PAIR
HALF = 5 * PAIR
EDGE_MASK = 2 * PLANE + HALF
EDGE_ROWS = EDGE_MASK + 3 * ZC


def one_where(truth):
    return truth.astype(F32).astype(BF16)


def unpick(rows, cols):
    row = iota((rows, cols), 0)
    return one_where(jnp.where(row < ZC, 2 * row, 2 * row - (Z - 1)) == iota((rows, cols), 1))


def low_a(rows):
    return iota((rows, LANES), 1) < 64


def low_b(rows):
    return (iota((rows, LANES), 1) & 32) == 0


def stacked(*parts):
    return jnp.concatenate(parts, axis=0)


def beside(*parts):
    return jnp.concatenate(parts, axis=1)


def pack_kernel(x_hbm, m_hbm, own_ref, up_ref, dn_ref, x_ref, m_ref, sems):
    copies = [pltpu.make_async_copy(m_hbm, m_ref, sems.at[4])]
    for cx in range(4):
        copies.append(pltpu.make_async_copy(x_hbm.at[:, pl.ds(2 * cx, 2)], x_ref.at[:, pl.ds(2 * cx, 2)], sems.at[cx]))
    for copy in copies:
        copy.start()
    sel = unpick(Z, Z)
    src = iota((512, LANES), 0)
    y = src & 7
    goal = ((y >> 1) << 7) + ((src >> 8) << 6) + ((y & 1) << 5) + ((src >> 3) & 31) - iota((512, LANES), 1)
    perm = [one_where(goal == LANES * i) for i in range(4)]
    copies[0].wait()
    mask = (m_ref[...] > 0).astype(F32).reshape(64, Z).astype(BF16)
    cols = nt(sel, mask)
    cols = beside(cols[:ZC], cols[ZC:]).astype(BF16)
    own_ref[OWN : OWN + ZC] = cols
    up_ref[SIDE_MASK:SIDE_ROWS] = cols
    dn_ref[SIDE_MASK:SIDE_ROWS] = cols
    ups, downs = [], []
    for cx in range(4):
        copies[1 + cx].wait()
        halves = []
        for a in BITS:
            x = 2 * cx + a
            tile = x_ref[:, x].astype(F32)
            tile = jnp.where(m_ref[x][None] > 0, tile, 0.0)
            halves.append(nt(sel, tile.reshape(8 * CH, Z).astype(BF16)).astype(BF16))
        both = beside(*halves)
        col = [nn(both, perm[cy]) for cy in range(4)]
        for cz in BITS:
            z = slice(ZC * cz, ZC * cz + ZC)
            first = stacked(col[0][z], col[1][z]).astype(BF16)
            second = stacked(col[2][z], col[3][z]).astype(BF16)
            own_ref[pl.ds((4 * cx + 2 * cz) * PAIR, PAIR)] = first
            own_ref[pl.ds((4 * cx + 2 * cz + 1) * PAIR, PAIR)] = second
            dn_ref[pl.ds((2 * cx + cz) * PAIR, PAIR)] = first
            up_ref[pl.ds((2 * cx + cz) * PAIR, PAIR)] = second
        ups.append(jnp.where(low_b(ZC), pltpu.roll(col[1][ZC:], LANES - 32, 1), col[1][:ZC]))
        downs.append(jnp.where(low_b(ZC), col[2][:ZC], pltpu.roll(col[2][ZC:], 32, 1)))
        if cx % 2 == 1:
            at = pl.ds(SIDE + (cx // 2) * PAIR, PAIR)
            up_ref[at] = stacked(*ups[-2:]).astype(BF16)
            dn_ref[at] = stacked(*downs[-2:]).astype(BF16)


def part(x, size):
    return pl.ds(pl.multiple_of(x * size, size), size)


def mid_kernel(odd_ref, own_ref, low_ref, high_ref, tie_ref, far_ref, near_ref, ends_ref):
    ends_ref[0] = low_ref[SIDE:SIDE_MASK].astype(F32)
    ends_ref[1] = high_ref[SIDE:SIDE_MASK].astype(F32)

    def layer(x, cz):
        return (
            low_ref[pl.ds(pl.multiple_of(x * 2 * PAIR + cz * PAIR, PAIR), PAIR)],
            own_ref[pl.ds(pl.multiple_of(x * 4 * PAIR + 2 * cz * PAIR, PAIR), 2 * PAIR)],
            high_ref[pl.ds(pl.multiple_of(x * 2 * PAIR + cz * PAIR, PAIR), PAIR)],
        )

    def ends(x):
        at = part(x, ZC)
        return stacked(ends_ref[0, at], ends_ref[1, at]).astype(BF16)

    lane_a = iota((PAIR, LANES), 1) >> 6
    for ref, right in ((far_ref, odd_ref[0]), (near_ref, 1 - odd_ref[0])):
        for i in range(2):
            x = 2 * right + i
            for cz in BITS:
                at = i * PLANE + 4 * cz * PAIR
                low, own, high = layer(x, cz)
                ref[at : at + PAIR] = low
                ref[at + PAIR : at + 3 * PAIR] = own
                ref[at + 3 * PAIR : at + 4 * PAIR] = high
            ref[i * PLANE + 8 * PAIR : (i + 1) * PLANE] = ends(x)
        x = 2 - right
        pieces = []
        for cz in BITS:
            low, own, high = layer(x, cz)
            pieces.append([v.astype(F32) for v in (low, own[:PAIR], own[PAIR:], high)])
        for i in range(4):
            v = jnp.where(lane_a == right, pieces[0][i], pltpu.roll(pieces[1][i], 64, 1))
            ref[2 * PLANE + i * PAIR : 2 * PLANE + (i + 1) * PAIR] = v.astype(BF16)
        ref[2 * PLANE + 4 * PAIR : EDGE_MASK] = ends(x)
        masks = [low_ref[SIDE_MASK:SIDE_ROWS], own_ref[OWN : OWN + ZC], high_ref[SIDE_MASK:SIDE_ROWS]]
        ref[EDGE_MASK:EDGE_ROWS] = stacked(*[m.astype(F32) for m in masks]).astype(BF16)


def tap_of(out_bit, in_bit, far):
    if far:
        return 2 * (1 - in_bit) if out_bit != in_bit else None
    return in_bit - out_bit + 1


def placed(w_ref, rows, taps, group):
    total = jnp.zeros((CH, LANES), F32)
    for g, tap in enumerate(taps):
        if tap is not None:
            total = jnp.where(group == g, w_ref[rows : rows + CH, LANES * tap : LANES * tap + LANES], total)
    return total


def block(w_ref, rows, group, far_x, far_y, a_in, b_in, cz_in, shifted, cz_out):
    if shifted:
        tz = None
        if cz_out == 0 and cz_in == 1:
            tz = 0
        if cz_out == 1 and cz_in == 0:
            tz = 2
    else:
        tz = cz_in - cz_out + 1
    taps = []
    for a_out in BITS:
        for b_out in BITS:
            tx = tap_of(a_out, a_in, far_x)
            ty = tap_of(b_out, b_in, far_y)
            taps.append(None if tx is None or ty is None or tz is None else 9 * tx + 3 * ty + tz)
    return placed(w_ref, rows, taps, group)


KINDS = ((0, 0), (1, 0), (0, 1), (1, 1))


def weights_kernel(we_ref, wd_ref, wn_ref, oe_ref, od_ref, on_ref, re_ref, rd_ref, te_ref, td_ref):
    for tap in range(27):
        for g in range(4):
            at = LANES * tap + CH * g
            re_ref[at : at + CH] = we_ref[tap]
            rd_ref[at : at + CH] = wd_ref[tap]
    one = (iota((CH, CH), 0) == iota((CH, CH), 1)).astype(F32).astype(BF16)
    te_ref[...] = nt(one, re_ref[...])
    one = (iota((2 * CH, 2 * CH), 0) == iota((2 * CH, 2 * CH), 1)).astype(F32).astype(BF16)
    td_ref[...] = nt(one, rd_ref[...])
    group = iota((CH, LANES), 1) >> 5
    for w_ref, o_ref in ((te_ref, oe_ref), (td_ref, od_ref)):
        for t, (fx, fy) in enumerate(KINDS):
            for cz in BITS:
                for a in BITS:
                    for b in BITS:
                        base = 256 * t + 128 * cz + 64 * a + 32 * b
                        for s in BITS:
                            for co in BITS:
                                v = block(w_ref, 0, group, fx, fy, a, b, cz, s, co)
                                o_ref[base : base + CH, 256 * s + 128 * co : 256 * s + 128 * co + LANES] = v.astype(BF16)
    for t, (fx, fy) in enumerate(KINDS):
        for a in BITS:
            for b in BITS:
                base = 1024 + 128 * t + 64 * a + 32 * b
                for s in BITS:
                    for co in BITS:
                        v = block(td_ref, CH, group, fx, fy, a, b, 0, s, co)
                        v = v + block(td_ref, CH, group, fx, fy, a, b, 1, s, co)
                        od_ref[base : base + CH, 256 * s + 128 * co : 256 * s + 128 * co + LANES] = v.astype(BF16)
    k = iota((8 * CH, LANES), 0)
    goal = (((k >> 5) & 1) << 7) + ((k >> 6) << 5) + (k & 31) - iota((8 * CH, LANES), 1)
    perm = jnp.concatenate([(goal == LANES * i).astype(F32).astype(BF16) for i in BITS], axis=1)
    on_ref[...] = nn(wn_ref[...], perm).astype(BF16)


def moved(t, amount, edge):
    rows = t.shape[0]
    return jnp.where(edge, 0.0, pltpu.roll(t, amount % rows, 0))


def depth_of(rows):
    return iota((rows, LANES), 0) % ZC


def quad(bias):
    return beside(bias, bias, bias, bias)


def put_plane(a_ref, v_ref, at, layers, ends):
    y0, y9 = ends[:ZC].astype(F32), ends[ZC:].astype(F32)
    for cz in BITS:
        a_ref[at, cz] = layers[cz].astype(BF16)
        f = layers[cz].astype(F32)
        if cz == 1:
            y0, y9 = pltpu.roll(y0, 32, 1), pltpu.roll(y9, LANES - 32, 1)
        f = stacked(y0, f, y9)
        v_ref[at, cz] = jnp.where(low_b(320), f[PAIR:], f[:320]).astype(BF16)


def load_own(own_ref, low_ref, high_ref, a_ref, v_ref):
    low_ends = low_ref[SIDE:SIDE_MASK].astype(F32)
    high_ends = high_ref[SIDE:SIDE_MASK].astype(F32)
    for x in range(4):
        layers = []
        for cz in BITS:
            at = (2 * x + cz) * PAIR
            mine = (4 * x + 2 * cz) * PAIR
            layers.append(
                stacked(low_ref[at : at + PAIR], own_ref[mine : mine + 2 * PAIR], high_ref[at : at + PAIR])
            )
        z = slice(ZC * x, ZC * x + ZC)
        put_plane(a_ref, v_ref, 3 + x, layers, stacked(low_ends[z], high_ends[z]))


def load_side(ref, right, a_ref, v_ref):
    for i in range(2):
        at = i * PLANE
        layers = [ref[at + 320 * cz : at + 320 * cz + 320] for cz in BITS]
        put_plane(a_ref, v_ref, 1 + 6 * right + i, layers, ref[at + 640 : at + PLANE].astype(F32))
    at = 2 * PLANE
    both = ref[at : at + 320].astype(F32)
    put_plane(a_ref, v_ref, 9 * right, [both, pltpu.roll(both, 64, 1)], ref[at + 320 : at + HALF].astype(F32))


def load_masks(at, parts, k_ref):
    for by, k in enumerate(parts):
        k = k.astype(F32)
        m = jnp.maximum(k, pltpu.roll(k, LANES - 1, 1))
        m = jnp.maximum(m, pltpu.roll(m, LANES - 8, 1))
        m = jnp.maximum(m, pltpu.roll(m, LANES - 64, 1))
        k_ref[0, at, by] = k
        k_ref[1, at, by] = m


def load_all(own_ref, low_ref, high_ref, side_ref, right, a_ref, v_ref, k_ref):
    load_own(own_ref, low_ref, high_ref, a_ref, v_ref)
    load_side(side_ref, right, a_ref, v_ref)
    load_masks(1, (low_ref[SIDE_MASK:SIDE_ROWS], own_ref[OWN : OWN + ZC], high_ref[SIDE_MASK:SIDE_ROWS]), k_ref)
    masks = side_ref[EDGE_MASK:EDGE_ROWS].astype(F32)
    load_masks(2 * right, [masks[ZC * i : ZC * i + ZC] for i in range(3)], k_ref)


def spread(k, index):
    return stacked(*[jnp.take_along_axis(k[8 * i : 8 * i + 8], index, axis=1, mode="promise_in_bounds") for i in range(5)])


def local(i):
    return (i + 1) >> 2, (i + 1) & 3


def silu(v):
    half = 0.5 * v
    return half + half * jnp.tanh(half)


def joined_x(ref, x, cz, lane_a, rows):
    return jnp.where(lane_a, ref[x + 1, cz, rows], ref[x - 1, cz, rows])


def lanes_a(rows):
    return one_where(low_a(rows)) > 0.5


def encode(xi, a_ref, v_ref, k_ref, e_ref, ev_ref, c_ref, d_ref, o_ref, we_ref, be, wn_ref, gain, shift):
    z8 = depth_of(320)
    first, last = z8 == 0, z8 == ZC - 1
    lane = iota((8, LANES), 1)
    lane_at = 8 * (lane >> 6) + ((lane >> 5) & 1)
    la = lanes_a(320)
    every = slice(0, 320)
    lhs = [a_ref[xi, cz] for cz in BITS] + [joined_x(a_ref, xi, cz, la, every) for cz in BITS]
    lhs += [v_ref[xi, cz] for cz in BITS] + [joined_x(v_ref, xi, cz, la, every) for cz in BITS]
    o = nn(beside(*lhs), we_ref[...])
    bx, lx = local(xi)
    expanded = [[], []]
    on = []
    for yi in range(1, 9):
        by, ly = local(yi)
        k = k_ref[0, bx, by]
        for cz in BITS:
            expanded[cz].append(spread(k, lane_at + (64 * cz + 2 * ly + 16 * lx)))
        on.append(spread(k_ref[1, bx, by], lane * 0 + (2 * ly + 16 * lx)))
    on = stacked(*on)
    pre = (
        o[:, 0:128] + moved(o[:, 256:384], 1, first) + be,
        o[:, 128:256] + moved(o[:, 384:512], -1, last) + be,
    )
    enc = []
    for cz in BITS:
        e = jnp.where(stacked(*expanded[cz]) > 0.5, silu(pre[cz]), 0.0)
        enc.append(e.astype(BF16))
        e_ref[xi - 1, cz] = enc[cz]
        ev_ref[xi - 1, cz] = jnp.where(low_b(160), e[120:280], e[40:200]).astype(BF16)
    lifted = nt(beside(*enc), wn_ref[...])
    c = jnp.where(on > 0.5, silu(lifted * gain + shift), 0.0)
    c_ref[xi - 1] = c.astype(BF16)
    d_ref[xi - 1] = c[40:280].astype(BF16)
    o_ref[xi - 1] = on[40:280]


def coarse(xo, c_ref, d_ref, o_ref, u_ref, wc_ref, bc, wu_ref):
    z6 = depth_of(240)
    first, last = z6 == 0, z6 == ZC - 1
    lhs, rhs = [], []
    for dx in range(3):
        for dy in range(3):
            lhs.append(d_ref[xo + dx] if dy == 1 else c_ref[xo + dx, 40 * dy : 40 * dy + 240])
            rhs.append(wc_ref[9 * dx + 3 * dy : 9 * dx + 3 * dy + 3].reshape(384, 128))
    p = nt(beside(*lhs), beside(*rhs))
    s = p[:, 128:256] + moved(p[:, 0:128], 1, first) + moved(p[:, 256:384], -1, last) + bc
    act = jnp.where(o_ref[xo + 1] > 0.5, silu(s), 0.0).astype(BF16)
    u = nt(act, stacked(*([wu_ref[...]] * 4)))
    u_ref[xo, 0] = u[40:200].astype(BF16)
    u_ref[xo, 1] = jnp.where(low_b(160), u[80:240], u[0:160]).astype(BF16)


def decode(xo, e_ref, ev_ref, u_ref, wd_ref, bd, perm, back, m_ref, out_ref):
    z4 = depth_of(160)
    first, last = z4 == 0, z4 == ZC - 1
    la = lanes_a(160)
    mid, every = slice(80, 240), slice(0, 160)
    x = xo + 2
    lhs = [e_ref[x, cz, mid] for cz in BITS] + [joined_x(e_ref, x, cz, la, mid) for cz in BITS]
    lhs += [ev_ref[x, cz] for cz in BITS] + [joined_x(ev_ref, x, cz, la, every) for cz in BITS]
    x = xo + 1
    for v in BITS:
        lhs += [u_ref[x, v], joined_x(u_ref, x, v, la, every)]
    o = nn(beside(*lhs), wd_ref[...])
    d0 = o[:, 0:128] + moved(o[:, 256:384], 1, first) + bd
    d1 = o[:, 128:256] + moved(o[:, 384:512], -1, last) + bd
    d = [beside(*[v[ZC * y : ZC * y + ZC] for y in range(4)]) for v in (d0, d1)]
    d = stacked(*d, jnp.zeros((LANES - Z, 512), F32)).astype(BF16)
    d = nn(d, perm)
    for a in BITS:
        t = jnp.transpose(d[:, 256 * a : 256 * a + 256]).astype(BF16)
        t = nn(t, back).reshape(CH, 8, Z)
        x = 2 * xo + a
        out_ref[:, x] = jnp.where(m_ref[x][None] > 0, t, 0.0).astype(BF16)


def near_kernel(
    right_ref, own_ref, low_ref, high_ref, side_ref, we_ref, be_ref, wn_ref, gain_ref, shift_ref, wc_ref, bc_ref,
    wu_ref, e_ref, ev_ref, c_ref, d_ref, o_ref, u_ref, a_ref, v_ref, k_ref,
):
    right = right_ref[0]
    load_all(own_ref, low_ref, high_ref, side_ref, right, a_ref, v_ref, k_ref)
    be = quad(be_ref[...])
    for i in range(5):
        encode(
            3 * right + 1 + i, a_ref, v_ref, k_ref, e_ref, ev_ref, c_ref, d_ref, o_ref, we_ref, be, wn_ref,
            gain_ref[...], shift_ref[...],
        )
    for i in range(3):
        coarse(3 * right + i, c_ref, d_ref, o_ref, u_ref, wc_ref, bc_ref[...], wu_ref)


def far_kernel(
    right_ref, own_ref, low_ref, high_ref, side_ref, we_ref, be_ref, wn_ref, gain_ref, shift_ref, wc_ref, bc_ref,
    wu_ref, e1_ref, ev1_ref, c1_ref, d1_ref, o1_ref, u1_ref, m_ref, wd_ref, bd_ref, out_hbm, a_ref, v_ref, k_ref,
    e_ref, ev_ref, c_ref, d_ref, o_ref, u_ref, out_ref, sems,
):
    right = 1 - right_ref[0]
    left = 1 - right
    load_all(own_ref, low_ref, high_ref, side_ref, right, a_ref, v_ref, k_ref)
    be = quad(be_ref[...])
    kept = ((e_ref, e1_ref), (ev_ref, ev1_ref), (c_ref, c1_ref), (d_ref, d1_ref), (o_ref, o1_ref))
    for i in range(5):
        for ref, given in kept:
            ref[3 * left + i] = given[3 * left + i]
    for i in range(3):
        u_ref[3 * left + i] = u1_ref[3 * left + i]
    for i in range(3):
        encode(
            5 * right + 1 + i, a_ref, v_ref, k_ref, e_ref, ev_ref, c_ref, d_ref, o_ref, we_ref, be, wn_ref,
            gain_ref[...], shift_ref[...],
        )
    for i in range(3):
        coarse(3 * right + i, c_ref, d_ref, o_ref, u_ref, wc_ref, bc_ref[...], wu_ref)
    bd = quad(bd_ref[...])
    back = unpick(LANES, Z)
    src = iota((512, LANES), 0)
    goal = (((src >> 6) & 1) << 8) + ((src & 31) << 3) + ((src >> 7) << 1) + ((src >> 5) & 1) - iota((512, LANES), 1)
    perm = beside(*[one_where(goal == LANES * i) for i in range(4)])
    copies = []
    for xo in range(4):
        decode(xo, e_ref, ev_ref, u_ref, wd_ref, bd, perm, back, m_ref, out_ref)
        at = pl.ds(2 * xo, 2)
        copies.append(pltpu.make_async_copy(out_ref.at[:, at], out_hbm.at[:, at], sems.at[xo]))
        copies[-1].start()
    for copy in copies:
        copy.wait()


def vmem(n):
    return [pl.BlockSpec(memory_space=pltpu.VMEM)] * n


def hbm(n):
    return [pl.BlockSpec(memory_space=pltpu.HBM)] * n


def call(kernel, outs, ins, out_specs, scratch, mib, flops):
    return pl.pallas_call(
        kernel,
        out_shape=outs,
        in_specs=ins,
        out_specs=out_specs,
        scratch_shapes=scratch,
        compiler_params=pltpu.CompilerParams(vmem_limit_bytes=mib << 20),
        cost_estimate=pl.CostEstimate(flops=flops, bytes_accessed=10**6, transcendentals=0),
    )


def array(*shape, kind=BF16):
    return jax.ShapeDtypeStruct(shape, kind)


def buffers(shapes):
    return [pltpu.VMEM(s, d) for s, d in shapes]


def shifted(value, axis, step):
    peers = lax.axis_size(axis)
    return lax.ppermute(value, axis, [(i, i + step) for i in range(peers) if 0 <= i + step < peers])


def swapped(value, axis, first):
    peers = lax.axis_size(axis)
    pairs = []
    for i in range(first, peers - 1, 2):
        pairs += [(i, i + 1), (i + 1, i)]
    return lax.ppermute(value, axis, pairs)


def time_features(timestep, embed_width):
    halves = embed_width // 2
    freqs = jnp.exp(-math.log(10000.0) * jnp.arange(halves, dtype=F32) / halves)
    angles = timestep[0].astype(F32) * freqs
    return jnp.concatenate([jnp.sin(angles), jnp.cos(angles)]).astype(BF16)


SCALAR = [pl.BlockSpec(memory_space=pltpu.SMEM)]
PLANES = [((10, 2, 320, LANES), BF16), ((10, 2, 320, LANES), BF16), ((2, 3, 3, ZC, LANES), F32)]
STATE = [
    ((8, 2, 320, LANES), BF16),
    ((8, 2, 160, LANES), BF16),
    ((8, 320, LANES), BF16),
    ((8, 240, LANES), BF16),
    ((8, 240, LANES), F32),
    ((6, 2, 160, LANES), BF16),
]


def on_device(
    fine_in, voxel_mask, timestep, w_enc, b_enc, w_down, w_time, w_coarse, b_coarse, w_up, w_dec, b_dec
):
    own, up, down = call(
        pack_kernel,
        [array(OWN + ZC, LANES), array(SIDE_ROWS, LANES), array(SIDE_ROWS, LANES)],
        hbm(2),
        vmem(3),
        [pltpu.VMEM(fine_in.shape, BF16), pltpu.VMEM(voxel_mask.shape, jnp.int32), pltpu.SemaphoreType.DMA((5,))],
        12,
        10**9,
    )(fine_in, voxel_mask)
    low = shifted(up, "wide", 1)
    high = shifted(down, "wide", -1)

    embedded = time_features(timestep, w_time.shape[0])
    film = jnp.dot(embedded[None], w_time, preferred_element_type=F32)
    chans = w_down.shape[0]
    gains = 1.0 + film[:, :chans]
    shifts = film[:, chans:]
    taps = 27 * LANES
    enc_w, dec_w, down_w = call(
        weights_kernel,
        [array(1024, 512), array(1536, 512), array(128, 256)],
        vmem(3),
        vmem(3),
        buffers([((taps, 32), BF16), ((taps, 64), BF16), ((32, taps), F32), ((64, taps), F32)]),
        16,
        4 * 10**9,
    )(w_enc, w_dec, w_down)

    odd = lax.axis_index("narrow").astype(jnp.int32)[None] & 1
    near_right = 1 - odd
    far, near = call(
        mid_kernel,
        [array(EDGE_ROWS, LANES), array(EDGE_ROWS, LANES)],
        SCALAR + vmem(4),
        vmem(2),
        buffers([((2, 4 * ZC, LANES), F32)]),
        8,
        10**8,
    )(odd, own, low, high, down_w)
    far_side = swapped(far, "narrow", 1)
    near_side = swapped(near, "narrow", 0)

    some = (enc_w, b_enc[None], down_w, gains, shifts, w_coarse, b_coarse[None], w_up)
    state = call(
        near_kernel, [array(*s, kind=d) for s, d in STATE], SCALAR + vmem(12), vmem(6), buffers(PLANES), 20, 5 * 10**9
    )(near_right, own, low, high, near_side, *some)
    return call(
        far_kernel,
        [array(*fine_in.shape)],
        SCALAR + vmem(21),
        hbm(1),
        buffers(PLANES + STATE) + [pltpu.VMEM(fine_in.shape, BF16), pltpu.SemaphoreType.DMA((4,))],
        24,
        5 * 10**9,
    )(near_right, own, low, high, far_side, *some, *state, voxel_mask, dec_w, b_dec[None])[0]


def solution(mesh):
    field = P(None, "narrow", "wide", None)
    return jax.shard_map(
        on_device,
        mesh=mesh,
        in_specs=(field, P("narrow", "wide", None)) + (P(),) * 10,
        out_specs=field,
        check_vma=False,
    )
```

```python
import math

import jax
import jax.numpy as jnp
from jax import lax
from jax.experimental import pallas as pl
from jax.experimental.pallas import tpu as pltpu
from jax.sharding import PartitionSpec as P


F32 = jnp.float32
BF16 = jnp.bfloat16
LANES = 128
ZC = 40
Z = 80
CH = 32
BITS = (0, 1)


def nn(a, b):
    return lax.dot_general(a, b, (((1,), (0,)), ((), ())), preferred_element_type=F32)


def nt(a, b):
    return lax.dot_general(a, b, (((1,), (1,)), ((), ())), preferred_element_type=F32)


def iota(shape, dim):
    return lax.broadcasted_iota(jnp.int32, shape, dim)


PAIR = 2 * ZC
OWN = 16 * PAIR
SIDE = 8 * PAIR
SIDE_MASK = SIDE + 4 * ZC
SIDE_ROWS = SIDE_MASK + ZC
PLANE = 9 * PAIR
HALF = 5 * PAIR
EDGE_MASK = 2 * PLANE + HALF
EDGE_ROWS = EDGE_MASK + 3 * ZC


def one_where(truth):
    return truth.astype(F32).astype(BF16)


def unpick(rows, cols):
    row = iota((rows, cols), 0)
    return one_where(jnp.where(row < ZC, 2 * row, 2 * row - (Z - 1)) == iota((rows, cols), 1))


def low_a(rows):
    return iota((rows, LANES), 1) < 64


def low_b(rows):
    return (iota((rows, LANES), 1) & 32) == 0


def stacked(*parts):
    return jnp.concatenate(parts, axis=0)


def beside(*parts):
    return jnp.concatenate(parts, axis=1)


def pack_kernel(x_hbm, m_hbm, own_ref, up_ref, dn_ref, x_ref, m_ref, sems):
    copies = [pltpu.make_async_copy(m_hbm, m_ref, sems.at[4])]
    for cx in range(4):
        copies.append(pltpu.make_async_copy(x_hbm.at[:, pl.ds(2 * cx, 2)], x_ref.at[:, pl.ds(2 * cx, 2)], sems.at[cx]))
    for copy in copies:
        copy.start()
    sel = unpick(Z, Z)
    src = iota((512, LANES), 0)
    y = src & 7
    goal = ((y >> 1) << 7) + ((src >> 8) << 6) + ((y & 1) << 5) + ((src >> 3) & 31) - iota((512, LANES), 1)
    perm = [one_where(goal == LANES * i) for i in range(4)]
    copies[0].wait()
    mask = (m_ref[...] > 0).astype(F32).reshape(64, Z).astype(BF16)
    cols = nt(sel, mask)
    cols = beside(cols[:ZC], cols[ZC:]).astype(BF16)
    own_ref[OWN : OWN + ZC] = cols
    up_ref[SIDE_MASK:SIDE_ROWS] = cols
    dn_ref[SIDE_MASK:SIDE_ROWS] = cols
    ups, downs = [], []
    for cx in range(4):
        copies[1 + cx].wait()
        halves = []
        for a in BITS:
            x = 2 * cx + a
            tile = x_ref[:, x].astype(F32)
            tile = jnp.where(m_ref[x][None] > 0, tile, 0.0)
            halves.append(nt(sel, tile.reshape(8 * CH, Z).astype(BF16)).astype(BF16))
        both = beside(*halves)
        col = [nn(both, perm[cy]) for cy in range(4)]
        for cz in BITS:
            z = slice(ZC * cz, ZC * cz + ZC)
            first = stacked(col[0][z], col[1][z]).astype(BF16)
            second = stacked(col[2][z], col[3][z]).astype(BF16)
            own_ref[pl.ds((4 * cx + 2 * cz) * PAIR, PAIR)] = first
            own_ref[pl.ds((4 * cx + 2 * cz + 1) * PAIR, PAIR)] = second
            dn_ref[pl.ds((2 * cx + cz) * PAIR, PAIR)] = first
            up_ref[pl.ds((2 * cx + cz) * PAIR, PAIR)] = second
        ups.append(jnp.where(low_b(ZC), pltpu.roll(col[1][ZC:], LANES - 32, 1), col[1][:ZC]))
        downs.append(jnp.where(low_b(ZC), col[2][:ZC], pltpu.roll(col[2][ZC:], 32, 1)))
        if cx % 2 == 1:
            at = pl.ds(SIDE + (cx // 2) * PAIR, PAIR)
            up_ref[at] = stacked(*ups[-2:]).astype(BF16)
            dn_ref[at] = stacked(*downs[-2:]).astype(BF16)


def part(x, size):
    return pl.ds(pl.multiple_of(x * size, size), size)


def mid_kernel(odd_ref, own_ref, low_ref, high_ref, tie_ref, far_ref, near_ref, ends_ref):
    ends_ref[0] = low_ref[SIDE:SIDE_MASK].astype(F32)
    ends_ref[1] = high_ref[SIDE:SIDE_MASK].astype(F32)

    def layer(x, cz):
        return (
            low_ref[pl.ds(pl.multiple_of(x * 2 * PAIR + cz * PAIR, PAIR), PAIR)],
            own_ref[pl.ds(pl.multiple_of(x * 4 * PAIR + 2 * cz * PAIR, PAIR), 2 * PAIR)],
            high_ref[pl.ds(pl.multiple_of(x * 2 * PAIR + cz * PAIR, PAIR), PAIR)],
        )

    def ends(x):
        at = part(x, ZC)
        return stacked(ends_ref[0, at], ends_ref[1, at]).astype(BF16)

    lane_a = iota((PAIR, LANES), 1) >> 6
    for ref, right in ((far_ref, odd_ref[0]), (near_ref, 1 - odd_ref[0])):
        for i in range(2):
            x = 2 * right + i
            for cz in BITS:
                at = i * PLANE + 4 * cz * PAIR
                low, own, high = layer(x, cz)
                ref[at : at + PAIR] = low
                ref[at + PAIR : at + 3 * PAIR] = own
                ref[at + 3 * PAIR : at + 4 * PAIR] = high
            ref[i * PLANE + 8 * PAIR : (i + 1) * PLANE] = ends(x)
        x = 2 - right
        pieces = []
        for cz in BITS:
            low, own, high = layer(x, cz)
            pieces.append([v.astype(F32) for v in (low, own[:PAIR], own[PAIR:], high)])
        for i in range(4):
            v = jnp.where(lane_a == right, pieces[0][i], pltpu.roll(pieces[1][i], 64, 1))
            ref[2 * PLANE + i * PAIR : 2 * PLANE + (i + 1) * PAIR] = v.astype(BF16)
        ref[2 * PLANE + 4 * PAIR : EDGE_MASK] = ends(x)
        masks = [low_ref[SIDE_MASK:SIDE_ROWS], own_ref[OWN : OWN + ZC], high_ref[SIDE_MASK:SIDE_ROWS]]
        ref[EDGE_MASK:EDGE_ROWS] = stacked(*[m.astype(F32) for m in masks]).astype(BF16)


def tap_of(out_bit, in_bit, far):
    if far:
        return 2 * (1 - in_bit) if out_bit != in_bit else None
    return in_bit - out_bit + 1


def placed(w_ref, rows, taps, group):
    total = jnp.zeros((CH, LANES), F32)
    for g, tap in enumerate(taps):
        if tap is not None:
            total = jnp.where(group == g, w_ref[rows : rows + CH, LANES * tap : LANES * tap + LANES], total)
    return total


def block(w_ref, rows, group, far_x, far_y, a_in, b_in, cz_in, shifted, cz_out):
    if shifted:
        tz = None
        if cz_out == 0 and cz_in == 1:
            tz = 0
        if cz_out == 1 and cz_in == 0:
            tz = 2
    else:
        tz = cz_in - cz_out + 1
    taps = []
    for a_out in BITS:
        for b_out in BITS:
            tx = tap_of(a_out, a_in, far_x)
            ty = tap_of(b_out, b_in, far_y)
            taps.append(None if tx is None or ty is None or tz is None else 9 * tx + 3 * ty + tz)
    return placed(w_ref, rows, taps, group)


KINDS = ((0, 0), (1, 0), (0, 1), (1, 1))


def weights_kernel(we_ref, wd_ref, wn_ref, oe_ref, od_ref, on_ref, op_ref, ob_ref, re_ref, rd_ref, te_ref, td_ref):
    for tap in range(27):
        for g in range(4):
            at = LANES * tap + CH * g
            re_ref[at : at + CH] = we_ref[tap]
            rd_ref[at : at + CH] = wd_ref[tap]
    one = (iota((CH, CH), 0) == iota((CH, CH), 1)).astype(F32).astype(BF16)
    te_ref[...] = nt(one, re_ref[...])
    one = (iota((2 * CH, 2 * CH), 0) == iota((2 * CH, 2 * CH), 1)).astype(F32).astype(BF16)
    td_ref[...] = nt(one, rd_ref[...])
    group = iota((CH, LANES), 1) >> 5
    for w_ref, o_ref in ((te_ref, oe_ref), (td_ref, od_ref)):
        for t, (fx, fy) in enumerate(KINDS):
            for cz in BITS:
                for a in BITS:
                    for b in BITS:
                        base = 256 * t + 128 * cz + 64 * a + 32 * b
                        for s in BITS:
                            for co in BITS:
                                v = block(w_ref, 0, group, fx, fy, a, b, cz, s, co)
                                o_ref[base : base + CH, 256 * s + 128 * co : 256 * s + 128 * co + LANES] = v.astype(BF16)
    for t, (fx, fy) in enumerate(KINDS):
        for a in BITS:
            for b in BITS:
                base = 1024 + 128 * t + 64 * a + 32 * b
                for s in BITS:
                    for co in BITS:
                        v = block(td_ref, CH, group, fx, fy, a, b, 0, s, co)
                        v = v + block(td_ref, CH, group, fx, fy, a, b, 1, s, co)
                        od_ref[base : base + CH, 256 * s + 128 * co : 256 * s + 128 * co + LANES] = v.astype(BF16)
    k = iota((8 * CH, LANES), 0)
    goal = (((k >> 5) & 1) << 7) + ((k >> 6) << 5) + (k & 31) - iota((8 * CH, LANES), 1)
    perm = jnp.concatenate([(goal == LANES * i).astype(F32).astype(BF16) for i in BITS], axis=1)
    on_ref[...] = nn(wn_ref[...], perm).astype(BF16)
    src = iota((512, LANES), 0)
    goal = (((src >> 6) & 1) << 8) + ((src & 31) << 3) + ((src >> 7) << 1) + ((src >> 5) & 1) - iota((512, LANES), 1)
    op_ref[...] = beside(*[one_where(goal == LANES * i) for i in range(4)])
    column = iota((Z, LANES), 1)
    goal = jnp.where(column < ZC, 2 * column, jnp.where(column < Z, 2 * column - (Z - 1), -1))
    ob_ref[...] = one_where(goal == iota((Z, LANES), 0))


def moved(t, amount, edge):
    rows = t.shape[0]
    return jnp.where(edge, 0.0, pltpu.roll(t, amount % rows, 0))


def depth_of(rows):
    return iota((rows, LANES), 0) % ZC


def quad(bias):
    return beside(bias, bias, bias, bias)


def put_plane(a_ref, v_ref, at, layers, ends):
    y0, y9 = ends[:ZC].astype(F32), ends[ZC:].astype(F32)
    for cz in BITS:
        a_ref[at, cz] = layers[cz].astype(BF16)
        f = layers[cz].astype(F32)
        if cz == 1:
            y0, y9 = pltpu.roll(y0, 32, 1), pltpu.roll(y9, LANES - 32, 1)
        f = stacked(y0, f, y9)
        v_ref[at, cz] = jnp.where(low_b(320), f[PAIR:], f[:320]).astype(BF16)


def load_own(own_ref, low_ref, high_ref, a_ref, v_ref):
    low_ends = low_ref[SIDE:SIDE_MASK].astype(F32)
    high_ends = high_ref[SIDE:SIDE_MASK].astype(F32)
    for x in range(4):
        layers = []
        for cz in BITS:
            at = (2 * x + cz) * PAIR
            mine = (4 * x + 2 * cz) * PAIR
            layers.append(
                stacked(low_ref[at : at + PAIR], own_ref[mine : mine + 2 * PAIR], high_ref[at : at + PAIR])
            )
        z = slice(ZC * x, ZC * x + ZC)
        put_plane(a_ref, v_ref, 3 + x, layers, stacked(low_ends[z], high_ends[z]))


def load_side(ref, right, a_ref, v_ref):
    for i in range(2):
        at = i * PLANE
        layers = [ref[at + 320 * cz : at + 320 * cz + 320] for cz in BITS]
        put_plane(a_ref, v_ref, 1 + 6 * right + i, layers, ref[at + 640 : at + PLANE].astype(F32))
    at = 2 * PLANE
    both = ref[at : at + 320].astype(F32)
    put_plane(a_ref, v_ref, 9 * right, [both, pltpu.roll(both, 64, 1)], ref[at + 320 : at + HALF].astype(F32))


def load_masks(at, parts, k_ref):
    for by, k in enumerate(parts):
        k = k.astype(F32)
        m = jnp.maximum(k, pltpu.roll(k, LANES - 1, 1))
        m = jnp.maximum(m, pltpu.roll(m, LANES - 8, 1))
        m = jnp.maximum(m, pltpu.roll(m, LANES - 64, 1))
        k_ref[0, at, by] = k
        k_ref[1, at, by] = m


def spread(k, index):
    return stacked(*[jnp.take_along_axis(k[8 * i : 8 * i + 8], index, axis=1, mode="promise_in_bounds") for i in range(5)])


def local(i):
    return (i + 1) >> 2, (i + 1) & 3


def silu(v):
    half = 0.5 * v
    return half + half * jnp.tanh(half)


def joined_x(ref, x, cz, lane_a, rows):
    return jnp.where(lane_a, ref[x + 1, cz, rows], ref[x - 1, cz, rows])


def lanes_a(rows):
    return one_where(low_a(rows)) > 0.5


def encode(xi, a_ref, v_ref, k_ref, e_ref, ev_ref, c_ref, d_ref, o_ref, we_ref, be, wn_ref, gain, shift):
    z8 = depth_of(320)
    first, last = z8 == 0, z8 == ZC - 1
    lane = iota((8, LANES), 1)
    lane_at = 8 * (lane >> 6) + ((lane >> 5) & 1)
    la = lanes_a(320)
    every = slice(0, 320)
    lhs = [a_ref[xi, cz] for cz in BITS] + [joined_x(a_ref, xi, cz, la, every) for cz in BITS]
    lhs += [v_ref[xi, cz] for cz in BITS] + [joined_x(v_ref, xi, cz, la, every) for cz in BITS]
    o = nn(beside(*lhs), we_ref[...])
    bx, lx = local(xi)
    expanded = [[], []]
    on = []
    for yi in range(1, 9):
        by, ly = local(yi)
        k = k_ref[0, bx, by]
        for cz in BITS:
            expanded[cz].append(spread(k, lane_at + (64 * cz + 2 * ly + 16 * lx)))
        on.append(spread(k_ref[1, bx, by], lane * 0 + (2 * ly + 16 * lx)))
    on = stacked(*on)
    pre = (
        o[:, 0:128] + moved(o[:, 256:384], 1, first) + be,
        o[:, 128:256] + moved(o[:, 384:512], -1, last) + be,
    )
    enc = []
    for cz in BITS:
        e = jnp.where(stacked(*expanded[cz]) > 0.5, silu(pre[cz]), 0.0)
        enc.append(e.astype(BF16))
        e_ref[xi - 1, cz] = enc[cz]
        ev_ref[xi - 1, cz] = jnp.where(low_b(160), e[120:280], e[40:200]).astype(BF16)
    lifted = nt(beside(*enc), wn_ref[...])
    c = jnp.where(on > 0.5, silu(lifted * gain + shift), 0.0)
    c_ref[xi - 1] = c.astype(BF16)
    d_ref[xi - 1] = c[40:280].astype(BF16)
    o_ref[xi - 1] = on[40:280]


def coarse(xo, c_ref, d_ref, o_ref, u_ref, wc_ref, bc, wu_ref):
    z6 = depth_of(240)
    first, last = z6 == 0, z6 == ZC - 1
    lhs, rhs = [], []
    for dx in range(3):
        for dy in range(3):
            lhs.append(d_ref[xo + dx] if dy == 1 else c_ref[xo + dx, 40 * dy : 40 * dy + 240])
            rhs.append(wc_ref[9 * dx + 3 * dy : 9 * dx + 3 * dy + 3].reshape(384, 128))
    p = nt(beside(*lhs), beside(*rhs))
    s = p[:, 128:256] + moved(p[:, 0:128], 1, first) + moved(p[:, 256:384], -1, last) + bc
    act = jnp.where(o_ref[xo + 1] > 0.5, silu(s), 0.0).astype(BF16)
    u = nt(act, stacked(*([wu_ref[...]] * 4)))
    u_ref[xo, 0] = u[40:200].astype(BF16)
    u_ref[xo, 1] = jnp.where(low_b(160), u[80:240], u[0:160]).astype(BF16)


def decode(xo, e_ref, ev_ref, u_ref, wd_ref, bd, perm, back, m_ref, out_ref, at):
    z4 = depth_of(160)
    first, last = z4 == 0, z4 == ZC - 1
    la = lanes_a(160)
    mid, every = slice(80, 240), slice(0, 160)
    x = xo + 2
    lhs = [e_ref[x, cz, mid] for cz in BITS] + [joined_x(e_ref, x, cz, la, mid) for cz in BITS]
    lhs += [ev_ref[x, cz] for cz in BITS] + [joined_x(ev_ref, x, cz, la, every) for cz in BITS]
    x = xo + 1
    for v in BITS:
        lhs += [u_ref[x, v], joined_x(u_ref, x, v, la, every)]
    o = nn(beside(*lhs), wd_ref[...])
    d0 = o[:, 0:128] + moved(o[:, 256:384], 1, first) + bd
    d1 = o[:, 128:256] + moved(o[:, 384:512], -1, last) + bd
    d = [beside(*[v[ZC * y : ZC * y + ZC] for y in range(4)]) for v in (d0, d1)]
    d = stacked(*d, jnp.zeros((LANES - Z, 512), F32)).astype(BF16)
    d = nn(nn(back, d).astype(BF16), perm)
    d = stacked(d, jnp.zeros((LANES - Z, 512), F32))
    for a in BITS:
        t = jnp.transpose(d[:, 256 * a : 256 * a + 256])[:, :Z].reshape(CH, 8, Z)
        out_ref[:, at + a] = jnp.where(m_ref[2 * xo + a][None] > 0, t, 0.0).astype(BF16)


def own_kernel(own_ref, low_ref, high_ref, we_ref, be_ref, wn_ref, gain_ref, shift_ref, *state):
    a_ref, v_ref, k_ref, e_ref, ev_ref, c_ref, d_ref, o_ref, _ = state
    load_own(own_ref, low_ref, high_ref, a_ref, v_ref)
    load_masks(1, (low_ref[SIDE_MASK:SIDE_ROWS], own_ref[OWN : OWN + ZC], high_ref[SIDE_MASK:SIDE_ROWS]), k_ref)
    be = quad(be_ref[...])
    for xi in (4, 5):
        encode(
            xi, a_ref, v_ref, k_ref, e_ref, ev_ref, c_ref, d_ref, o_ref, we_ref, be, wn_ref, gain_ref[...],
            shift_ref[...],
        )


def side_work(right, side_ref, we_ref, be_ref, wn_ref, gain_ref, shift_ref, wc_ref, bc_ref, wu_ref, state):
    a_ref, v_ref, k_ref, e_ref, ev_ref, c_ref, d_ref, o_ref, u_ref = state
    load_side(side_ref, right, a_ref, v_ref)
    masks = side_ref[EDGE_MASK:EDGE_ROWS].astype(F32)
    load_masks(2 * right, [masks[ZC * i : ZC * i + ZC] for i in range(3)], k_ref)
    be = quad(be_ref[...])
    for i in range(3):
        encode(
            5 * right + 1 + i, a_ref, v_ref, k_ref, e_ref, ev_ref, c_ref, d_ref, o_ref, we_ref, be, wn_ref,
            gain_ref[...], shift_ref[...],
        )
    for i in range(3):
        coarse(3 * right + i, c_ref, d_ref, o_ref, u_ref, wc_ref, bc_ref[...], wu_ref)


N_STATE = 9


def near_kernel(
    right_ref, side_ref, we_ref, be_ref, wn_ref, gain_ref, shift_ref, wc_ref, bc_ref, wu_ref, m_ref, wd_ref, bd_ref,
    perm_ref, back_ref, *refs
):
    state = refs[N_STATE : 2 * N_STATE]
    out_ref = refs[2 * N_STATE]
    right = right_ref[0]
    side_work(right, side_ref, we_ref, be_ref, wn_ref, gain_ref, shift_ref, wc_ref, bc_ref, wu_ref, state)
    decode(
        3 * right, state[3], state[4], state[8], wd_ref, quad(bd_ref[...]), perm_ref[...], back_ref[...], m_ref, out_ref, 0
    )


def far_kernel(
    right_ref, side_ref, we_ref, be_ref, wn_ref, gain_ref, shift_ref, wc_ref, bc_ref, wu_ref, m_ref, wd_ref, bd_ref,
    perm_ref, back_ref, done_ref, *refs
):
    state = refs[N_STATE : 2 * N_STATE]
    out_hbm = refs[2 * N_STATE]
    out_ref, sems = refs[2 * N_STATE + 1 :]
    right = 1 - right_ref[0]
    copies = [pltpu.make_async_copy(done_ref, out_hbm.at[:, pl.ds(6 * (1 - right), 2)], sems.at[3])]
    copies[0].start()
    side_work(right, side_ref, we_ref, be_ref, wn_ref, gain_ref, shift_ref, wc_ref, bc_ref, wu_ref, state)
    bd = quad(bd_ref[...])
    for i in range(3):
        decode(
            right + i, state[3], state[4], state[8], wd_ref, bd, perm_ref[...], back_ref[...], m_ref, out_ref, 2 * i
        )
        copies.append(
            pltpu.make_async_copy(
                out_ref.at[:, pl.ds(2 * i, 2)], out_hbm.at[:, pl.ds(2 * (right + i), 2)], sems.at[i]
            )
        )
        copies[-1].start()
    for copy in copies:
        copy.wait()


def vmem(n):
    return [pl.BlockSpec(memory_space=pltpu.VMEM)] * n


def hbm(n):
    return [pl.BlockSpec(memory_space=pltpu.HBM)] * n


def call(kernel, outs, ins, out_specs, scratch, mib, flops, aliases=()):
    return pl.pallas_call(
        kernel,
        out_shape=outs,
        in_specs=ins,
        out_specs=out_specs,
        scratch_shapes=scratch,
        input_output_aliases=dict(aliases),
        compiler_params=pltpu.CompilerParams(vmem_limit_bytes=mib << 20),
        cost_estimate=pl.CostEstimate(flops=flops, bytes_accessed=10**6, transcendentals=0),
    )


def array(*shape, kind=BF16):
    return jax.ShapeDtypeStruct(shape, kind)


def buffers(shapes):
    return [pltpu.VMEM(s, d) for s, d in shapes]


def shifted(value, axis, step):
    peers = lax.axis_size(axis)
    return lax.ppermute(value, axis, [(i, i + step) for i in range(peers) if 0 <= i + step < peers])


def swapped(value, axis, first):
    peers = lax.axis_size(axis)
    pairs = []
    for i in range(first, peers - 1, 2):
        pairs += [(i, i + 1), (i + 1, i)]
    return lax.ppermute(value, axis, pairs)


def time_features(timestep, embed_width):
    halves = embed_width // 2
    freqs = jnp.exp(-math.log(10000.0) * jnp.arange(halves, dtype=F32) / halves)
    angles = timestep[0].astype(F32) * freqs
    return jnp.concatenate([jnp.sin(angles), jnp.cos(angles)]).astype(BF16)


SCALAR = [pl.BlockSpec(memory_space=pltpu.SMEM)]
STATE = [
    ((10, 2, 320, LANES), BF16),
    ((10, 2, 320, LANES), BF16),
    ((2, 3, 3, ZC, LANES), F32),
    ((8, 2, 320, LANES), BF16),
    ((8, 2, 160, LANES), BF16),
    ((8, 320, LANES), BF16),
    ((8, 240, LANES), BF16),
    ((8, 240, LANES), F32),
    ((6, 2, 160, LANES), BF16),
]


def on_device(
    fine_in, voxel_mask, timestep, w_enc, b_enc, w_down, w_time, w_coarse, b_coarse, w_up, w_dec, b_dec
):
    own, up, down = call(
        pack_kernel,
        [array(OWN + ZC, LANES), array(SIDE_ROWS, LANES), array(SIDE_ROWS, LANES)],
        hbm(2),
        vmem(3),
        [pltpu.VMEM(fine_in.shape, BF16), pltpu.VMEM(voxel_mask.shape, jnp.int32), pltpu.SemaphoreType.DMA((5,))],
        12,
        10**9,
    )(pltpu.with_memory_space_constraint(fine_in, pltpu.HBM), pltpu.with_memory_space_constraint(voxel_mask, pltpu.HBM))
    low = shifted(up, "wide", 1)
    high = shifted(down, "wide", -1)

    embedded = time_features(timestep, w_time.shape[0])
    film = jnp.dot(embedded[None], w_time, preferred_element_type=F32)
    chans = w_down.shape[0]
    gains = 1.0 + film[:, :chans]
    shifts = film[:, chans:]
    taps = 27 * LANES
    enc_w, dec_w, down_w, perm, back = call(
        weights_kernel,
        [array(1024, 512), array(1536, 512), array(128, 256), array(512, 512), array(Z, LANES)],
        vmem(3),
        vmem(5),
        buffers([((taps, 32), BF16), ((taps, 64), BF16), ((32, taps), F32), ((64, taps), F32)]),
        16,
        4 * 10**9,
    )(w_enc, w_dec, w_down)

    odd = lax.axis_index("narrow").astype(jnp.int32)[None] & 1
    near_right = 1 - odd
    far, near = call(
        mid_kernel,
        [array(EDGE_ROWS, LANES), array(EDGE_ROWS, LANES)],
        SCALAR + vmem(4),
        vmem(2),
        buffers([((2, 4 * ZC, LANES), F32)]),
        8,
        10**8,
    )(odd, own, low, high, down_w)
    far_side = swapped(far, "narrow", 1)
    near_side = swapped(near, "narrow", 0)

    encoder = (enc_w, b_enc[None], down_w, gains, shifts)
    shapes = [array(*shape, kind=kind) for shape, kind in STATE]
    state = call(own_kernel, shapes, vmem(8), vmem(N_STATE), [], 12, 2 * 10**9)(own, low, high, *encoder)
    some = encoder + (w_coarse, b_coarse[None], w_up, voxel_mask, dec_w, b_dec[None], perm, back)
    rows = (fine_in.shape[0], 2) + fine_in.shape[2:]
    *state, done = call(
        near_kernel,
        shapes + [array(*rows)],
        SCALAR + vmem(14 + N_STATE),
        vmem(N_STATE + 1),
        [],
        16,
        4 * 10**9,
        [(15 + i, i) for i in range(N_STATE)],
    )(near_right, near_side, *some, *state)
    return call(
        far_kernel,
        shapes + [array(*fine_in.shape)],
        SCALAR + vmem(15 + N_STATE),
        vmem(N_STATE) + hbm(1),
        [pltpu.VMEM((fine_in.shape[0], 6) + fine_in.shape[2:], BF16), pltpu.SemaphoreType.DMA((4,))],
        16,
        5 * 10**9,
        [(16 + i, i) for i in range(N_STATE)],
    )(near_right, far_side, *some, done, *state)[N_STATE]


def solution(mesh):
    field = P(None, "narrow", "wide", None)
    return jax.shard_map(
        on_device,
        mesh=mesh,
        in_specs=(field, P("narrow", "wide", None)) + (P(),) * 10,
        out_specs=field,
        check_vma=False,
    )
```

```python
import math

import jax
import jax.numpy as jnp
from jax import lax
from jax.experimental import pallas as pl
from jax.experimental.pallas import tpu as pltpu
from jax.sharding import PartitionSpec as P


F32 = jnp.float32
BF16 = jnp.bfloat16
LANES = 128
ZC = 40
Z = 80
CH = 32
BITS = (0, 1)


def nn(a, b):
    return lax.dot_general(a, b, (((1,), (0,)), ((), ())), preferred_element_type=F32)


def nt(a, b):
    return lax.dot_general(a, b, (((1,), (1,)), ((), ())), preferred_element_type=F32)


def iota(shape, dim):
    return lax.broadcasted_iota(jnp.int32, shape, dim)


PAIR = 2 * ZC
OWN = 16 * PAIR
SIDE = 8 * PAIR
SIDE_MASK = SIDE + 4 * ZC
SIDE_ROWS = SIDE_MASK + ZC
PLANE = 9 * PAIR
HALF = 5 * PAIR
EDGE_MASK = 2 * PLANE + HALF
EDGE_ROWS = EDGE_MASK + 3 * ZC


def one_where(truth):
    return truth.astype(F32).astype(BF16)


def unpick(rows, cols):
    row = iota((rows, cols), 0)
    return one_where(jnp.where(row < ZC, 2 * row, 2 * row - (Z - 1)) == iota((rows, cols), 1))


def low_a(rows):
    return iota((rows, LANES), 1) < 64


def low_b(rows):
    return (iota((rows, LANES), 1) & 32) == 0


def stacked(*parts):
    return jnp.concatenate(parts, axis=0)


def beside(*parts):
    return jnp.concatenate(parts, axis=1)


def pack_kernel(x_hbm, m_hbm, own_ref, up_ref, dn_ref, x_ref, m_ref, sems):
    copies = [pltpu.make_async_copy(m_hbm, m_ref, sems.at[4])]
    for cx in range(4):
        copies.append(pltpu.make_async_copy(x_hbm.at[:, pl.ds(2 * cx, 2)], x_ref.at[:, pl.ds(2 * cx, 2)], sems.at[cx]))
    for copy in copies:
        copy.start()
    sel = unpick(Z, Z)
    src = iota((512, LANES), 0)
    y = src & 7
    goal = ((y >> 1) << 7) + ((src >> 8) << 6) + ((y & 1) << 5) + ((src >> 3) & 31) - iota((512, LANES), 1)
    perm = [one_where(goal == LANES * i) for i in range(4)]
    copies[0].wait()
    mask = (m_ref[...] > 0).astype(F32).reshape(64, Z).astype(BF16)
    cols = nt(sel, mask)
    cols = beside(cols[:ZC], cols[ZC:]).astype(BF16)
    own_ref[OWN : OWN + ZC] = cols
    up_ref[SIDE_MASK:SIDE_ROWS] = cols
    dn_ref[SIDE_MASK:SIDE_ROWS] = cols
    sides = [[], []]
    for cx in range(4):
        copies[1 + cx].wait()
        for a in BITS:
            x = 2 * cx + a
            tile = x_ref[:, x].astype(F32)
            tile = jnp.where(m_ref[x][None] > 0, tile, 0.0)
            sides[a].append(nt(sel, tile.reshape(8 * CH, Z).astype(BF16)).astype(BF16))
    both = beside(stacked(*sides[0]), stacked(*sides[1]))
    cols = [nn(both, perm[cy]) for cy in range(4)]
    ups, downs = [], []
    for cx in range(4):
        col = [v[Z * cx : Z * cx + Z] for v in cols]
        for cz in BITS:
            z = slice(ZC * cz, ZC * cz + ZC)
            first = stacked(col[0][z], col[1][z]).astype(BF16)
            second = stacked(col[2][z], col[3][z]).astype(BF16)
            own_ref[pl.ds((4 * cx + 2 * cz) * PAIR, PAIR)] = first
            own_ref[pl.ds((4 * cx + 2 * cz + 1) * PAIR, PAIR)] = second
            dn_ref[pl.ds((2 * cx + cz) * PAIR, PAIR)] = first
            up_ref[pl.ds((2 * cx + cz) * PAIR, PAIR)] = second
        ups.append(jnp.where(low_b(ZC), pltpu.roll(col[1][ZC:], LANES - 32, 1), col[1][:ZC]))
        downs.append(jnp.where(low_b(ZC), col[2][:ZC], pltpu.roll(col[2][ZC:], 32, 1)))
        if cx % 2 == 1:
            at = pl.ds(SIDE + (cx // 2) * PAIR, PAIR)
            up_ref[at] = stacked(*ups[-2:]).astype(BF16)
            dn_ref[at] = stacked(*downs[-2:]).astype(BF16)


def part(x, size):
    return pl.ds(pl.multiple_of(x * size, size), size)


def mid_kernel(odd_ref, own_ref, low_ref, high_ref, tie_ref, tie2_ref, far_ref, near_ref, ends_ref):
    ends_ref[0] = low_ref[SIDE:SIDE_MASK].astype(F32)
    ends_ref[1] = high_ref[SIDE:SIDE_MASK].astype(F32)

    def layer(x, cz):
        return (
            low_ref[pl.ds(pl.multiple_of(x * 2 * PAIR + cz * PAIR, PAIR), PAIR)],
            own_ref[pl.ds(pl.multiple_of(x * 4 * PAIR + 2 * cz * PAIR, PAIR), 2 * PAIR)],
            high_ref[pl.ds(pl.multiple_of(x * 2 * PAIR + cz * PAIR, PAIR), PAIR)],
        )

    def ends(x):
        at = part(x, ZC)
        return stacked(ends_ref[0, at], ends_ref[1, at]).astype(BF16)

    lane_a = iota((PAIR, LANES), 1) >> 6
    for ref, right in ((far_ref, odd_ref[0]), (near_ref, 1 - odd_ref[0])):
        for i in range(2):
            x = 2 * right + i
            for cz in BITS:
                at = i * PLANE + 4 * cz * PAIR
                low, own, high = layer(x, cz)
                ref[at : at + PAIR] = low
                ref[at + PAIR : at + 3 * PAIR] = own
                ref[at + 3 * PAIR : at + 4 * PAIR] = high
            ref[i * PLANE + 8 * PAIR : (i + 1) * PLANE] = ends(x)
        x = 2 - right
        pieces = []
        for cz in BITS:
            low, own, high = layer(x, cz)
            pieces.append([v.astype(F32) for v in (low, own[:PAIR], own[PAIR:], high)])
        for i in range(4):
            v = jnp.where(lane_a == right, pieces[0][i], pltpu.roll(pieces[1][i], 64, 1))
            ref[2 * PLANE + i * PAIR : 2 * PLANE + (i + 1) * PAIR] = v.astype(BF16)
        ref[2 * PLANE + 4 * PAIR : EDGE_MASK] = ends(x)
        masks = [low_ref[SIDE_MASK:SIDE_ROWS], own_ref[OWN : OWN + ZC], high_ref[SIDE_MASK:SIDE_ROWS]]
        ref[EDGE_MASK:EDGE_ROWS] = stacked(*[m.astype(F32) for m in masks]).astype(BF16)


def tap_of(out_bit, in_bit, far):
    if far:
        return 2 * (1 - in_bit) if out_bit != in_bit else None
    return in_bit - out_bit + 1


def placed(w_ref, rows, taps, group):
    total = jnp.zeros((CH, LANES), F32)
    for g, tap in enumerate(taps):
        if tap is not None:
            total = jnp.where(group == g, w_ref[rows : rows + CH, LANES * tap : LANES * tap + LANES], total)
    return total


def block(w_ref, rows, group, far_x, far_y, a_in, b_in, cz_in, shifted, cz_out):
    if shifted:
        tz = None
        if cz_out == 0 and cz_in == 1:
            tz = 0
        if cz_out == 1 and cz_in == 0:
            tz = 2
    else:
        tz = cz_in - cz_out + 1
    taps = []
    for a_out in BITS:
        for b_out in BITS:
            tx = tap_of(a_out, a_in, far_x)
            ty = tap_of(b_out, b_in, far_y)
            taps.append(None if tx is None or ty is None or tz is None else 9 * tx + 3 * ty + tz)
    return placed(w_ref, rows, taps, group)


KINDS = ((0, 0), (1, 0), (0, 1), (1, 1))


def weights_kernel(
    we_ref, wd_ref, wn_ref, wc_ref, oe_ref, od_ref, on_ref, op_ref, ob_ref, oc_ref, re_ref, rd_ref, te_ref, td_ref
):
    for tap in range(27):
        for g in range(4):
            at = LANES * tap + CH * g
            re_ref[at : at + CH] = we_ref[tap]
            rd_ref[at : at + CH] = wd_ref[tap]
    one = (iota((CH, CH), 0) == iota((CH, CH), 1)).astype(F32).astype(BF16)
    te_ref[...] = nt(one, re_ref[...])
    one = (iota((2 * CH, 2 * CH), 0) == iota((2 * CH, 2 * CH), 1)).astype(F32).astype(BF16)
    td_ref[...] = nt(one, rd_ref[...])
    one = one_where(iota((LANES, LANES), 0) == iota((LANES, LANES), 1))
    for i in range(9):
        oc_ref[LANES * i : LANES * i + LANES] = nt(one, wc_ref[3 * i : 3 * i + 3].reshape(384, LANES)).astype(BF16)
    group = iota((CH, LANES), 1) >> 5
    for w_ref, o_ref in ((te_ref, oe_ref), (td_ref, od_ref)):
        for t, (fx, fy) in enumerate(KINDS):
            for cz in BITS:
                for a in BITS:
                    for b in BITS:
                        base = 256 * t + 128 * cz + 64 * a + 32 * b
                        for s in BITS:
                            for co in BITS:
                                v = block(w_ref, 0, group, fx, fy, a, b, cz, s, co)
                                o_ref[base : base + CH, 256 * s + 128 * co : 256 * s + 128 * co + LANES] = v.astype(BF16)
    for t, (fx, fy) in enumerate(KINDS):
        for a in BITS:
            for b in BITS:
                base = 1024 + 128 * t + 64 * a + 32 * b
                for s in BITS:
                    for co in BITS:
                        v = block(td_ref, CH, group, fx, fy, a, b, 0, s, co)
                        v = v + block(td_ref, CH, group, fx, fy, a, b, 1, s, co)
                        od_ref[base : base + CH, 256 * s + 128 * co : 256 * s + 128 * co + LANES] = v.astype(BF16)
    k = iota((8 * CH, LANES), 0)
    goal = (((k >> 5) & 1) << 7) + ((k >> 6) << 5) + (k & 31) - iota((8 * CH, LANES), 1)
    perm = jnp.concatenate([(goal == LANES * i).astype(F32).astype(BF16) for i in BITS], axis=1)
    on_ref[...] = nn(wn_ref[...], perm).astype(BF16)
    src = iota((512, LANES), 0)
    goal = (((src >> 6) & 1) << 8) + ((src & 31) << 3) + ((src >> 7) << 1) + ((src >> 5) & 1) - iota((512, LANES), 1)
    op_ref[...] = beside(*[one_where(goal == LANES * i) for i in range(4)])
    column = iota((Z, LANES), 1)
    goal = jnp.where(column < ZC, 2 * column, jnp.where(column < Z, 2 * column - (Z - 1), -1))
    ob_ref[...] = one_where(goal == iota((Z, LANES), 0))


def moved(t, amount, edge):
    rows = t.shape[0]
    return jnp.where(edge, 0.0, pltpu.roll(t, amount % rows, 0))


def depth_of(rows):
    return iota((rows, LANES), 0) % ZC


def quad(bias):
    return beside(bias, bias, bias, bias)


def put_plane(a_ref, v_ref, at, layers, ends):
    y0, y9 = ends[:ZC].astype(F32), ends[ZC:].astype(F32)
    for cz in BITS:
        a_ref[at, cz] = layers[cz].astype(BF16)
        f = layers[cz].astype(F32)
        if cz == 1:
            y0, y9 = pltpu.roll(y0, 32, 1), pltpu.roll(y9, LANES - 32, 1)
        f = stacked(y0, f, y9)
        v_ref[at, cz] = jnp.where(low_b(320), f[PAIR:], f[:320]).astype(BF16)


def load_own(own_ref, low_ref, high_ref, a_ref, v_ref):
    low_ends = low_ref[SIDE:SIDE_MASK].astype(F32)
    high_ends = high_ref[SIDE:SIDE_MASK].astype(F32)
    for x in range(4):
        layers = []
        for cz in BITS:
            at = (2 * x + cz) * PAIR
            mine = (4 * x + 2 * cz) * PAIR
            layers.append(
                stacked(low_ref[at : at + PAIR], own_ref[mine : mine + 2 * PAIR], high_ref[at : at + PAIR])
            )
        z = slice(ZC * x, ZC * x + ZC)
        put_plane(a_ref, v_ref, x, layers, stacked(low_ends[z], high_ends[z]))


def load_side(ref, right, a_ref, v_ref):
    for i in range(2):
        at = i * PLANE
        layers = [ref[at + 320 * cz : at + 320 * cz + 320] for cz in BITS]
        put_plane(a_ref, v_ref, 1 + 6 * right + i, layers, ref[at + 640 : at + PLANE].astype(F32))
    at = 2 * PLANE
    both = ref[at : at + 320].astype(F32)
    put_plane(a_ref, v_ref, 9 * right, [both, pltpu.roll(both, 64, 1)], ref[at + 320 : at + HALF].astype(F32))


def load_masks(at, parts, k_ref):
    for by, k in enumerate(parts):
        k = k.astype(F32)
        m = jnp.maximum(k, pltpu.roll(k, LANES - 1, 1))
        m = jnp.maximum(m, pltpu.roll(m, LANES - 8, 1))
        m = jnp.maximum(m, pltpu.roll(m, LANES - 64, 1))
        k_ref[0, at, by] = k
        k_ref[1, at, by] = m


def spread(k, index):
    return stacked(*[jnp.take_along_axis(k[8 * i : 8 * i + 8], index, axis=1, mode="promise_in_bounds") for i in range(5)])


def local(i):
    return (i + 1) >> 2, (i + 1) & 3


def silu(v):
    half = 0.5 * v
    return half + half * jnp.tanh(half)


def joined_x(ref, x, cz, lane_a, rows):
    return jnp.where(lane_a, ref[x + 1, cz, rows], ref[x - 1, cz, rows])


def lanes_a(rows):
    return one_where(low_a(rows)) > 0.5


def encode(xi, ai, ei, a_ref, v_ref, k_ref, e_ref, ev_ref, c_ref, d_ref, o_ref, we_ref, be, wn_ref, gain, shift):
    z8 = depth_of(320)
    first, last = z8 == 0, z8 == ZC - 1
    lane = iota((8, LANES), 1)
    lane_at = 8 * (lane >> 6) + ((lane >> 5) & 1)
    la = lanes_a(320)
    every = slice(0, 320)
    lhs = [a_ref[ai, cz] for cz in BITS] + [joined_x(a_ref, ai, cz, la, every) for cz in BITS]
    lhs += [v_ref[ai, cz] for cz in BITS] + [joined_x(v_ref, ai, cz, la, every) for cz in BITS]
    o = nn(beside(*lhs), we_ref[...])
    bx, lx = local(xi)
    expanded = [[], []]
    on = []
    for yi in range(1, 9):
        by, ly = local(yi)
        k = k_ref[0, bx, by]
        for cz in BITS:
            expanded[cz].append(spread(k, lane_at + (64 * cz + 2 * ly + 16 * lx)))
        on.append(spread(k_ref[1, bx, by], lane * 0 + (2 * ly + 16 * lx)))
    on = stacked(*on)
    pre = (
        o[:, 0:128] + moved(o[:, 256:384], 1, first) + be,
        o[:, 128:256] + moved(o[:, 384:512], -1, last) + be,
    )
    enc = []
    for cz in BITS:
        e = jnp.where(stacked(*expanded[cz]) > 0.5, silu(pre[cz]), 0.0)
        enc.append(e.astype(BF16))
        e_ref[ei, cz] = enc[cz]
        ev_ref[ei, cz] = jnp.where(low_b(160), e[120:280], e[40:200]).astype(BF16)
    lifted = nt(beside(*enc), wn_ref[...])
    c = jnp.where(on > 0.5, silu(lifted * gain + shift), 0.0)
    c_ref[ei] = c.astype(BF16)
    d_ref[ei] = c[40:280].astype(BF16)
    o_ref[ei] = on[40:280]


def coarse(xo, c_ref, d_ref, o_ref, u_ref, wc_ref, bc, wu_ref):
    z6 = depth_of(240)
    first, last = z6 == 0, z6 == ZC - 1
    lhs = []
    for dx in range(3):
        lhs += [c_ref[xo + dx, 0:240], d_ref[xo + dx], c_ref[xo + dx, 80:320]]
    p = nn(beside(*lhs), wc_ref[...])
    s = p[:, 128:256] + moved(p[:, 0:128], 1, first) + moved(p[:, 256:384], -1, last) + bc
    act = jnp.where(o_ref[xo + 1] > 0.5, silu(s), 0.0).astype(BF16)
    u = nt(act, stacked(*([wu_ref[...]] * 4)))
    u_ref[xo, 0] = u[40:200].astype(BF16)
    u_ref[xo, 1] = jnp.where(low_b(160), u[80:240], u[0:160]).astype(BF16)


def decode(xo, e_ref, ev_ref, u_ref, wd_ref, bd, perm, back, m_ref, out_ref, at):
    z4 = depth_of(160)
    first, last = z4 == 0, z4 == ZC - 1
    la = lanes_a(160)
    mid, every = slice(80, 240), slice(0, 160)
    x = xo + 2
    lhs = [e_ref[x, cz, mid] for cz in BITS] + [joined_x(e_ref, x, cz, la, mid) for cz in BITS]
    lhs += [ev_ref[x, cz] for cz in BITS] + [joined_x(ev_ref, x, cz, la, every) for cz in BITS]
    x = xo + 1
    for v in BITS:
        lhs += [u_ref[x, v], joined_x(u_ref, x, v, la, every)]
    o = nn(beside(*lhs), wd_ref[...])
    d0 = o[:, 0:128] + moved(o[:, 256:384], 1, first) + bd
    d1 = o[:, 128:256] + moved(o[:, 384:512], -1, last) + bd
    d = [beside(*[v[ZC * y : ZC * y + ZC] for y in range(4)]) for v in (d0, d1)]
    d = stacked(*d, jnp.zeros((LANES - Z, 512), F32)).astype(BF16)
    d = nn(nn(back, d).astype(BF16), perm)
    d = stacked(d, jnp.zeros((LANES - Z, 512), F32))
    for a in BITS:
        t = jnp.transpose(d[:, 256 * a : 256 * a + 256])[:, :Z].reshape(CH, 8, Z)
        out_ref[:, at + a] = jnp.where(m_ref[2 * xo + a][None] > 0, t, 0.0).astype(BF16)


def own_kernel(
    own_ref, low_ref, high_ref, we_ref, be_ref, wn_ref, gain_ref, shift_ref, a_ref, v_ref, e_ref, ev_ref, c_ref, d_ref,
    o_ref, k_ref
):
    load_own(own_ref, low_ref, high_ref, a_ref, v_ref)
    load_masks(1, (low_ref[SIDE_MASK:SIDE_ROWS], own_ref[OWN : OWN + ZC], high_ref[SIDE_MASK:SIDE_ROWS]), k_ref)
    be = quad(be_ref[...])
    for i in range(2):
        encode(
            4 + i, 1 + i, i, a_ref, v_ref, k_ref, e_ref, ev_ref, c_ref, d_ref, o_ref, we_ref, be, wn_ref,
            gain_ref[...], shift_ref[...],
        )


def side_work(right, side_ref, weights, own, scratch):
    we_ref, be_ref, wn_ref, gain_ref, shift_ref, wc_ref, bc_ref, wu_ref = weights
    a_ref, v_ref, e_ref, ev_ref, c_ref, d_ref, o_ref, k_ref, u_ref = scratch
    for i in range(2):
        for ref, given in zip((a_ref, v_ref), own[0:2]):
            ref[3 + 2 * right + i] = given[2 * right + i]
        for ref, given in zip((e_ref, ev_ref, c_ref, d_ref, o_ref), own[2:7]):
            ref[3 + i] = given[i]
        k_ref[i, 1] = own[7][i, 1]
    load_side(side_ref, right, a_ref, v_ref)
    masks = side_ref[EDGE_MASK:EDGE_ROWS].astype(F32)
    load_masks(2 * right, [masks[ZC * i : ZC * i + ZC] for i in range(3)], k_ref)
    be = quad(be_ref[...])
    for i in range(3):
        xi = 5 * right + 1 + i
        encode(
            xi, xi, xi - 1, a_ref, v_ref, k_ref, e_ref, ev_ref, c_ref, d_ref, o_ref, we_ref, be, wn_ref,
            gain_ref[...], shift_ref[...],
        )
    for i in range(3):
        coarse(3 * right + i, c_ref, d_ref, o_ref, u_ref, wc_ref, bc_ref[...], wu_ref)


def near_kernel(right_ref, side_ref, *refs):
    weights, (m_ref, wd_ref, bd_ref, perm_ref, back_ref), own = refs[:8], refs[8:13], refs[13:21]
    done_ref, e1_ref, ev1_ref, u1_ref = refs[21:25]
    scratch = refs[25:]
    right = right_ref[0]
    side_work(right, side_ref, weights, own, scratch)
    e_ref, ev_ref, u_ref = scratch[2], scratch[3], scratch[8]
    decode(
        3 * right, e_ref, ev_ref, u_ref, wd_ref, quad(bd_ref[...]), perm_ref[...], back_ref[...], m_ref, done_ref, 0
    )
    e1_ref[...] = e_ref[2 + 3 * right]
    ev1_ref[...] = ev_ref[2 + 3 * right]
    for i in range(2):
        u1_ref[i] = u_ref[1 + 2 * right + i]


def far_kernel(right_ref, side_ref, *refs):
    weights, (m_ref, wd_ref, bd_ref, perm_ref, back_ref), own = refs[:8], refs[8:13], refs[13:21]
    done_ref, e1_ref, ev1_ref, u1_ref, out_hbm = refs[21:26]
    scratch = refs[26:35]
    out_ref, sems = refs[35:]
    left = right_ref[0]
    right = 1 - left
    copies = [pltpu.make_async_copy(done_ref, out_hbm.at[:, pl.ds(6 * left, 2)], sems.at[3])]
    copies[0].start()
    side_work(right, side_ref, weights, own, scratch)
    e_ref, ev_ref, u_ref = scratch[2], scratch[3], scratch[8]
    e_ref[2 + 3 * left] = e1_ref[...]
    ev_ref[2 + 3 * left] = ev1_ref[...]
    for i in range(2):
        u_ref[1 + 2 * left + i] = u1_ref[i]
    bd = quad(bd_ref[...])
    for i in range(3):
        decode(right + i, e_ref, ev_ref, u_ref, wd_ref, bd, perm_ref[...], back_ref[...], m_ref, out_ref, 2 * i)
        copies.append(
            pltpu.make_async_copy(
                out_ref.at[:, pl.ds(2 * i, 2)], out_hbm.at[:, pl.ds(2 * (right + i), 2)], sems.at[i]
            )
        )
        copies[-1].start()
    for copy in copies:
        copy.wait()


def vmem(n):
    return [pl.BlockSpec(memory_space=pltpu.VMEM)] * n


def hbm(n):
    return [pl.BlockSpec(memory_space=pltpu.HBM)] * n


def call(kernel, outs, ins, out_specs, scratch, mib, flops):
    return pl.pallas_call(
        kernel,
        out_shape=outs,
        in_specs=ins,
        out_specs=out_specs,
        scratch_shapes=scratch,
        compiler_params=pltpu.CompilerParams(vmem_limit_bytes=mib << 20),
        cost_estimate=pl.CostEstimate(flops=flops, bytes_accessed=10**6, transcendentals=0),
    )


def array(*shape, kind=BF16):
    return jax.ShapeDtypeStruct(shape, kind)


def buffers(shapes):
    return [pltpu.VMEM(s, d) for s, d in shapes]


def shifted(value, axis, step):
    peers = lax.axis_size(axis)
    return lax.ppermute(value, axis, [(i, i + step) for i in range(peers) if 0 <= i + step < peers])


def swapped(value, axis, first):
    peers = lax.axis_size(axis)
    pairs = []
    for i in range(first, peers - 1, 2):
        pairs += [(i, i + 1), (i + 1, i)]
    return lax.ppermute(value, axis, pairs)


def time_features(timestep, embed_width):
    halves = embed_width // 2
    freqs = jnp.exp(-math.log(10000.0) * jnp.arange(halves, dtype=F32) / halves)
    angles = timestep[0].astype(F32) * freqs
    return jnp.concatenate([jnp.sin(angles), jnp.cos(angles)]).astype(BF16)


SCALAR = [pl.BlockSpec(memory_space=pltpu.SMEM)]


def state(own, planes):
    masks = (2, 3, 3, ZC, LANES)
    return [
        ((own, 2, 320, LANES), BF16),
        ((own, 2, 320, LANES), BF16),
        ((planes, 2, 320, LANES), BF16),
        ((planes, 2, 160, LANES), BF16),
        ((planes, 320, LANES), BF16),
        ((planes, 240, LANES), BF16),
        ((planes, 240, LANES), F32),
        (masks, F32),
    ]


LIFTED = (6, 2, 160, LANES)


def on_device(
    fine_in, voxel_mask, timestep, w_enc, b_enc, w_down, w_time, w_coarse, b_coarse, w_up, w_dec, b_dec
):
    own, up, down = call(
        pack_kernel,
        [array(OWN + ZC, LANES), array(SIDE_ROWS, LANES), array(SIDE_ROWS, LANES)],
        hbm(2),
        vmem(3),
        [pltpu.VMEM(fine_in.shape, BF16), pltpu.VMEM(voxel_mask.shape, jnp.int32), pltpu.SemaphoreType.DMA((5,))],
        12,
        10**9,
    )(pltpu.with_memory_space_constraint(fine_in, pltpu.HBM), pltpu.with_memory_space_constraint(voxel_mask, pltpu.HBM))
    low = shifted(up, "wide", 1)
    high = shifted(down, "wide", -1)

    embedded = time_features(timestep, w_time.shape[0])
    film = jnp.dot(embedded[None], w_time, preferred_element_type=F32)
    chans = w_down.shape[0]
    gains = 1.0 + film[:, :chans]
    shifts = film[:, chans:]
    taps = 27 * LANES
    enc_w, dec_w, down_w, perm, back, coarse_w = call(
        weights_kernel,
        [array(1024, 512), array(1536, 512), array(128, 256), array(512, 512), array(Z, LANES)]
        + [array(9 * LANES, 384)],
        vmem(4),
        vmem(6),
        buffers([((taps, 32), BF16), ((taps, 64), BF16), ((32, taps), F32), ((64, taps), F32)]),
        16,
        4 * 10**9,
    )(w_enc, w_dec, w_down, w_coarse)

    odd = lax.axis_index("narrow").astype(jnp.int32)[None] & 1
    near_right = 1 - odd
    far, near = call(
        mid_kernel,
        [array(EDGE_ROWS, LANES), array(EDGE_ROWS, LANES)],
        SCALAR + vmem(5),
        vmem(2),
        buffers([((2, 4 * ZC, LANES), F32)]),
        8,
        10**8,
    )(odd, own, low, high, down_w, gains)
    far_side = swapped(far, "narrow", 1)
    near_side = swapped(near, "narrow", 0)

    encoder = (enc_w, b_enc[None], down_w, gains, shifts)
    mine = call(
        own_kernel, [array(*d, kind=k) for d, k in state(4, 2)], vmem(8), vmem(8), [], 12, 2 * 10**9
    )(own, low, high, *encoder)
    some = encoder + (coarse_w, b_coarse[None], w_up, voxel_mask, dec_w, b_dec[None], perm, back) + tuple(mine)
    scratch = buffers(state(10, 8) + [(LIFTED, BF16)])
    pair = (fine_in.shape[0], 2) + fine_in.shape[2:]
    done = call(
        near_kernel,
        [array(*pair), array(2, 320, LANES), array(2, 160, LANES), array(2, 2, 160, LANES)],
        SCALAR + vmem(22),
        vmem(4),
        scratch,
        24,
        4 * 10**9,
    )(near_right, near_side, *some)
    rest = (fine_in.shape[0], 6) + fine_in.shape[2:]
    return call(
        far_kernel,
        [array(*fine_in.shape)],
        SCALAR + vmem(26),
        hbm(1),
        scratch + [pltpu.VMEM(rest, BF16), pltpu.SemaphoreType.DMA((4,))],
        24,
        5 * 10**9,
    )(near_right, far_side, *some, *done)[0]


def solution(mesh):
    field = P(None, "narrow", "wide", None)
    return jax.shard_map(
        on_device,
        mesh=mesh,
        in_specs=(field, P("narrow", "wide", None)) + (P(),) * 10,
        out_specs=field,
        check_vma=False,
    )
```

```python
import math

import jax
import jax.numpy as jnp
from jax import lax
from jax.experimental import pallas as pl
from jax.experimental.pallas import tpu as pltpu
from jax.sharding import PartitionSpec as P


F32 = jnp.float32
BF16 = jnp.bfloat16
LANES = 128
ZC = 40
Z = 80
CH = 32
BITS = (0, 1)


def nn(a, b):
    return lax.dot_general(a, b, (((1,), (0,)), ((), ())), preferred_element_type=F32)


def nt(a, b):
    return lax.dot_general(a, b, (((1,), (1,)), ((), ())), preferred_element_type=F32)


def iota(shape, dim):
    return lax.broadcasted_iota(jnp.int32, shape, dim)


PAIR = 2 * ZC
OWN = 16 * PAIR
SIDE = 8 * PAIR
SIDE_MASK = SIDE + 4 * ZC
SIDE_ROWS = SIDE_MASK + ZC
PLANE = 9 * PAIR
HALF = 5 * PAIR
EDGE_MASK = 2 * PLANE + HALF
EDGE_ROWS = EDGE_MASK + 3 * ZC


def one_where(truth):
    return truth.astype(F32).astype(BF16)


def unpick(rows, cols):
    row = iota((rows, cols), 0)
    return one_where(jnp.where(row < ZC, 2 * row, 2 * row - (Z - 1)) == iota((rows, cols), 1))


def low_b(rows):
    return (iota((rows, LANES), 1) & 32) == 0


def stacked(*parts):
    return jnp.concatenate(parts, axis=0)


def beside(*parts):
    return jnp.concatenate(parts, axis=1)


def pack_kernel(x_hbm, m_hbm, own_ref, up_ref, dn_ref, x_ref, m_ref, sems):
    copies = [pltpu.make_async_copy(m_hbm, m_ref, sems.at[4])]
    for cx in range(4):
        copies.append(pltpu.make_async_copy(x_hbm.at[:, pl.ds(2 * cx, 2)], x_ref.at[:, pl.ds(2 * cx, 2)], sems.at[cx]))
    for copy in copies:
        copy.start()
    sel = unpick(Z, Z)
    src = iota((512, LANES), 0)
    y = src & 7
    goal = ((y >> 1) << 7) + ((src >> 8) << 6) + ((y & 1) << 5) + ((src >> 3) & 31) - iota((512, LANES), 1)
    perm = [one_where(goal == LANES * i) for i in range(4)]
    copies[0].wait()
    mask = (m_ref[...] > 0).astype(F32).reshape(64, Z).astype(BF16)
    cols = nt(sel, mask)
    cols = beside(cols[:ZC], cols[ZC:]).astype(BF16)
    own_ref[OWN : OWN + ZC] = cols
    up_ref[SIDE_MASK:SIDE_ROWS] = cols
    dn_ref[SIDE_MASK:SIDE_ROWS] = cols
    sides = [[], []]
    for cx in range(4):
        copies[1 + cx].wait()
        for a in BITS:
            x = 2 * cx + a
            tile = x_ref[:, x].astype(F32)
            tile = jnp.where(m_ref[x][None] > 0, tile, 0.0)
            sides[a].append(nt(sel, tile.reshape(8 * CH, Z).astype(BF16)).astype(BF16))
    both = beside(stacked(*sides[0]), stacked(*sides[1]))
    cols = [nn(both, perm[cy]) for cy in range(4)]
    ups, downs = [], []
    for cx in range(4):
        col = [v[Z * cx : Z * cx + Z] for v in cols]
        for cz in BITS:
            z = slice(ZC * cz, ZC * cz + ZC)
            first = stacked(col[0][z], col[1][z]).astype(BF16)
            second = stacked(col[2][z], col[3][z]).astype(BF16)
            own_ref[pl.ds((4 * cx + 2 * cz) * PAIR, PAIR)] = first
            own_ref[pl.ds((4 * cx + 2 * cz + 1) * PAIR, PAIR)] = second
            dn_ref[pl.ds((2 * cx + cz) * PAIR, PAIR)] = first
            up_ref[pl.ds((2 * cx + cz) * PAIR, PAIR)] = second
        ups.append(jnp.where(low_b(ZC), pltpu.roll(col[1][ZC:], LANES - 32, 1), col[1][:ZC]))
        downs.append(jnp.where(low_b(ZC), col[2][:ZC], pltpu.roll(col[2][ZC:], 32, 1)))
        if cx % 2 == 1:
            at = pl.ds(SIDE + (cx // 2) * PAIR, PAIR)
            up_ref[at] = stacked(*ups[-2:]).astype(BF16)
            dn_ref[at] = stacked(*downs[-2:]).astype(BF16)


def part(x, size):
    return pl.ds(pl.multiple_of(x * size, size), size)


def mid_kernel(odd_ref, own_ref, low_ref, high_ref, tie_ref, tie2_ref, far_ref, near_ref, ends_ref):
    ends_ref[0] = low_ref[SIDE:SIDE_MASK].astype(F32)
    ends_ref[1] = high_ref[SIDE:SIDE_MASK].astype(F32)

    def layer(x, cz):
        return (
            low_ref[pl.ds(pl.multiple_of(x * 2 * PAIR + cz * PAIR, PAIR), PAIR)],
            own_ref[pl.ds(pl.multiple_of(x * 4 * PAIR + 2 * cz * PAIR, PAIR), 2 * PAIR)],
            high_ref[pl.ds(pl.multiple_of(x * 2 * PAIR + cz * PAIR, PAIR), PAIR)],
        )

    def ends(x):
        at = part(x, ZC)
        return stacked(ends_ref[0, at], ends_ref[1, at]).astype(BF16)

    lane_a = iota((PAIR, LANES), 1) >> 6
    for ref, right in ((far_ref, odd_ref[0]), (near_ref, 1 - odd_ref[0])):
        for i in range(2):
            x = 3 * right + i * (1 - 2 * right)
            for cz in BITS:
                at = i * PLANE + 4 * cz * PAIR
                low, own, high = layer(x, cz)
                ref[at : at + PAIR] = low
                ref[at + PAIR : at + 3 * PAIR] = own
                ref[at + 3 * PAIR : at + 4 * PAIR] = high
            ref[i * PLANE + 8 * PAIR : (i + 1) * PLANE] = ends(x)
        x = 2 - right
        pieces = []
        for cz in BITS:
            low, own, high = layer(x, cz)
            pieces.append([v.astype(F32) for v in (low, own[:PAIR], own[PAIR:], high)])
        for i in range(4):
            v = jnp.where(lane_a == right, pieces[0][i], pltpu.roll(pieces[1][i], 64, 1))
            ref[2 * PLANE + i * PAIR : 2 * PLANE + (i + 1) * PAIR] = v.astype(BF16)
        ref[2 * PLANE + 4 * PAIR : EDGE_MASK] = ends(x)
        masks = [low_ref[SIDE_MASK:SIDE_ROWS], own_ref[OWN : OWN + ZC], high_ref[SIDE_MASK:SIDE_ROWS]]
        ref[EDGE_MASK:EDGE_ROWS] = stacked(*[m.astype(F32) for m in masks]).astype(BF16)


def tap_of(out_bit, in_bit, far):
    if far:
        return 2 * (1 - in_bit) if out_bit != in_bit else None
    return in_bit - out_bit + 1


def placed(w_ref, rows, taps, group):
    total = jnp.zeros((CH, LANES), F32)
    for g, tap in enumerate(taps):
        if tap is not None:
            total = jnp.where(group == g, w_ref[rows : rows + CH, LANES * tap : LANES * tap + LANES], total)
    return total


def block(w_ref, rows, group, far_x, far_y, a_in, b_in, cz_in, shifted, cz_out):
    if shifted:
        tz = None
        if cz_out == 0 and cz_in == 1:
            tz = 0
        if cz_out == 1 and cz_in == 0:
            tz = 2
    else:
        tz = cz_in - cz_out + 1
    taps = []
    for a_out in BITS:
        for b_out in BITS:
            tx = tap_of(a_out, a_in, far_x)
            ty = tap_of(b_out, b_in, far_y)
            taps.append(None if tx is None or ty is None or tz is None else 9 * tx + 3 * ty + tz)
    return placed(w_ref, rows, taps, group)


KINDS = ((0, 0), (1, 0), (0, 1), (1, 1))


def weights_kernel(
    we_ref, wd_ref, wn_ref, wc_ref, oe_ref, od_ref, on_ref, op_ref, ob_ref, oc_ref, re_ref, rd_ref, te_ref, td_ref
):
    for tap in range(27):
        for g in range(4):
            at = LANES * tap + CH * g
            re_ref[at : at + CH] = we_ref[tap]
            rd_ref[at : at + CH] = wd_ref[tap]
    one = (iota((CH, CH), 0) == iota((CH, CH), 1)).astype(F32).astype(BF16)
    te_ref[...] = nt(one, re_ref[...])
    one = (iota((2 * CH, 2 * CH), 0) == iota((2 * CH, 2 * CH), 1)).astype(F32).astype(BF16)
    td_ref[...] = nt(one, rd_ref[...])
    one = one_where(iota((LANES, LANES), 0) == iota((LANES, LANES), 1))
    for i in range(9):
        oc_ref[LANES * i : LANES * i + LANES] = nt(one, wc_ref[3 * i : 3 * i + 3].reshape(384, LANES)).astype(BF16)
    group = iota((CH, LANES), 1) >> 5
    for w_ref, o_ref in ((te_ref, oe_ref), (td_ref, od_ref)):
        for t, (fx, fy) in enumerate(KINDS):
            for cz in BITS:
                for a in BITS:
                    for b in BITS:
                        base = 256 * t + 128 * cz + 64 * a + 32 * b
                        for s in BITS:
                            for co in BITS:
                                v = block(w_ref, 0, group, fx, fy, a, b, cz, s, co)
                                o_ref[base : base + CH, 256 * s + 128 * co : 256 * s + 128 * co + LANES] = v.astype(BF16)
    for t, (fx, fy) in enumerate(KINDS):
        for a in BITS:
            for b in BITS:
                base = 1024 + 128 * t + 64 * a + 32 * b
                for s in BITS:
                    for co in BITS:
                        v = block(td_ref, CH, group, fx, fy, a, b, 0, s, co)
                        v = v + block(td_ref, CH, group, fx, fy, a, b, 1, s, co)
                        od_ref[base : base + CH, 256 * s + 128 * co : 256 * s + 128 * co + LANES] = v.astype(BF16)
    k = iota((8 * CH, LANES), 0)
    goal = (((k >> 5) & 1) << 7) + ((k >> 6) << 5) + (k & 31) - iota((8 * CH, LANES), 1)
    perm = jnp.concatenate([(goal == LANES * i).astype(F32).astype(BF16) for i in BITS], axis=1)
    on_ref[...] = nn(wn_ref[...], perm).astype(BF16)
    src = iota((512, LANES), 0)
    goal = (((src >> 6) & 1) << 8) + ((src & 31) << 3) + ((src >> 7) << 1) + ((src >> 5) & 1) - iota((512, LANES), 1)
    op_ref[...] = beside(*[one_where(goal == LANES * i) for i in range(4)])
    column = iota((Z, LANES), 1)
    goal = jnp.where(column < ZC, 2 * column, jnp.where(column < Z, 2 * column - (Z - 1), -1))
    ob_ref[...] = one_where(goal == iota((Z, LANES), 0))


def moved(t, amount, edge):
    rows = t.shape[0]
    return jnp.where(edge, 0.0, pltpu.roll(t, amount % rows, 0))


def depth_of(rows):
    return iota((rows, LANES), 0) % ZC


def quad(bias):
    return beside(bias, bias, bias, bias)


def put_plane(a_ref, v_ref, at, layers, ends):
    y0, y9 = ends[:ZC].astype(F32), ends[ZC:].astype(F32)
    for cz in BITS:
        a_ref[at, cz] = layers[cz].astype(BF16)
        f = layers[cz].astype(F32)
        if cz == 1:
            y0, y9 = pltpu.roll(y0, 32, 1), pltpu.roll(y9, LANES - 32, 1)
        f = stacked(y0, f, y9)
        v_ref[at, cz] = jnp.where(low_b(320), f[PAIR:], f[:320]).astype(BF16)


def load_own(own_ref, low_ref, high_ref, a_ref, v_ref):
    low_ends = low_ref[SIDE:SIDE_MASK].astype(F32)
    high_ends = high_ref[SIDE:SIDE_MASK].astype(F32)
    for x in range(4):
        layers = []
        for cz in BITS:
            at = (2 * x + cz) * PAIR
            mine = (4 * x + 2 * cz) * PAIR
            layers.append(
                stacked(low_ref[at : at + PAIR], own_ref[mine : mine + 2 * PAIR], high_ref[at : at + PAIR])
            )
        z = slice(ZC * x, ZC * x + ZC)
        put_plane(a_ref, v_ref, x, layers, stacked(low_ends[z], high_ends[z]))


def load_side(ref, a_ref, v_ref):
    for i in range(2):
        at = i * PLANE
        layers = [ref[at + 320 * cz : at + 320 * cz + 320] for cz in BITS]
        put_plane(a_ref, v_ref, 2 + i, layers, ref[at + 640 : at + PLANE].astype(F32))
    at = 2 * PLANE
    both = ref[at : at + 320].astype(F32)
    put_plane(a_ref, v_ref, 4, [both, pltpu.roll(both, 64, 1)], ref[at + 320 : at + HALF].astype(F32))


def load_masks(at, parts, k_ref):
    for by, k in enumerate(parts):
        k = k.astype(F32)
        m = jnp.maximum(k, pltpu.roll(k, LANES - 1, 1))
        m = jnp.maximum(m, pltpu.roll(m, LANES - 8, 1))
        m = jnp.maximum(m, pltpu.roll(m, LANES - 64, 1))
        k_ref[0, at, by, 0:ZC] = k
        k_ref[1, at, by, 0:ZC] = m


def spread(k, index):
    return stacked(*[jnp.take_along_axis(k[8 * i : 8 * i + 8], index, axis=1, mode="promise_in_bounds") for i in range(5)])


def silu(v):
    half = 0.5 * v
    return half + half * jnp.tanh(half)


def joined_x(ref, p, part, right, rows):
    count = rows.stop - rows.start
    takes_next = one_where((1 - (iota((count, LANES), 1) >> 6)) == right) > 0.5
    return jnp.where(takes_next, ref[p + 1, part, rows], ref[p - 1, part, rows])


def spans(ref, p, parts, right, rows):
    return [ref[p, part, rows] for part in parts] + [joined_x(ref, p, part, right, rows) for part in parts]


def encode_dot(p, right, a_ref, v_ref, we_ref):
    every = slice(0, 320)
    return nn(beside(*spans(a_ref, p, BITS, right, every), *spans(v_ref, p, BITS, right, every)), we_ref[...])


def encode_finish(o, at, block, lx, k_ref, e_ref, ev_ref, be, wn_ref):
    z8 = depth_of(320)
    first, last = z8 == 0, z8 == ZC - 1
    lane = iota((8, LANES), 1)
    lane_at = 8 * (lane >> 6) + ((lane >> 5) & 1) + 16 * lx
    pre = (
        o[:, 0:128] + moved(o[:, 256:384], 1, first) + be,
        o[:, 128:256] + moved(o[:, 384:512], -1, last) + be,
    )
    enc = []
    for cz in BITS:
        active = []
        for yi in range(1, 9):
            by, ly = (yi + 1) >> 2, (yi + 1) & 3
            active.append(spread(k_ref[0, block, by, 0:ZC], lane_at + (64 * cz + 2 * ly)))
        e = jnp.where(stacked(*active) > 0.5, silu(pre[cz]), 0.0)
        enc.append(e.astype(BF16))
        e_ref[at, cz] = enc[cz]
        ev_ref[at, cz, 0:160] = jnp.where(low_b(160), e[120:280], e[40:200]).astype(BF16)
    return nt(beside(*enc), wn_ref[...])


def strided_finish(lifted, at, block, lx, k_ref, c_ref, d_ref, o_ref, gain, shift):
    where = iota((8, LANES), 1) * 0 + 16 * lx
    on = []
    for yi in range(1, 9):
        by, ly = (yi + 1) >> 2, (yi + 1) & 3
        on.append(spread(k_ref[1, block, by, 0:ZC], where + 2 * ly))
    on = stacked(*on)
    c = jnp.where(on > 0.5, silu(lifted * gain + shift), 0.0)
    c_ref[at] = c.astype(BF16)
    d_ref[at, 0:240] = c[40:280].astype(BF16)
    o_ref[at, 0:240] = on[40:280]


def coarse_dot(q, right, c_ref, d_ref, wc_ref):
    lhs, rhs = [], []
    for i in range(3):
        lhs += [c_ref[q - 1 + i, 0:240], d_ref[q - 1 + i, 0:240], c_ref[q - 1 + i, 80:320]]
        first = 768 * (1 - right) + 384 * i * (2 * right - 1)
        rhs.append(wc_ref[pl.ds(pl.multiple_of(first, 384), 384)])
    return nn(beside(*lhs), stacked(*rhs))


def coarse_finish(p, q, at, o_ref, u_ref, bc, wu_ref):
    z6 = depth_of(240)
    first, last = z6 == 0, z6 == ZC - 1
    s = p[:, 128:256] + moved(p[:, 0:128], 1, first) + moved(p[:, 256:384], -1, last) + bc
    act = jnp.where(o_ref[q, 0:240] > 0.5, silu(s), 0.0).astype(BF16)
    u = nt(act, stacked(*([wu_ref[...]] * 4)))
    u_ref[at, 0, 0:160] = u[40:200].astype(BF16)
    u_ref[at, 1, 0:160] = jnp.where(low_b(160), u[80:240], u[0:160]).astype(BF16)


def decode_dot(p, right, e_ref, ev_ref, u_ref, wd_ref):
    mid, every = slice(80, 240), slice(0, 160)
    lhs = spans(e_ref, p, BITS, right, mid) + spans(ev_ref, p, BITS, right, every)
    for v in BITS:
        lhs += spans(u_ref, p, (v,), right, every)
    return nn(beside(*lhs), wd_ref[...])


def decode_finish(o, xo, bd, perm, back, m_ref, out_ref, at):
    z4 = depth_of(160)
    first, last = z4 == 0, z4 == ZC - 1
    d0 = o[:, 0:128] + moved(o[:, 256:384], 1, first) + bd
    d1 = o[:, 128:256] + moved(o[:, 384:512], -1, last) + bd
    d = [beside(*[v[ZC * y : ZC * y + ZC] for y in range(4)]) for v in (d0, d1)]
    d = stacked(*d, jnp.zeros((LANES - Z, 512), F32)).astype(BF16)
    d = nn(nn(back, d).astype(BF16), perm)
    d = stacked(d, jnp.zeros((LANES - Z, 512), F32))
    for a in BITS:
        t = jnp.transpose(d[:, 256 * a : 256 * a + 256])[:, :Z].reshape(CH, 8, Z)
        out_ref[:, at + a] = jnp.where(m_ref[2 * xo + a][None] > 0, t, 0.0).astype(BF16)


def own_kernel(
    own_ref, low_ref, high_ref, we_ref, be_ref, wn_ref, gain_ref, shift_ref, a_ref, v_ref, e_ref, ev_ref, c_ref, d_ref,
    o_ref, k_ref
):
    load_own(own_ref, low_ref, high_ref, a_ref, v_ref)
    load_masks(1, (low_ref[SIDE_MASK:SIDE_ROWS], own_ref[OWN : OWN + ZC], high_ref[SIDE_MASK:SIDE_ROWS]), k_ref)
    be = quad(be_ref[...])
    dots = [encode_dot(1 + i, 1, a_ref, v_ref, we_ref) for i in range(2)]
    lifted = [encode_finish(dots[i], i, 1, 1 + i, k_ref, e_ref, ev_ref, be, wn_ref) for i in range(2)]
    for i in range(2):
        strided_finish(lifted[i], i, 1, 1 + i, k_ref, c_ref, d_ref, o_ref, gain_ref[...], shift_ref[...])


def side_kernel(right, side_ref, weights, misc, own, scratch, decoded, given, emit):
    we_ref, be_ref, wn_ref, gain_ref, shift_ref, wc_ref, bc_ref, wu_ref = weights
    m_ref, wd_ref, bd_ref, perm_ref, back_ref = misc
    a_ref, v_ref, e_ref, ev_ref, c_ref, d_ref, o_ref, k_ref, u_ref = scratch
    for i in range(2):
        at = right * (1 + 2 * i) + 1 - i
        for ref, source in zip((a_ref, v_ref), own[0:2]):
            ref[i] = source[at]
        at = right * (2 * i - 1) + 1 - i
        for ref, source in zip((c_ref, d_ref, o_ref), own[4:7]):
            ref[i] = source[at]
        for ref, source in zip((e_ref, ev_ref), own[2:4]):
            ref[1 + i] = source[at]
        k_ref[i, 1] = own[7][i, 1]
    if given is not None:
        e_ref[0] = given[0][...]
        ev_ref[0] = given[1][...]
        for i in range(2):
            u_ref[i] = given[2][1 - i]
    load_side(side_ref, a_ref, v_ref)
    masks = side_ref[EDGE_MASK:EDGE_ROWS].astype(F32)
    load_masks(0, [masks[ZC * i : ZC * i + ZC] for i in range(3)], k_ref)
    be, bd = quad(be_ref[...]), quad(bd_ref[...])
    gain, shift = gain_ref[...], shift_ref[...]
    perm, back = perm_ref[...], back_ref[...]
    block = (1, 0, 0)
    lx = (3 * right, 3 - 3 * right, 2 - right)

    def e_dot(i):
        return encode_dot(1 + i, right, a_ref, v_ref, we_ref)

    def e_finish(i, dot):
        return encode_finish(dot, 3 + i, block[i], lx[i], k_ref, e_ref, ev_ref, be, wn_ref)

    def s_finish(i, lifted):
        strided_finish(lifted, 2 + i, block[i], lx[i], k_ref, c_ref, d_ref, o_ref, gain, shift)

    def c_dot(i):
        return coarse_dot(1 + i, right, c_ref, d_ref, wc_ref)

    def c_finish(i, dot):
        coarse_finish(dot, 1 + i, 2 + i, o_ref, u_ref, bc_ref[...], wu_ref)

    def d_dot(i):
        return decode_dot(1 + i, right, e_ref, ev_ref, u_ref, wd_ref)

    def d_finish(i, dot):
        emit(i, dot, bd, perm, back, m_ref)

    e0 = e_dot(0)
    e1 = e_dot(1)
    l0 = e_finish(0, e0)
    e2 = e_dot(2)
    s_finish(0, l0)
    l1 = e_finish(1, e1)
    c0 = c_dot(0)
    s_finish(1, l1)
    l2 = e_finish(2, e2)
    c_finish(0, c0)
    c1 = c_dot(1)
    s_finish(2, l2)
    d0 = d_dot(0) if 0 in decoded else None
    c_finish(1, c1)
    c2 = c_dot(2)
    if 0 in decoded:
        d_finish(0, d0)
    d1 = d_dot(1) if 1 in decoded else None
    c_finish(2, c2)
    d2 = d_dot(2)
    if 1 in decoded:
        d_finish(1, d1)
    d_finish(2, d2)


def near_kernel(right_ref, side_ref, *refs):
    done_ref, e1_ref, ev1_ref, u1_ref = refs[21:25]
    scratch = refs[25:]
    right = right_ref[0]

    def emit(i, dot, bd, perm, back, m_ref):
        decode_finish(dot, 3 * right, bd, perm, back, m_ref, done_ref, 0)

    side_kernel(right, side_ref, refs[:8], refs[8:13], refs[13:21], scratch, (2,), None, emit)
    e1_ref[...] = scratch[2][3]
    ev1_ref[...] = scratch[3][3]
    for i in range(2):
        u1_ref[i] = scratch[8][2 + i]


def far_kernel(right_ref, side_ref, *refs):
    done_ref, e1_ref, ev1_ref, u1_ref, out_hbm = refs[21:26]
    scratch = refs[26:35]
    out_ref, sems = refs[35:]
    left = right_ref[0]
    right = 1 - left
    copies = [pltpu.make_async_copy(done_ref, out_hbm.at[:, pl.ds(6 * left, 2)], sems.at[3])]
    copies[0].start()

    def emit(i, dot, bd, perm, back, m_ref):
        xo = right * (2 * i - 1) + 2 - i
        decode_finish(dot, xo, bd, perm, back, m_ref, out_ref, 2 * i)
        copies.append(
            pltpu.make_async_copy(out_ref.at[:, pl.ds(2 * i, 2)], out_hbm.at[:, pl.ds(2 * xo, 2)], sems.at[i])
        )
        copies[-1].start()

    side_kernel(
        right, side_ref, refs[:8], refs[8:13], refs[13:21], scratch, (0, 1, 2), (e1_ref, ev1_ref, u1_ref), emit
    )
    for copy in copies:
        copy.wait()


def vmem(n):
    return [pl.BlockSpec(memory_space=pltpu.VMEM)] * n


def hbm(n):
    return [pl.BlockSpec(memory_space=pltpu.HBM)] * n


def call(kernel, outs, ins, out_specs, scratch, mib, flops):
    return pl.pallas_call(
        kernel,
        out_shape=outs,
        in_specs=ins,
        out_specs=out_specs,
        scratch_shapes=scratch,
        compiler_params=pltpu.CompilerParams(vmem_limit_bytes=mib << 20),
        cost_estimate=pl.CostEstimate(flops=flops, bytes_accessed=10**6, transcendentals=0),
    )


def array(*shape, kind=BF16):
    return jax.ShapeDtypeStruct(shape, kind)


def buffers(shapes):
    return [pltpu.VMEM(s, d) for s, d in shapes]


def shifted(value, axis, step):
    peers = lax.axis_size(axis)
    return lax.ppermute(value, axis, [(i, i + step) for i in range(peers) if 0 <= i + step < peers])


def swapped(value, axis, first):
    peers = lax.axis_size(axis)
    pairs = []
    for i in range(first, peers - 1, 2):
        pairs += [(i, i + 1), (i + 1, i)]
    return lax.ppermute(value, axis, pairs)


def time_features(timestep, embed_width):
    halves = embed_width // 2
    freqs = jnp.exp(-math.log(10000.0) * jnp.arange(halves, dtype=F32) / halves)
    angles = timestep[0].astype(F32) * freqs
    return jnp.concatenate([jnp.sin(angles), jnp.cos(angles)]).astype(BF16)


SCALAR = [pl.BlockSpec(memory_space=pltpu.SMEM)]


def state(own, planes, more):
    masks = (2, 2, 3, 64, LANES)
    return [
        ((own, 2, 320, LANES), BF16),
        ((own, 2, 320, LANES), BF16),
        ((planes + more, 2, 320, LANES), BF16),
        ((planes + more, 2, 192, LANES), BF16),
        ((planes, 320, LANES), BF16),
        ((planes, 256, LANES), BF16),
        ((planes, 256, LANES), F32),
        (masks, F32),
    ]


LIFTED = (5, 2, 192, LANES)


def on_device(
    fine_in, voxel_mask, timestep, w_enc, b_enc, w_down, w_time, w_coarse, b_coarse, w_up, w_dec, b_dec
):
    own, up, down = call(
        pack_kernel,
        [array(OWN + ZC, LANES), array(SIDE_ROWS, LANES), array(SIDE_ROWS, LANES)],
        hbm(2),
        vmem(3),
        [pltpu.VMEM(fine_in.shape, BF16), pltpu.VMEM(voxel_mask.shape, jnp.int32), pltpu.SemaphoreType.DMA((5,))],
        12,
        10**9,
    )(pltpu.with_memory_space_constraint(fine_in, pltpu.HBM), pltpu.with_memory_space_constraint(voxel_mask, pltpu.HBM))
    low = shifted(up, "wide", 1)
    high = shifted(down, "wide", -1)

    embedded = time_features(timestep, w_time.shape[0])
    film = jnp.dot(embedded[None], w_time, preferred_element_type=F32)
    chans = w_down.shape[0]
    gains = 1.0 + film[:, :chans]
    shifts = film[:, chans:]
    taps = 27 * LANES
    enc_w, dec_w, down_w, perm, back, coarse_w = call(
        weights_kernel,
        [array(1024, 512), array(1536, 512), array(128, 256), array(512, 512), array(Z, LANES)]
        + [array(9 * LANES, 384)],
        vmem(4),
        vmem(6),
        buffers([((taps, 32), BF16), ((taps, 64), BF16), ((32, taps), F32), ((64, taps), F32)]),
        16,
        4 * 10**9,
    )(w_enc, w_dec, w_down, w_coarse)

    odd = lax.axis_index("narrow").astype(jnp.int32)[None] & 1
    near_right = 1 - odd
    far, near = call(
        mid_kernel,
        [array(EDGE_ROWS, LANES), array(EDGE_ROWS, LANES)],
        SCALAR + vmem(5),
        vmem(2),
        buffers([((2, 4 * ZC, LANES), F32)]),
        8,
        10**8,
    )(odd, own, low, high, down_w, gains)
    far_side = swapped(far, "narrow", 1)
    near_side = swapped(near, "narrow", 0)

    encoder = (enc_w, b_enc[None], down_w, gains, shifts)
    mine = call(
        own_kernel, [array(*d, kind=k) for d, k in state(4, 2, 0)], vmem(8), vmem(8), [], 12, 2 * 10**9
    )(own, low, high, *encoder)
    some = encoder + (coarse_w, b_coarse[None], w_up, voxel_mask, dec_w, b_dec[None], perm, back) + tuple(mine)
    scratch = buffers(state(5, 5, 1) + [(LIFTED, BF16)])
    pair = (fine_in.shape[0], 2) + fine_in.shape[2:]
    done = call(
        near_kernel,
        [array(*pair), array(2, 320, LANES), array(2, 192, LANES), array(2, 2, 192, LANES)],
        SCALAR + vmem(22),
        vmem(4),
        scratch,
        24,
        4 * 10**9,
    )(near_right, near_side, *some)
    rest = (fine_in.shape[0], 6) + fine_in.shape[2:]
    return call(
        far_kernel,
        [array(*fine_in.shape)],
        SCALAR + vmem(26),
        hbm(1),
        scratch + [pltpu.VMEM(rest, BF16), pltpu.SemaphoreType.DMA((4,))],
        24,
        5 * 10**9,
    )(near_right, far_side, *some, *done)[0]


def solution(mesh):
    field = P(None, "narrow", "wide", None)
    return jax.shard_map(
        on_device,
        mesh=mesh,
        in_specs=(field, P("narrow", "wide", None)) + (P(),) * 10,
        out_specs=field,
        check_vma=False,
    )
```

```python
import math

import jax
import jax.numpy as jnp
from jax import lax
from jax.experimental import pallas as pl
from jax.experimental.pallas import tpu as pltpu
from jax.sharding import PartitionSpec as P


F32 = jnp.float32
BF16 = jnp.bfloat16
LANES = 128
ZC = 40
Z = 80
CH = 32
BITS = (0, 1)


def nn(a, b):
    return lax.dot_general(a, b, (((1,), (0,)), ((), ())), preferred_element_type=F32)


def nt(a, b):
    return lax.dot_general(a, b, (((1,), (1,)), ((), ())), preferred_element_type=F32)


def iota(shape, dim):
    return lax.broadcasted_iota(jnp.int32, shape, dim)


PAIR = 2 * ZC
OWN = 16 * PAIR
SIDE = 8 * PAIR
SIDE_MASK = SIDE + 4 * ZC
SIDE_ROWS = SIDE_MASK + ZC
PLANE = 9 * PAIR
HALF = 5 * PAIR
MASKS = 3 * ZC


def one_where(truth):
    return truth.astype(F32).astype(BF16)


def unpick(rows, cols):
    row = iota((rows, cols), 0)
    return one_where(jnp.where(row < ZC, 2 * row, 2 * row - (Z - 1)) == iota((rows, cols), 1))


def low_b(rows):
    return (iota((rows, LANES), 1) & 32) == 0


def stacked(*parts):
    return jnp.concatenate(parts, axis=0)


def beside(*parts):
    return jnp.concatenate(parts, axis=1)


def pack_kernel(x_hbm, m_hbm, own_ref, up_ref, dn_ref, x_ref, m_ref, sems):
    copies = [pltpu.make_async_copy(m_hbm, m_ref, sems.at[4])]
    for cx in range(4):
        copies.append(pltpu.make_async_copy(x_hbm.at[:, pl.ds(2 * cx, 2)], x_ref.at[:, pl.ds(2 * cx, 2)], sems.at[cx]))
    for copy in copies:
        copy.start()
    sel = unpick(Z, Z)
    src = iota((512, LANES), 0)
    y = src & 7
    goal = ((y >> 1) << 7) + ((src >> 8) << 6) + ((y & 1) << 5) + ((src >> 3) & 31) - iota((512, LANES), 1)
    perm = [one_where(goal == LANES * i) for i in range(4)]
    copies[0].wait()
    mask = (m_ref[...] > 0).astype(F32).reshape(64, Z).astype(BF16)
    cols = nt(sel, mask)
    cols = beside(cols[:ZC], cols[ZC:]).astype(BF16)
    own_ref[OWN : OWN + ZC] = cols
    up_ref[SIDE_MASK:SIDE_ROWS] = cols
    dn_ref[SIDE_MASK:SIDE_ROWS] = cols
    sides = [[], []]
    for cx in range(4):
        copies[1 + cx].wait()
        for a in BITS:
            x = 2 * cx + a
            tile = x_ref[:, x].astype(F32)
            tile = jnp.where(m_ref[x][None] > 0, tile, 0.0)
            sides[a].append(nt(sel, tile.reshape(8 * CH, Z).astype(BF16)).astype(BF16))
    both = beside(stacked(*sides[0]), stacked(*sides[1]))
    cols = [nn(both, perm[cy]) for cy in range(4)]
    ups, downs = [], []
    for cx in range(4):
        col = [v[Z * cx : Z * cx + Z] for v in cols]
        for cz in BITS:
            z = slice(ZC * cz, ZC * cz + ZC)
            first = stacked(col[0][z], col[1][z]).astype(BF16)
            second = stacked(col[2][z], col[3][z]).astype(BF16)
            own_ref[pl.ds((4 * cx + 2 * cz) * PAIR, PAIR)] = first
            own_ref[pl.ds((4 * cx + 2 * cz + 1) * PAIR, PAIR)] = second
            dn_ref[pl.ds((2 * cx + cz) * PAIR, PAIR)] = first
            up_ref[pl.ds((2 * cx + cz) * PAIR, PAIR)] = second
        ups.append(jnp.where(low_b(ZC), pltpu.roll(col[1][ZC:], LANES - 32, 1), col[1][:ZC]))
        downs.append(jnp.where(low_b(ZC), col[2][:ZC], pltpu.roll(col[2][ZC:], 32, 1)))
        if cx % 2 == 1:
            at = pl.ds(SIDE + (cx // 2) * PAIR, PAIR)
            up_ref[at] = stacked(*ups[-2:]).astype(BF16)
            dn_ref[at] = stacked(*downs[-2:]).astype(BF16)


def part(x, size):
    return pl.ds(pl.multiple_of(x * size, size), size)


def mid_kernel(odd_ref, own_ref, low_ref, high_ref, tie_ref, tie2_ref, far_a_ref, far_b_ref, near_ref, ends_ref):
    ends_ref[0] = low_ref[SIDE:SIDE_MASK].astype(F32)
    ends_ref[1] = high_ref[SIDE:SIDE_MASK].astype(F32)

    def layer(x, cz):
        return (
            low_ref[pl.ds(pl.multiple_of(x * 2 * PAIR + cz * PAIR, PAIR), PAIR)],
            own_ref[pl.ds(pl.multiple_of(x * 4 * PAIR + 2 * cz * PAIR, PAIR), 2 * PAIR)],
            high_ref[pl.ds(pl.multiple_of(x * 2 * PAIR + cz * PAIR, PAIR), PAIR)],
        )

    def ends(x):
        at = part(x, ZC)
        return stacked(ends_ref[0, at], ends_ref[1, at]).astype(BF16)

    lane_a = iota((PAIR, LANES), 1) >> 6

    def full(ref, at, x):
        for cz in BITS:
            low, own, high = layer(x, cz)
            ref[at : at + PAIR] = low
            ref[at + PAIR : at + 3 * PAIR] = own
            ref[at + 3 * PAIR : at + 4 * PAIR] = high
            at = at + 4 * PAIR
        ref[at : at + PAIR] = ends(x)

    def half(ref, at, x, right):
        pieces = []
        for cz in BITS:
            low, own, high = layer(x, cz)
            pieces.append([v.astype(F32) for v in (low, own[:PAIR], own[PAIR:], high)])
        for i in range(4):
            v = jnp.where(lane_a == right, pieces[0][i], pltpu.roll(pieces[1][i], 64, 1))
            ref[at + i * PAIR : at + (i + 1) * PAIR] = v.astype(BF16)
        ref[at + 4 * PAIR : at + HALF] = ends(x)

    def masks(ref, at):
        parts = [low_ref[SIDE_MASK:SIDE_ROWS], own_ref[OWN : OWN + ZC], high_ref[SIDE_MASK:SIDE_ROWS]]
        ref[at : at + MASKS] = stacked(*[m.astype(F32) for m in parts]).astype(BF16)

    for (a_ref, a_at), (b_ref, b_at), (m_ref, m_at), right in (
        ((far_a_ref, 0), (far_b_ref, 0), (far_a_ref, PLANE), odd_ref[0]),
        ((near_ref, 0), (near_ref, PLANE), (near_ref, 2 * PLANE + HALF), 1 - odd_ref[0]),
    ):
        full(a_ref, a_at, 3 * right)
        full(b_ref, b_at, 1 + right)
        half(b_ref, b_at + PLANE, 2 - right, right)
        masks(m_ref, m_at)


def tap_of(out_bit, in_bit, far):
    if far:
        return 2 * (1 - in_bit) if out_bit != in_bit else None
    return in_bit - out_bit + 1


def placed(w_ref, rows, taps, group):
    total = jnp.zeros((CH, LANES), F32)
    for g, tap in enumerate(taps):
        if tap is not None:
            total = jnp.where(group == g, w_ref[rows : rows + CH, LANES * tap : LANES * tap + LANES], total)
    return total


def block(w_ref, rows, group, far_x, far_y, a_in, b_in, cz_in, shifted, cz_out):
    if shifted:
        tz = None
        if cz_out == 0 and cz_in == 1:
            tz = 0
        if cz_out == 1 and cz_in == 0:
            tz = 2
    else:
        tz = cz_in - cz_out + 1
    taps = []
    for a_out in BITS:
        for b_out in BITS:
            tx = tap_of(a_out, a_in, far_x)
            ty = tap_of(b_out, b_in, far_y)
            taps.append(None if tx is None or ty is None or tz is None else 9 * tx + 3 * ty + tz)
    return placed(w_ref, rows, taps, group)


KINDS = ((0, 0), (1, 0), (0, 1), (1, 1))


def weights_kernel(
    we_ref, wd_ref, wn_ref, wc_ref, oe_ref, od_ref, on_ref, op_ref, ob_ref, oc_ref, re_ref, rd_ref, te_ref, td_ref
):
    for tap in range(27):
        for g in range(4):
            at = LANES * tap + CH * g
            re_ref[at : at + CH] = we_ref[tap]
            rd_ref[at : at + CH] = wd_ref[tap]
    one = (iota((CH, CH), 0) == iota((CH, CH), 1)).astype(F32).astype(BF16)
    te_ref[...] = nt(one, re_ref[...])
    one = (iota((2 * CH, 2 * CH), 0) == iota((2 * CH, 2 * CH), 1)).astype(F32).astype(BF16)
    td_ref[...] = nt(one, rd_ref[...])
    one = one_where(iota((LANES, LANES), 0) == iota((LANES, LANES), 1))
    for i in range(9):
        oc_ref[LANES * i : LANES * i + LANES] = nt(one, wc_ref[3 * i : 3 * i + 3].reshape(384, LANES)).astype(BF16)
    group = iota((CH, LANES), 1) >> 5
    for w_ref, o_ref in ((te_ref, oe_ref), (td_ref, od_ref)):
        for t, (fx, fy) in enumerate(KINDS):
            for cz in BITS:
                for a in BITS:
                    for b in BITS:
                        base = 256 * t + 128 * cz + 64 * a + 32 * b
                        for s in BITS:
                            for co in BITS:
                                v = block(w_ref, 0, group, fx, fy, a, b, cz, s, co)
                                o_ref[base : base + CH, 256 * s + 128 * co : 256 * s + 128 * co + LANES] = v.astype(BF16)
    for t, (fx, fy) in enumerate(KINDS):
        for a in BITS:
            for b in BITS:
                base = 1024 + 128 * t + 64 * a + 32 * b
                for s in BITS:
                    for co in BITS:
                        v = block(td_ref, CH, group, fx, fy, a, b, 0, s, co)
                        v = v + block(td_ref, CH, group, fx, fy, a, b, 1, s, co)
                        od_ref[base : base + CH, 256 * s + 128 * co : 256 * s + 128 * co + LANES] = v.astype(BF16)
    k = iota((8 * CH, LANES), 0)
    goal = (((k >> 5) & 1) << 7) + ((k >> 6) << 5) + (k & 31) - iota((8 * CH, LANES), 1)
    perm = jnp.concatenate([(goal == LANES * i).astype(F32).astype(BF16) for i in BITS], axis=1)
    on_ref[...] = nn(wn_ref[...], perm).astype(BF16)
    src = iota((512, LANES), 0)
    goal = (((src >> 6) & 1) << 8) + ((src & 31) << 3) + ((src >> 7) << 1) + ((src >> 5) & 1) - iota((512, LANES), 1)
    op_ref[...] = beside(*[one_where(goal == LANES * i) for i in range(4)])
    column = iota((Z, LANES), 1)
    goal = jnp.where(column < ZC, 2 * column, jnp.where(column < Z, 2 * column - (Z - 1), -1))
    ob_ref[...] = one_where(goal == iota((Z, LANES), 0))


def moved(t, amount, edge):
    rows = t.shape[0]
    return jnp.where(edge, 0.0, pltpu.roll(t, amount % rows, 0))


def depth_of(rows):
    return iota((rows, LANES), 0) % ZC


def quad(bias):
    return beside(bias, bias, bias, bias)


def put_plane(a_ref, v_ref, layers, ends):
    y0, y9 = ends[:ZC].astype(F32), ends[ZC:].astype(F32)
    for cz in BITS:
        a_ref[cz] = layers[cz].astype(BF16)
        f = layers[cz].astype(F32)
        if cz == 1:
            y0, y9 = pltpu.roll(y0, 32, 1), pltpu.roll(y9, LANES - 32, 1)
        f = stacked(y0, f, y9)
        v_ref[cz] = jnp.where(low_b(320), f[PAIR:], f[:320]).astype(BF16)


def load_own(own_ref, low_ref, high_ref, a_ref, v_ref):
    low_ends = low_ref[SIDE:SIDE_MASK].astype(F32)
    high_ends = high_ref[SIDE:SIDE_MASK].astype(F32)
    for x in range(4):
        layers = []
        for cz in BITS:
            at = (2 * x + cz) * PAIR
            mine = (4 * x + 2 * cz) * PAIR
            layers.append(
                stacked(low_ref[at : at + PAIR], own_ref[mine : mine + 2 * PAIR], high_ref[at : at + PAIR])
            )
        z = slice(ZC * x, ZC * x + ZC)
        put_plane(a_ref.at[x], v_ref.at[x], layers, stacked(low_ends[z], high_ends[z]))


def load_full(ref, at, a_ref, v_ref):
    layers = [ref[at + 320 * cz : at + 320 * cz + 320] for cz in BITS]
    put_plane(a_ref, v_ref, layers, ref[at + 640 : at + PLANE].astype(F32))


def load_half(ref, at, a_ref, v_ref):
    both = ref[at : at + 320].astype(F32)
    put_plane(a_ref, v_ref, [both, pltpu.roll(both, 64, 1)], ref[at + 320 : at + HALF].astype(F32))


def load_masks(parts, k_ref):
    for by, k in enumerate(parts):
        k = k.astype(F32)
        m = jnp.maximum(k, pltpu.roll(k, LANES - 1, 1))
        m = jnp.maximum(m, pltpu.roll(m, LANES - 8, 1))
        m = jnp.maximum(m, pltpu.roll(m, LANES - 64, 1))
        k_ref[0, by, 0:ZC] = k
        k_ref[1, by, 0:ZC] = m


def load_side_masks(ref, at, k_ref):
    masks = ref[at : at + MASKS].astype(F32)
    load_masks([masks[ZC * i : ZC * i + ZC] for i in range(3)], k_ref)


def spread(k, index):
    return stacked(*[jnp.take_along_axis(k[8 * i : 8 * i + 8], index, axis=1, mode="promise_in_bounds") for i in range(5)])


def silu(v):
    half = 0.5 * v
    return half + half * jnp.tanh(half)


def joined_x(planes, p, part, right, rows):
    count = rows.stop - rows.start
    takes_next = one_where((1 - (iota((count, LANES), 1) >> 6)) == right) > 0.5
    return jnp.where(takes_next, planes[p + 1][part, rows], planes[p - 1][part, rows])


def spans(planes, p, parts, right, rows):
    return [planes[p][part, rows] for part in parts] + [joined_x(planes, p, part, right, rows) for part in parts]


def encode_dot(p, right, a, v, we_ref):
    every = slice(0, 320)
    return nn(beside(*spans(a, p, BITS, right, every), *spans(v, p, BITS, right, every)), we_ref[...])


def encode_finish(o, lx, k_ref, e_ref, ev_ref, be, wn_ref):
    z8 = depth_of(320)
    first, last = z8 == 0, z8 == ZC - 1
    lane = iota((8, LANES), 1)
    lane_at = 8 * (lane >> 6) + ((lane >> 5) & 1) + 16 * lx
    pre = (
        o[:, 0:128] + moved(o[:, 256:384], 1, first) + be,
        o[:, 128:256] + moved(o[:, 384:512], -1, last) + be,
    )
    enc = []
    for cz in BITS:
        active = []
        for yi in range(1, 9):
            by, ly = (yi + 1) >> 2, (yi + 1) & 3
            active.append(spread(k_ref[0, by, 0:ZC], lane_at + (64 * cz + 2 * ly)))
        e = jnp.where(stacked(*active) > 0.5, silu(pre[cz]), 0.0)
        enc.append(e.astype(BF16))
        if e_ref is None:
            continue
        e_ref[cz] = enc[cz]
        ev_ref[cz, 0:160] = jnp.where(low_b(160), e[120:280], e[40:200]).astype(BF16)
    return nt(beside(*enc), wn_ref[...])


def strided_finish(lifted, lx, k_ref, c_ref, d_ref, o_ref, gain, shift):
    where = iota((8, LANES), 1) * 0 + 16 * lx
    on = []
    for yi in range(1, 9):
        by, ly = (yi + 1) >> 2, (yi + 1) & 3
        on.append(spread(k_ref[1, by, 0:ZC], where + 2 * ly))
    on = stacked(*on)
    c = jnp.where(on > 0.5, silu(lifted * gain + shift), 0.0)
    c_ref[...] = c.astype(BF16)
    d_ref[0:240] = c[40:280].astype(BF16)
    o_ref[0:240] = on[40:280]


def coarse_dot(q, right, c, d, wc_ref):
    lhs, rhs = [], []
    for i in range(3):
        lhs += [c[q - 1 + i][0:240], d[q - 1 + i][0:240], c[q - 1 + i][80:320]]
        first = 768 * (1 - right) + 384 * i * (2 * right - 1)
        rhs.append(wc_ref[pl.ds(pl.multiple_of(first, 384), 384)])
    return nn(beside(*lhs), stacked(*rhs))


def coarse_finish(p, o_ref, u_ref, bc, wu_ref):
    z6 = depth_of(240)
    first, last = z6 == 0, z6 == ZC - 1
    s = p[:, 128:256] + moved(p[:, 0:128], 1, first) + moved(p[:, 256:384], -1, last) + bc
    act = jnp.where(o_ref[0:240] > 0.5, silu(s), 0.0).astype(BF16)
    u = nt(act, stacked(*([wu_ref[...]] * 4)))
    u_ref[0, 0:160] = u[40:200].astype(BF16)
    u_ref[1, 0:160] = jnp.where(low_b(160), u[80:240], u[0:160]).astype(BF16)


def decode_dot(p, right, e, ev, u, wd_ref):
    mid, every = slice(80, 240), slice(0, 160)
    lhs = spans(e, p, BITS, right, mid) + spans(ev, p, BITS, right, every)
    for v in BITS:
        lhs += spans(u, p, (v,), right, every)
    return nn(beside(*lhs), wd_ref[...])


def decode_finish(o, xo, bd, perm, back, m_ref, out_ref, at):
    z4 = depth_of(160)
    first, last = z4 == 0, z4 == ZC - 1
    d0 = o[:, 0:128] + moved(o[:, 256:384], 1, first) + bd
    d1 = o[:, 128:256] + moved(o[:, 384:512], -1, last) + bd
    d = [beside(*[v[ZC * y : ZC * y + ZC] for y in range(4)]) for v in (d0, d1)]
    d = stacked(*d, jnp.zeros((LANES - Z, 512), F32)).astype(BF16)
    d = nn(nn(back, d).astype(BF16), perm)
    d = stacked(d, jnp.zeros((LANES - Z, 512), F32))
    for a in BITS:
        t = jnp.transpose(d[:, 256 * a : 256 * a + 256])[:, :Z].reshape(CH, 8, Z)
        out_ref[:, at + a] = jnp.where(m_ref[2 * xo + a][None] > 0, t, 0.0).astype(BF16)


def own_kernel(
    own_ref, low_ref, high_ref, we_ref, be_ref, wn_ref, gain_ref, shift_ref, a_ref, v_ref, e_ref, ev_ref, c_ref, d_ref,
    o_ref, k_ref
):
    load_own(own_ref, low_ref, high_ref, a_ref, v_ref)
    load_masks((low_ref[SIDE_MASK:SIDE_ROWS], own_ref[OWN : OWN + ZC], high_ref[SIDE_MASK:SIDE_ROWS]), k_ref)
    be = quad(be_ref[...])
    a, v = ([ref.at[x] for x in range(4)] for ref in (a_ref, v_ref))
    dots = [encode_dot(1 + i, 1, a, v, we_ref) for i in range(2)]
    lifted = [encode_finish(dots[i], 1 + i, k_ref, e_ref.at[i], ev_ref.at[i], be, wn_ref) for i in range(2)]
    for i in range(2):
        strided_finish(
            lifted[i], 1 + i, k_ref, c_ref.at[i], d_ref.at[i], o_ref.at[i], gain_ref[...], shift_ref[...]
        )


def own_planes(right, own):
    two = [right * (1 + 2 * i) + 1 - i for i in range(2)]
    one = [right * (2 * i - 1) + 1 - i for i in range(2)]
    a, v = ([ref.at[at] for at in two] for ref in own[0:2])
    e, ev, c, d, o = ([ref.at[at] for at in one] for ref in own[2:7])
    return a, v, e, ev, c, d, o


class Stages:
    def __init__(self, right, weights, misc, planes, side_k, own_k, emit):
        self.right, self.planes, self.emit = right, planes, emit
        self.we, be, self.wn, gain, shift, self.wc, bc, self.wu = weights
        self.m, self.wd, bd, perm, back = misc
        self.be, self.bd = quad(be[...]), quad(bd[...])
        self.gain, self.shift, self.bc = gain[...], shift[...], bc[...]
        self.perm, self.back = perm[...], back[...]
        self.k = (own_k, side_k, side_k)
        self.lx = (3 * right, 3 - 3 * right, 2 - right)

    def e_dot(self, i):
        return encode_dot(1 + i, self.right, self.planes[0], self.planes[1], self.we)

    def e_finish(self, i, dot):
        e, ev = self.planes[2], self.planes[3]
        at = (e[3 + i], ev[3 + i]) if i < 2 else (None, None)
        return encode_finish(dot, self.lx[i], self.k[i], *at, self.be, self.wn)

    def s_finish(self, i, lifted):
        c, d, o = self.planes[4:7]
        strided_finish(lifted, self.lx[i], self.k[i], c[2 + i], d[2 + i], o[2 + i], self.gain, self.shift)

    def c_dot(self, i):
        return coarse_dot(1 + i, self.right, self.planes[4], self.planes[5], self.wc)

    def c_finish(self, i, dot):
        coarse_finish(dot, self.planes[6][1 + i], self.planes[7][2 + i], self.bc, self.wu)

    def d_dot(self, i):
        return decode_dot(1 + i, self.right, self.planes[2], self.planes[3], self.planes[7], self.wd)

    def d_finish(self, i, dot):
        self.emit(i, dot, self.bd, self.perm, self.back, self.m)


def near_kernel(right_ref, side_ref, *refs):
    weights, misc, own = refs[:8], refs[8:13], refs[13:21]
    done_ref, e1_ref, ev1_ref, u1_ref = refs[21:25]
    a_ref, v_ref, e_ref, ev_ref, c_ref, d_ref, o_ref, k_ref, u_ref = refs[25:]
    right = right_ref[0]
    a, v, e, ev, c, d, o = own_planes(right, own)
    a, v, c, d, o = (x + [r.at[i] for i in range(3)] for x, r in zip((a, v, c, d, o), (a_ref, v_ref, c_ref, d_ref, o_ref)))
    e, ev = [None] + e + [e1_ref, e_ref.at[0]], [None] + ev + [ev1_ref, ev_ref.at[0]]
    u = [None, None, u1_ref.at[0], u1_ref.at[1], u_ref.at[0]]
    for i in range(2):
        load_full(side_ref, i * PLANE, a[2 + i], v[2 + i])
    load_half(side_ref, 2 * PLANE, a[4], v[4])
    load_side_masks(side_ref, 2 * PLANE + HALF, k_ref)

    def emit(i, dot, bd, perm, back, m_ref):
        decode_finish(dot, 3 * right, bd, perm, back, m_ref, done_ref, 0)

    w = Stages(right, weights, misc, (a, v, e, ev, c, d, o, u), k_ref, own[7], emit)
    e0 = w.e_dot(0)
    e1 = w.e_dot(1)
    l0 = w.e_finish(0, e0)
    e2 = w.e_dot(2)
    w.s_finish(0, l0)
    l1 = w.e_finish(1, e1)
    c0 = w.c_dot(0)
    w.s_finish(1, l1)
    l2 = w.e_finish(2, e2)
    w.c_finish(0, c0)
    c1 = w.c_dot(1)
    w.s_finish(2, l2)
    w.c_finish(1, c1)
    c2 = w.c_dot(2)
    w.c_finish(2, c2)
    w.d_finish(2, w.d_dot(2))


def far_place(right, i):
    return right * (2 * i - 1) + 2 - i


def first_kernel(right_ref, side_ref, *refs):
    weights, misc, own = refs[:8], refs[8:13], refs[13:21]
    e1_ref, ev1_ref, u1_ref = refs[21:24]
    done_ref, a_ref, v_ref, e_ref, ev_ref, c_ref, d_ref, o_ref, k_ref, u_ref = refs[24:]
    right = 1 - right_ref[0]
    a, v, e, ev, c, d, o = own_planes(right, own)
    a, v, c, d, o = (x + [r] for x, r in zip((a, v, c, d, o), (a_ref, v_ref, c_ref, d_ref, o_ref)))
    e, ev = [e1_ref] + e + [e_ref], [ev1_ref] + ev + [ev_ref]
    u = [u1_ref.at[1], u1_ref.at[0], u_ref]
    load_full(side_ref, 0, a[2], v[2])
    load_side_masks(side_ref, PLANE, k_ref)

    def emit(i, dot, bd, perm, back, m_ref):
        decode_finish(dot, far_place(right, i), bd, perm, back, m_ref, done_ref, 0)

    w = Stages(right, weights, misc, (a, v, e, ev, c, d, o, u), k_ref, own[7], emit)
    w.s_finish(0, w.e_finish(0, w.e_dot(0)))
    w.c_finish(0, w.c_dot(0))
    w.d_finish(0, w.d_dot(0))


def last_kernel(right_ref, side_ref, *refs):
    weights, misc, own = refs[:8], refs[8:13], refs[13:21]
    near_done_ref, u1_ref = refs[21:23]
    done_ref, a1_ref, v1_ref, e1_ref, ev1_ref, c1_ref, d1_ref, o1_ref, k_ref, u0_ref = refs[23:33]
    out_hbm = refs[33]
    a_ref, v_ref, e_ref, ev_ref, c_ref, d_ref, o_ref, u_ref, out_ref, sems = refs[34:]
    left = right_ref[0]
    right = 1 - left
    copies = [
        pltpu.make_async_copy(near_done_ref, out_hbm.at[:, pl.ds(6 * left, 2)], sems.at[2]),
        pltpu.make_async_copy(done_ref, out_hbm.at[:, pl.ds(2 * far_place(right, 0), 2)], sems.at[3]),
    ]
    for copy in copies:
        copy.start()
    a, v, e, ev, c, d, o = own_planes(right, own)
    a, v, c, d, o = (
        x + [g] + [r.at[i] for i in range(2)]
        for x, g, r in zip(
            (a, v, c, d, o), (a1_ref, v1_ref, c1_ref, d1_ref, o1_ref), (a_ref, v_ref, c_ref, d_ref, o_ref)
        )
    )
    e, ev = [None] + e + [e1_ref, e_ref], [None] + ev + [ev1_ref, ev_ref]
    u = [None, u1_ref.at[0], u0_ref, u_ref.at[0], u_ref.at[1]]
    load_full(side_ref, 0, a[3], v[3])
    load_half(side_ref, PLANE, a[4], v[4])

    def emit(i, dot, bd, perm, back, m_ref):
        xo = far_place(right, i)
        at = pl.ds(2 * i - 2, 2)
        decode_finish(dot, xo, bd, perm, back, m_ref, out_ref, 2 * i - 2)
        copies.append(pltpu.make_async_copy(out_ref.at[:, at], out_hbm.at[:, pl.ds(2 * xo, 2)], sems.at[i - 1]))
        copies[-1].start()

    w = Stages(right, weights, misc, (a, v, e, ev, c, d, o, u), k_ref, own[7], emit)
    e1 = w.e_dot(1)
    e2 = w.e_dot(2)
    l1 = w.e_finish(1, e1)
    w.s_finish(1, l1)
    c1 = w.c_dot(1)
    l2 = w.e_finish(2, e2)
    w.s_finish(2, l2)
    w.c_finish(1, c1)
    c2 = w.c_dot(2)
    d1 = w.d_dot(1)
    w.c_finish(2, c2)
    w.d_finish(1, d1)
    w.d_finish(2, w.d_dot(2))
    for copy in copies:
        copy.wait()


def vmem(n):
    return [pl.BlockSpec(memory_space=pltpu.VMEM)] * n


def hbm(n):
    return [pl.BlockSpec(memory_space=pltpu.HBM)] * n


def call(kernel, outs, ins, out_specs, scratch, mib, flops):
    return pl.pallas_call(
        kernel,
        out_shape=outs,
        in_specs=ins,
        out_specs=out_specs,
        scratch_shapes=scratch,
        compiler_params=pltpu.CompilerParams(vmem_limit_bytes=mib << 20),
        cost_estimate=pl.CostEstimate(flops=flops, bytes_accessed=10**6, transcendentals=0),
    )


def array(*shape, kind=BF16):
    return jax.ShapeDtypeStruct(shape, kind)


def buffers(shapes):
    return [pltpu.VMEM(s, d) for s, d in shapes]


def shifted(value, axis, step):
    peers = lax.axis_size(axis)
    return lax.ppermute(value, axis, [(i, i + step) for i in range(peers) if 0 <= i + step < peers])


def swapped(value, axis, first):
    peers = lax.axis_size(axis)
    pairs = []
    for i in range(first, peers - 1, 2):
        pairs += [(i, i + 1), (i + 1, i)]
    return lax.ppermute(value, axis, pairs)


def time_features(timestep, embed_width):
    halves = embed_width // 2
    freqs = jnp.exp(-math.log(10000.0) * jnp.arange(halves, dtype=F32) / halves)
    angles = timestep[0].astype(F32) * freqs
    return jnp.concatenate([jnp.sin(angles), jnp.cos(angles)]).astype(BF16)


SCALAR = [pl.BlockSpec(memory_space=pltpu.SMEM)]


def state(own, planes, encoded):
    return [
        (own + (2, 320, LANES), BF16),
        (own + (2, 320, LANES), BF16),
        (encoded + (2, 320, LANES), BF16),
        (encoded + (2, 192, LANES), BF16),
        (planes + (320, LANES), BF16),
        (planes + (256, LANES), BF16),
        (planes + (256, LANES), F32),
        ((2, 3, 64, LANES), F32),
    ]


LIFTED = (2, 192, LANES)


def arrays(shapes):
    return [array(*shape, kind=kind) for shape, kind in shapes]


def on_device(
    fine_in, voxel_mask, timestep, w_enc, b_enc, w_down, w_time, w_coarse, b_coarse, w_up, w_dec, b_dec
):
    own, up, down = call(
        pack_kernel,
        [array(OWN + ZC, LANES), array(SIDE_ROWS, LANES), array(SIDE_ROWS, LANES)],
        hbm(2),
        vmem(3),
        [pltpu.VMEM(fine_in.shape, BF16), pltpu.VMEM(voxel_mask.shape, jnp.int32), pltpu.SemaphoreType.DMA((5,))],
        12,
        10**9,
    )(pltpu.with_memory_space_constraint(fine_in, pltpu.HBM), pltpu.with_memory_space_constraint(voxel_mask, pltpu.HBM))
    low = shifted(up, "wide", 1)
    high = shifted(down, "wide", -1)

    embedded = time_features(timestep, w_time.shape[0])
    film = jnp.dot(embedded[None], w_time, preferred_element_type=F32)
    chans = w_down.shape[0]
    gains = 1.0 + film[:, :chans]
    shifts = film[:, chans:]
    taps = 27 * LANES
    enc_w, dec_w, down_w, perm, back, coarse_w = call(
        weights_kernel,
        [array(1024, 512), array(1536, 512), array(128, 256), array(512, 512), array(Z, LANES)]
        + [array(9 * LANES, 384)],
        vmem(4),
        vmem(6),
        buffers([((taps, 32), BF16), ((taps, 64), BF16), ((32, taps), F32), ((64, taps), F32)]),
        16,
        4 * 10**9,
    )(w_enc, w_dec, w_down, w_coarse)

    odd = lax.axis_index("narrow").astype(jnp.int32)[None] & 1
    near_right = 1 - odd
    far_a, far_b, near = call(
        mid_kernel,
        [array(PLANE + MASKS, LANES), array(PLANE + HALF, LANES), array(2 * PLANE + HALF + MASKS, LANES)],
        SCALAR + vmem(5),
        vmem(3),
        buffers([((2, 4 * ZC, LANES), F32)]),
        8,
        10**8,
    )(odd, own, low, high, down_w, gains)
    far_a = swapped(far_a, "narrow", 1)
    far_b = swapped(far_b, "narrow", 1)
    near = swapped(near, "narrow", 0)

    encoder = (enc_w, b_enc[None], down_w, gains, shifts)
    mine = call(own_kernel, arrays(state((4,), (2,), (2,))), vmem(8), vmem(8), [], 12, 2 * 10**9)(
        own, low, high, *encoder
    )
    some = encoder + (coarse_w, b_coarse[None], w_up, voxel_mask, dec_w, b_dec[None], perm, back) + tuple(mine)
    pair = array(fine_in.shape[0], 2, *fine_in.shape[2:])
    near_done, e1, ev1, u1 = call(
        near_kernel,
        [pair] + arrays(state((), (), ())[2:4] + [((2,) + LIFTED, BF16)]),
        SCALAR + vmem(22),
        vmem(4),
        buffers(state((3,), (3,), (1,)) + [((1,) + LIFTED, BF16)]),
        24,
        4 * 10**9,
    )(near_right, near, *some)
    first = call(
        first_kernel,
        [pair] + arrays(state((), (), ()) + [(LIFTED, BF16)]),
        SCALAR + vmem(25),
        vmem(10),
        [],
        24,
        2 * 10**9,
    )(near_right, far_a, *some, e1, ev1, u1)
    rest = pltpu.VMEM((fine_in.shape[0], 4) + fine_in.shape[2:], BF16)
    return call(
        last_kernel,
        [array(*fine_in.shape)],
        SCALAR + vmem(34),
        hbm(1),
        buffers(state((2,), (2,), ())[:7] + [((2,) + LIFTED, BF16)]) + [rest, pltpu.SemaphoreType.DMA((4,))],
        24,
        4 * 10**9,
    )(near_right, far_b, *some, near_done, u1, *first)[0]


def solution(mesh):
    field = P(None, "narrow", "wide", None)
    return jax.shard_map(
        on_device,
        mesh=mesh,
        in_specs=(field, P("narrow", "wide", None)) + (P(),) * 10,
        out_specs=field,
        check_vma=False,
    )
```

```python
import math

import jax
import jax.numpy as jnp
from jax import lax
from jax.experimental import pallas as pl
from jax.experimental.pallas import tpu as pltpu
from jax.sharding import PartitionSpec as P


F32 = jnp.float32
BF16 = jnp.bfloat16
LANES = 128
ZC = 40
Z = 80
CH = 32
BITS = (0, 1)


def nn(a, b):
    return lax.dot_general(a, b, (((1,), (0,)), ((), ())), preferred_element_type=F32)


def nt(a, b):
    return lax.dot_general(a, b, (((1,), (1,)), ((), ())), preferred_element_type=F32)


def iota(shape, dim):
    return lax.broadcasted_iota(jnp.int32, shape, dim)


PAIR = 2 * ZC
OWN = 16 * PAIR
SIDE = 8 * PAIR
SIDE_MASK = SIDE + 4 * ZC
SIDE_ROWS = SIDE_MASK + ZC
PLANE = 9 * PAIR
HALF = 5 * PAIR
MASKS = 3 * ZC
MIDDLE = 10 * PAIR
FLANKS = 13 * PAIR


def one_where(truth):
    return truth.astype(F32).astype(BF16)


def unpick(rows, cols):
    row = iota((rows, cols), 0)
    return one_where(jnp.where(row < ZC, 2 * row, 2 * row - (Z - 1)) == iota((rows, cols), 1))


def low_b(rows):
    return (iota((rows, LANES), 1) & 32) == 0


def stacked(*parts):
    return jnp.concatenate(parts, axis=0)


def beside(*parts):
    return jnp.concatenate(parts, axis=1)


def pack_kernel(x_hbm, m_hbm, own_ref, up_ref, dn_ref, x_ref, m_ref, sems):
    copies = [pltpu.make_async_copy(m_hbm, m_ref, sems.at[4])]
    for cx in range(4):
        copies.append(pltpu.make_async_copy(x_hbm.at[:, pl.ds(2 * cx, 2)], x_ref.at[:, pl.ds(2 * cx, 2)], sems.at[cx]))
    for copy in copies:
        copy.start()
    sel = unpick(Z, Z)
    src = iota((512, LANES), 0)
    y = src & 7
    goal = ((y >> 1) << 7) + ((src >> 8) << 6) + ((y & 1) << 5) + ((src >> 3) & 31) - iota((512, LANES), 1)
    perm = [one_where(goal == LANES * i) for i in range(4)]
    copies[0].wait()
    mask = (m_ref[...] > 0).astype(F32).reshape(64, Z).astype(BF16)
    cols = nt(sel, mask)
    cols = beside(cols[:ZC], cols[ZC:]).astype(BF16)
    own_ref[OWN : OWN + ZC] = cols
    up_ref[SIDE_MASK:SIDE_ROWS] = cols
    dn_ref[SIDE_MASK:SIDE_ROWS] = cols
    sides = [[], []]
    for cx in range(4):
        copies[1 + cx].wait()
        for a in BITS:
            x = 2 * cx + a
            tile = x_ref[:, x].astype(F32)
            tile = jnp.where(m_ref[x][None] > 0, tile, 0.0)
            sides[a].append(nt(sel, tile.reshape(8 * CH, Z).astype(BF16)).astype(BF16))
    both = beside(stacked(*sides[0]), stacked(*sides[1]))
    cols = [nn(both, perm[cy]) for cy in range(4)]
    ups, downs = [], []
    for cx in range(4):
        col = [v[Z * cx : Z * cx + Z] for v in cols]
        for cz in BITS:
            z = slice(ZC * cz, ZC * cz + ZC)
            first = stacked(col[0][z], col[1][z]).astype(BF16)
            second = stacked(col[2][z], col[3][z]).astype(BF16)
            own_ref[pl.ds((4 * cx + 2 * cz) * PAIR, PAIR)] = first
            own_ref[pl.ds((4 * cx + 2 * cz + 1) * PAIR, PAIR)] = second
            dn_ref[pl.ds((2 * cx + cz) * PAIR, PAIR)] = first
            up_ref[pl.ds((2 * cx + cz) * PAIR, PAIR)] = second
        ups.append(jnp.where(low_b(ZC), pltpu.roll(col[1][ZC:], LANES - 32, 1), col[1][:ZC]))
        downs.append(jnp.where(low_b(ZC), col[2][:ZC], pltpu.roll(col[2][ZC:], 32, 1)))
        if cx % 2 == 1:
            at = pl.ds(SIDE + (cx // 2) * PAIR, PAIR)
            up_ref[at] = stacked(*ups[-2:]).astype(BF16)
            dn_ref[at] = stacked(*downs[-2:]).astype(BF16)


def part(x, size):
    return pl.ds(pl.multiple_of(x * size, size), size)


def folded(pieces, right):
    lane_a = iota(pieces[0].shape, 1) >> 6
    even, odd = (v.astype(F32) for v in pieces)
    return jnp.where(lane_a == right, even, pltpu.roll(odd, 64, 1)).astype(BF16)


def edge_kernel(odd_ref, own_ref, out_ref):
    right = odd_ref[0]
    for i, x in enumerate((3 * right, 1 + right)):
        out_ref[4 * PAIR * i : 4 * PAIR * (i + 1)] = own_ref[part(x, 4 * PAIR)]
    x = 2 - right
    pieces = [own_ref[pl.ds(pl.multiple_of((4 * x + 2 * cz) * PAIR, PAIR), 2 * PAIR)] for cz in BITS]
    out_ref[8 * PAIR : 10 * PAIR] = folded(pieces, right)
    out_ref[MIDDLE : MIDDLE + ZC] = own_ref[OWN : OWN + ZC]


def mid_kernel(odd_ref, own_ref, low_ref, high_ref, tie_ref, tie2_ref, far_ref, near_ref, ends_ref):
    ends_ref[0] = low_ref[SIDE:SIDE_MASK].astype(F32)
    ends_ref[1] = high_ref[SIDE:SIDE_MASK].astype(F32)

    def layer(x, cz):
        return (
            low_ref[pl.ds(pl.multiple_of(x * 2 * PAIR + cz * PAIR, PAIR), PAIR)],
            own_ref[pl.ds(pl.multiple_of(x * 4 * PAIR + 2 * cz * PAIR, PAIR), 2 * PAIR)],
            high_ref[pl.ds(pl.multiple_of(x * 2 * PAIR + cz * PAIR, PAIR), PAIR)],
        )

    def ends(x):
        at = part(x, ZC)
        return stacked(ends_ref[0, at], ends_ref[1, at]).astype(BF16)

    right = 1 - odd_ref[0]
    for i, x in enumerate((3 * right, 1 + right)):
        at = i * PLANE
        for cz in BITS:
            low, own, high = layer(x, cz)
            near_ref[at : at + PAIR] = low
            near_ref[at + PAIR : at + 3 * PAIR] = own
            near_ref[at + 3 * PAIR : at + 4 * PAIR] = high
            at = at + 4 * PAIR
        near_ref[at : at + PAIR] = ends(x)
    x, at = 2 - right, 2 * PLANE
    low, own, high = zip(*[layer(x, cz) for cz in BITS])
    near_ref[at : at + PAIR] = folded(low, right)
    near_ref[at + PAIR : at + 3 * PAIR] = folded(own, right)
    near_ref[at + 3 * PAIR : at + 4 * PAIR] = folded(high, right)
    near_ref[at + 4 * PAIR : at + HALF] = ends(x)
    masks = [low_ref[SIDE_MASK:SIDE_ROWS], own_ref[OWN : OWN + ZC], high_ref[SIDE_MASK:SIDE_ROWS]]
    near_ref[at + HALF : at + HALF + MASKS] = stacked(*[m.astype(F32) for m in masks]).astype(BF16)
    right = odd_ref[0]
    for i, x in enumerate((3 * right, 1 + right)):
        at = 5 * PAIR * i
        far_ref[at : at + 2 * PAIR] = low_ref[part(x, 2 * PAIR)]
        far_ref[at + 2 * PAIR : at + 4 * PAIR] = high_ref[part(x, 2 * PAIR)]
        far_ref[at + 4 * PAIR : at + 5 * PAIR] = ends(x)
    x, at = 2 - right, 10 * PAIR
    low, own, high = zip(*[layer(x, cz) for cz in BITS])
    far_ref[at : at + PAIR] = folded(low, right)
    far_ref[at + PAIR : at + 2 * PAIR] = folded(high, right)
    far_ref[at + 2 * PAIR : at + 3 * PAIR] = ends(x)
    masks = [low_ref[SIDE_MASK:SIDE_ROWS], high_ref[SIDE_MASK:SIDE_ROWS]]
    far_ref[FLANKS : FLANKS + PAIR] = stacked(*[m.astype(F32) for m in masks]).astype(BF16)


def tap_of(out_bit, in_bit, far):
    if far:
        return 2 * (1 - in_bit) if out_bit != in_bit else None
    return in_bit - out_bit + 1


def placed(w_ref, rows, taps, group):
    total = jnp.zeros((CH, LANES), F32)
    for g, tap in enumerate(taps):
        if tap is not None:
            total = jnp.where(group == g, w_ref[rows : rows + CH, LANES * tap : LANES * tap + LANES], total)
    return total


def block(w_ref, rows, group, far_x, far_y, a_in, b_in, cz_in, shifted, cz_out):
    if shifted:
        tz = None
        if cz_out == 0 and cz_in == 1:
            tz = 0
        if cz_out == 1 and cz_in == 0:
            tz = 2
    else:
        tz = cz_in - cz_out + 1
    taps = []
    for a_out in BITS:
        for b_out in BITS:
            tx = tap_of(a_out, a_in, far_x)
            ty = tap_of(b_out, b_in, far_y)
            taps.append(None if tx is None or ty is None or tz is None else 9 * tx + 3 * ty + tz)
    return placed(w_ref, rows, taps, group)


KINDS = ((0, 0), (1, 0), (0, 1), (1, 1))


def weights_kernel(
    we_ref, wd_ref, wn_ref, wc_ref, oe_ref, od_ref, on_ref, op_ref, ob_ref, oc_ref, re_ref, rd_ref, te_ref, td_ref
):
    for tap in range(27):
        for g in range(4):
            at = LANES * tap + CH * g
            re_ref[at : at + CH] = we_ref[tap]
            rd_ref[at : at + CH] = wd_ref[tap]
    one = (iota((CH, CH), 0) == iota((CH, CH), 1)).astype(F32).astype(BF16)
    te_ref[...] = nt(one, re_ref[...])
    one = (iota((2 * CH, 2 * CH), 0) == iota((2 * CH, 2 * CH), 1)).astype(F32).astype(BF16)
    td_ref[...] = nt(one, rd_ref[...])
    one = one_where(iota((LANES, LANES), 0) == iota((LANES, LANES), 1))
    for i in range(9):
        oc_ref[LANES * i : LANES * i + LANES] = nt(one, wc_ref[3 * i : 3 * i + 3].reshape(384, LANES)).astype(BF16)
    group = iota((CH, LANES), 1) >> 5
    for w_ref, o_ref in ((te_ref, oe_ref), (td_ref, od_ref)):
        for t, (fx, fy) in enumerate(KINDS):
            for cz in BITS:
                for a in BITS:
                    for b in BITS:
                        base = 256 * t + 128 * cz + 64 * a + 32 * b
                        for s in BITS:
                            for co in BITS:
                                v = block(w_ref, 0, group, fx, fy, a, b, cz, s, co)
                                o_ref[base : base + CH, 256 * s + 128 * co : 256 * s + 128 * co + LANES] = v.astype(BF16)
    for t, (fx, fy) in enumerate(KINDS):
        for a in BITS:
            for b in BITS:
                base = 1024 + 128 * t + 64 * a + 32 * b
                for s in BITS:
                    for co in BITS:
                        v = block(td_ref, CH, group, fx, fy, a, b, 0, s, co)
                        v = v + block(td_ref, CH, group, fx, fy, a, b, 1, s, co)
                        od_ref[base : base + CH, 256 * s + 128 * co : 256 * s + 128 * co + LANES] = v.astype(BF16)
    k = iota((8 * CH, LANES), 0)
    goal = (((k >> 5) & 1) << 7) + ((k >> 6) << 5) + (k & 31) - iota((8 * CH, LANES), 1)
    perm = jnp.concatenate([(goal == LANES * i).astype(F32).astype(BF16) for i in BITS], axis=1)
    on_ref[...] = nn(wn_ref[...], perm).astype(BF16)
    src = iota((512, LANES), 0)
    goal = (((src >> 6) & 1) << 8) + ((src & 31) << 3) + ((src >> 7) << 1) + ((src >> 5) & 1) - iota((512, LANES), 1)
    op_ref[...] = beside(*[one_where(goal == LANES * i) for i in range(4)])
    column = iota((Z, LANES), 1)
    goal = jnp.where(column < ZC, 2 * column, jnp.where(column < Z, 2 * column - (Z - 1), -1))
    ob_ref[...] = one_where(goal == iota((Z, LANES), 0))


def moved(t, amount, edge):
    rows = t.shape[0]
    return jnp.where(edge, 0.0, pltpu.roll(t, amount % rows, 0))


def depth_of(rows):
    return iota((rows, LANES), 0) % ZC


def quad(bias):
    return beside(bias, bias, bias, bias)


def put_plane(a_ref, v_ref, layers, ends):
    y0, y9 = ends[:ZC].astype(F32), ends[ZC:].astype(F32)
    for cz in BITS:
        a_ref[cz] = layers[cz].astype(BF16)
        f = layers[cz].astype(F32)
        if cz == 1:
            y0, y9 = pltpu.roll(y0, 32, 1), pltpu.roll(y9, LANES - 32, 1)
        f = stacked(y0, f, y9)
        v_ref[cz] = jnp.where(low_b(320), f[PAIR:], f[:320]).astype(BF16)


def load_own(own_ref, low_ref, high_ref, a_ref, v_ref):
    low_ends = low_ref[SIDE:SIDE_MASK].astype(F32)
    high_ends = high_ref[SIDE:SIDE_MASK].astype(F32)
    for x in range(4):
        layers = []
        for cz in BITS:
            at = (2 * x + cz) * PAIR
            mine = (4 * x + 2 * cz) * PAIR
            layers.append(
                stacked(low_ref[at : at + PAIR], own_ref[mine : mine + 2 * PAIR], high_ref[at : at + PAIR])
            )
        z = slice(ZC * x, ZC * x + ZC)
        put_plane(a_ref.at[x], v_ref.at[x], layers, stacked(low_ends[z], high_ends[z]))


def load_full(ref, at, a_ref, v_ref):
    layers = [ref[at + 320 * cz : at + 320 * cz + 320] for cz in BITS]
    put_plane(a_ref, v_ref, layers, ref[at + 640 : at + PLANE].astype(F32))


def load_half(ref, at, a_ref, v_ref):
    both = ref[at : at + 320].astype(F32)
    put_plane(a_ref, v_ref, [both, pltpu.roll(both, 64, 1)], ref[at + 320 : at + HALF].astype(F32))


def load_far(mid_ref, flank_ref, a, v, k_ref):
    for i in range(2):
        mine, at = 4 * PAIR * i, 5 * PAIR * i
        layers = []
        for cz in BITS:
            low, high = at + PAIR * cz, at + PAIR * (2 + cz)
            own = mine + 2 * PAIR * cz
            layers.append(
                stacked(flank_ref[low : low + PAIR], mid_ref[own : own + 2 * PAIR], flank_ref[high : high + PAIR])
            )
        put_plane(a[i], v[i], layers, flank_ref[at + 4 * PAIR : at + 5 * PAIR].astype(F32))
    at = 10 * PAIR
    both = stacked(
        flank_ref[at : at + PAIR], mid_ref[8 * PAIR : 10 * PAIR], flank_ref[at + PAIR : at + 2 * PAIR]
    ).astype(F32)
    put_plane(a[2], v[2], [both, pltpu.roll(both, 64, 1)], flank_ref[at + 2 * PAIR : at + 3 * PAIR].astype(F32))
    masks = flank_ref[FLANKS : FLANKS + PAIR].astype(F32)
    load_masks([masks[:ZC], mid_ref[MIDDLE : MIDDLE + ZC], masks[ZC:]], k_ref)


def load_masks(parts, k_ref):
    for by, k in enumerate(parts):
        k = k.astype(F32)
        m = jnp.maximum(k, pltpu.roll(k, LANES - 1, 1))
        m = jnp.maximum(m, pltpu.roll(m, LANES - 8, 1))
        m = jnp.maximum(m, pltpu.roll(m, LANES - 64, 1))
        k_ref[0, by, 0:ZC] = k
        k_ref[1, by, 0:ZC] = m


def load_side_masks(ref, at, k_ref):
    masks = ref[at : at + MASKS].astype(F32)
    load_masks([masks[ZC * i : ZC * i + ZC] for i in range(3)], k_ref)


def spread(k, index):
    return stacked(*[jnp.take_along_axis(k[8 * i : 8 * i + 8], index, axis=1, mode="promise_in_bounds") for i in range(5)])


def silu(v):
    half = 0.5 * v
    return half + half * jnp.tanh(half)


def joined_x(planes, p, part, right, rows):
    count = rows.stop - rows.start
    takes_next = one_where((1 - (iota((count, LANES), 1) >> 6)) == right) > 0.5
    return jnp.where(takes_next, planes[p + 1][part, rows], planes[p - 1][part, rows])


def spans(planes, p, parts, right, rows):
    return [planes[p][part, rows] for part in parts] + [joined_x(planes, p, part, right, rows) for part in parts]


def encode_dot(p, right, a, v, we_ref):
    every = slice(0, 320)
    return nn(beside(*spans(a, p, BITS, right, every), *spans(v, p, BITS, right, every)), we_ref[...])


def encode_finish(o, lx, k_ref, e_ref, ev_ref, be, wn_ref):
    z8 = depth_of(320)
    first, last = z8 == 0, z8 == ZC - 1
    lane = iota((8, LANES), 1)
    lane_at = 8 * (lane >> 6) + ((lane >> 5) & 1) + 16 * lx
    pre = (
        o[:, 0:128] + moved(o[:, 256:384], 1, first) + be,
        o[:, 128:256] + moved(o[:, 384:512], -1, last) + be,
    )
    enc = []
    for cz in BITS:
        active = []
        for yi in range(1, 9):
            by, ly = (yi + 1) >> 2, (yi + 1) & 3
            active.append(spread(k_ref[0, by, 0:ZC], lane_at + (64 * cz + 2 * ly)))
        e = jnp.where(stacked(*active) > 0.5, silu(pre[cz]), 0.0)
        enc.append(e.astype(BF16))
        if e_ref is None:
            continue
        e_ref[cz] = enc[cz]
        ev_ref[cz, 0:160] = jnp.where(low_b(160), e[120:280], e[40:200]).astype(BF16)
    return nt(beside(*enc), wn_ref[...])


def strided_finish(lifted, lx, k_ref, c_ref, d_ref, o_ref, gain, shift):
    where = iota((8, LANES), 1) * 0 + 16 * lx
    on = []
    for yi in range(1, 9):
        by, ly = (yi + 1) >> 2, (yi + 1) & 3
        on.append(spread(k_ref[1, by, 0:ZC], where + 2 * ly))
    on = stacked(*on)
    c = jnp.where(on > 0.5, silu(lifted * gain + shift), 0.0)
    c_ref[...] = c.astype(BF16)
    d_ref[0:240] = c[40:280].astype(BF16)
    o_ref[0:240] = on[40:280]


def coarse_dot(q, right, c, d, wc_ref):
    lhs, rhs = [], []
    for i in range(3):
        lhs += [c[q - 1 + i][0:240], d[q - 1 + i][0:240], c[q - 1 + i][80:320]]
        first = 768 * (1 - right) + 384 * i * (2 * right - 1)
        rhs.append(wc_ref[pl.ds(pl.multiple_of(first, 384), 384)])
    return nn(beside(*lhs), stacked(*rhs))


def coarse_finish(p, o_ref, u_ref, bc, wu_ref):
    z6 = depth_of(240)
    first, last = z6 == 0, z6 == ZC - 1
    s = p[:, 128:256] + moved(p[:, 0:128], 1, first) + moved(p[:, 256:384], -1, last) + bc
    act = jnp.where(o_ref[0:240] > 0.5, silu(s), 0.0).astype(BF16)
    u = nt(act, stacked(*([wu_ref[...]] * 4)))
    u_ref[0, 0:160] = u[40:200].astype(BF16)
    u_ref[1, 0:160] = jnp.where(low_b(160), u[80:240], u[0:160]).astype(BF16)


def decode_dot(p, right, e, ev, u, wd_ref):
    mid, every = slice(80, 240), slice(0, 160)
    lhs = spans(e, p, BITS, right, mid) + spans(ev, p, BITS, right, every)
    for v in BITS:
        lhs += spans(u, p, (v,), right, every)
    return nn(beside(*lhs), wd_ref[...])


def decode_finish(o, xo, bd, perm, back, m_ref, out_ref, at):
    z4 = depth_of(160)
    first, last = z4 == 0, z4 == ZC - 1
    d0 = o[:, 0:128] + moved(o[:, 256:384], 1, first) + bd
    d1 = o[:, 128:256] + moved(o[:, 384:512], -1, last) + bd
    d = [beside(*[v[ZC * y : ZC * y + ZC] for y in range(4)]) for v in (d0, d1)]
    d = stacked(*d, jnp.zeros((LANES - Z, 512), F32)).astype(BF16)
    d = nn(nn(back, d).astype(BF16), perm)
    d = stacked(d, jnp.zeros((LANES - Z, 512), F32))
    for a in BITS:
        t = jnp.transpose(d[:, 256 * a : 256 * a + 256])[:, :Z].reshape(CH, 8, Z)
        out_ref[:, at + a] = jnp.where(m_ref[2 * xo + a][None] > 0, t, 0.0).astype(BF16)


def own_kernel(
    own_ref, low_ref, high_ref, we_ref, be_ref, wn_ref, gain_ref, shift_ref, a_ref, v_ref, e_ref, ev_ref, c_ref, d_ref,
    o_ref, k_ref
):
    load_own(own_ref, low_ref, high_ref, a_ref, v_ref)
    load_masks((low_ref[SIDE_MASK:SIDE_ROWS], own_ref[OWN : OWN + ZC], high_ref[SIDE_MASK:SIDE_ROWS]), k_ref)
    be = quad(be_ref[...])
    a, v = ([ref.at[x] for x in range(4)] for ref in (a_ref, v_ref))
    dots = [encode_dot(1 + i, 1, a, v, we_ref) for i in range(2)]
    lifted = [encode_finish(dots[i], 1 + i, k_ref, e_ref.at[i], ev_ref.at[i], be, wn_ref) for i in range(2)]
    for i in range(2):
        strided_finish(
            lifted[i], 1 + i, k_ref, c_ref.at[i], d_ref.at[i], o_ref.at[i], gain_ref[...], shift_ref[...]
        )


def own_planes(right, own):
    two = [right * (1 + 2 * i) + 1 - i for i in range(2)]
    one = [right * (2 * i - 1) + 1 - i for i in range(2)]
    a, v = ([ref.at[at] for at in two] for ref in own[0:2])
    e, ev, c, d, o = ([ref.at[at] for at in one] for ref in own[2:7])
    return a, v, e, ev, c, d, o


class Stages:
    def __init__(self, right, weights, misc, planes, side_k, own_k, emit):
        self.right, self.planes, self.emit = right, planes, emit
        self.we, be, self.wn, gain, shift, self.wc, bc, self.wu = weights
        self.m, self.wd, bd, perm, back = misc
        self.be, self.bd = quad(be[...]), quad(bd[...])
        self.gain, self.shift, self.bc = gain[...], shift[...], bc[...]
        self.perm, self.back = perm[...], back[...]
        self.k = (own_k, side_k, side_k)
        self.lx = (3 * right, 3 - 3 * right, 2 - right)

    def e_dot(self, i):
        return encode_dot(1 + i, self.right, self.planes[0], self.planes[1], self.we)

    def e_finish(self, i, dot):
        e, ev = self.planes[2], self.planes[3]
        at = (e[3 + i], ev[3 + i]) if i < 2 else (None, None)
        return encode_finish(dot, self.lx[i], self.k[i], *at, self.be, self.wn)

    def s_finish(self, i, lifted):
        c, d, o = self.planes[4:7]
        strided_finish(lifted, self.lx[i], self.k[i], c[2 + i], d[2 + i], o[2 + i], self.gain, self.shift)

    def c_dot(self, i):
        return coarse_dot(1 + i, self.right, self.planes[4], self.planes[5], self.wc)

    def c_finish(self, i, dot):
        coarse_finish(dot, self.planes[6][1 + i], self.planes[7][2 + i], self.bc, self.wu)

    def d_dot(self, i):
        return decode_dot(1 + i, self.right, self.planes[2], self.planes[3], self.planes[7], self.wd)

    def d_finish(self, i, dot):
        self.emit(i, dot, self.bd, self.perm, self.back, self.m)


def near_kernel(right_ref, side_ref, *refs):
    weights, misc, own = refs[:8], refs[8:13], refs[13:21]
    done_ref, e1_ref, ev1_ref, u1_ref = refs[21:25]
    a_ref, v_ref, e_ref, ev_ref, c_ref, d_ref, o_ref, k_ref, u_ref = refs[25:]
    right = right_ref[0]
    a, v, e, ev, c, d, o = own_planes(right, own)
    a, v, c, d, o = (x + [r.at[i] for i in range(3)] for x, r in zip((a, v, c, d, o), (a_ref, v_ref, c_ref, d_ref, o_ref)))
    e, ev = [None] + e + [e1_ref, e_ref.at[0]], [None] + ev + [ev1_ref, ev_ref.at[0]]
    u = [None, None, u1_ref.at[0], u1_ref.at[1], u_ref.at[0]]
    for i in range(2):
        load_full(side_ref, i * PLANE, a[2 + i], v[2 + i])
    load_half(side_ref, 2 * PLANE, a[4], v[4])
    load_side_masks(side_ref, 2 * PLANE + HALF, k_ref)

    def emit(i, dot, bd, perm, back, m_ref):
        decode_finish(dot, 3 * right, bd, perm, back, m_ref, done_ref, 0)

    w = Stages(right, weights, misc, (a, v, e, ev, c, d, o, u), k_ref, own[7], emit)
    e0 = w.e_dot(0)
    e1 = w.e_dot(1)
    l0 = w.e_finish(0, e0)
    e2 = w.e_dot(2)
    w.s_finish(0, l0)
    l1 = w.e_finish(1, e1)
    c0 = w.c_dot(0)
    w.s_finish(1, l1)
    l2 = w.e_finish(2, e2)
    w.c_finish(0, c0)
    c1 = w.c_dot(1)
    w.s_finish(2, l2)
    w.c_finish(1, c1)
    c2 = w.c_dot(2)
    w.c_finish(2, c2)
    w.d_finish(2, w.d_dot(2))


def far_place(right, i):
    return right * (2 * i - 1) + 2 - i


def far_kernel(right_ref, middle_ref, flanks_ref, *refs):
    weights, misc, own = refs[:8], refs[8:13], refs[13:21]
    near_done_ref, e1_ref, ev1_ref, u1_ref, out_hbm = refs[21:26]
    a_ref, v_ref, e_ref, ev_ref, c_ref, d_ref, o_ref, k_ref, u_ref, out_ref, sems = refs[26:]
    left = right_ref[0]
    right = 1 - left
    copies = [pltpu.make_async_copy(near_done_ref, out_hbm.at[:, pl.ds(6 * left, 2)], sems.at[3])]
    copies[0].start()
    a, v, e, ev, c, d, o = own_planes(right, own)
    a, v, c, d, o = (x + [r.at[i] for i in range(3)] for x, r in zip((a, v, c, d, o), (a_ref, v_ref, c_ref, d_ref, o_ref)))
    e = [e1_ref] + e + [e_ref.at[0], e_ref.at[1]]
    ev = [ev1_ref] + ev + [ev_ref.at[0], ev_ref.at[1]]
    u = [u1_ref.at[1], u1_ref.at[0]] + [u_ref.at[i] for i in range(3)]
    load_far(middle_ref, flanks_ref, a[2:], v[2:], k_ref)

    def emit(i, dot, bd, perm, back, m_ref):
        xo = far_place(right, i)
        at = pl.ds(2 * i, 2)
        decode_finish(dot, xo, bd, perm, back, m_ref, out_ref, 2 * i)
        copies.append(pltpu.make_async_copy(out_ref.at[:, at], out_hbm.at[:, pl.ds(2 * xo, 2)], sems.at[i]))
        copies[-1].start()

    w = Stages(right, weights, misc, (a, v, e, ev, c, d, o, u), k_ref, own[7], emit)
    e0 = w.e_dot(0)
    e1 = w.e_dot(1)
    l0 = w.e_finish(0, e0)
    e2 = w.e_dot(2)
    w.s_finish(0, l0)
    l1 = w.e_finish(1, e1)
    c0 = w.c_dot(0)
    w.s_finish(1, l1)
    l2 = w.e_finish(2, e2)
    w.c_finish(0, c0)
    c1 = w.c_dot(1)
    w.s_finish(2, l2)
    d0 = w.d_dot(0)
    w.c_finish(1, c1)
    c2 = w.c_dot(2)
    w.d_finish(0, d0)
    d1 = w.d_dot(1)
    w.c_finish(2, c2)
    d2 = w.d_dot(2)
    w.d_finish(1, d1)
    w.d_finish(2, d2)
    for copy in copies:
        copy.wait()


def vmem(n):
    return [pl.BlockSpec(memory_space=pltpu.VMEM)] * n


def hbm(n):
    return [pl.BlockSpec(memory_space=pltpu.HBM)] * n


def call(kernel, outs, ins, out_specs, scratch, mib, flops):
    return pl.pallas_call(
        kernel,
        out_shape=outs,
        in_specs=ins,
        out_specs=out_specs,
        scratch_shapes=scratch,
        compiler_params=pltpu.CompilerParams(vmem_limit_bytes=mib << 20),
        cost_estimate=pl.CostEstimate(flops=flops, bytes_accessed=10**6, transcendentals=0),
    )


def array(*shape, kind=BF16):
    return jax.ShapeDtypeStruct(shape, kind)


def buffers(shapes):
    return [pltpu.VMEM(s, d) for s, d in shapes]


def shifted(value, axis, step):
    peers = lax.axis_size(axis)
    return lax.ppermute(value, axis, [(i, i + step) for i in range(peers) if 0 <= i + step < peers])


def swapped(value, axis, first):
    peers = lax.axis_size(axis)
    pairs = []
    for i in range(first, peers - 1, 2):
        pairs += [(i, i + 1), (i + 1, i)]
    return lax.ppermute(value, axis, pairs)


def time_features(timestep, embed_width):
    halves = embed_width // 2
    freqs = jnp.exp(-math.log(10000.0) * jnp.arange(halves, dtype=F32) / halves)
    angles = timestep[0].astype(F32) * freqs
    return jnp.concatenate([jnp.sin(angles), jnp.cos(angles)]).astype(BF16)


SCALAR = [pl.BlockSpec(memory_space=pltpu.SMEM)]


def state(own, planes, encoded):
    return [
        (own + (2, 320, LANES), BF16),
        (own + (2, 320, LANES), BF16),
        (encoded + (2, 320, LANES), BF16),
        (encoded + (2, 192, LANES), BF16),
        (planes + (320, LANES), BF16),
        (planes + (256, LANES), BF16),
        (planes + (256, LANES), F32),
        ((2, 3, 64, LANES), F32),
    ]


LIFTED = (2, 192, LANES)


def arrays(shapes):
    return [array(*shape, kind=kind) for shape, kind in shapes]


def on_device(
    fine_in, voxel_mask, timestep, w_enc, b_enc, w_down, w_time, w_coarse, b_coarse, w_up, w_dec, b_dec
):
    own, up, down = call(
        pack_kernel,
        [array(OWN + ZC, LANES), array(SIDE_ROWS, LANES), array(SIDE_ROWS, LANES)],
        hbm(2),
        vmem(3),
        [pltpu.VMEM(fine_in.shape, BF16), pltpu.VMEM(voxel_mask.shape, jnp.int32), pltpu.SemaphoreType.DMA((5,))],
        12,
        10**9,
    )(pltpu.with_memory_space_constraint(fine_in, pltpu.HBM), pltpu.with_memory_space_constraint(voxel_mask, pltpu.HBM))
    low = shifted(up, "wide", 1)
    high = shifted(down, "wide", -1)

    odd = lax.axis_index("narrow").astype(jnp.int32)[None] & 1
    near_right = 1 - odd
    middle = call(edge_kernel, [array(MIDDLE + ZC, LANES)], SCALAR + vmem(1), vmem(1), [], 8, 10**8)(odd, own)[0]
    middle = swapped(middle, "narrow", 1)

    embedded = time_features(timestep, w_time.shape[0])
    film = jnp.dot(embedded[None], w_time, preferred_element_type=F32)
    chans = w_down.shape[0]
    gains = 1.0 + film[:, :chans]
    shifts = film[:, chans:]
    taps = 27 * LANES
    enc_w, dec_w, down_w, perm, back, coarse_w = call(
        weights_kernel,
        [array(1024, 512), array(1536, 512), array(128, 256), array(512, 512), array(Z, LANES)]
        + [array(9 * LANES, 384)],
        vmem(4),
        vmem(6),
        buffers([((taps, 32), BF16), ((taps, 64), BF16), ((32, taps), F32), ((64, taps), F32)]),
        16,
        4 * 10**9,
    )(w_enc, w_dec, w_down, w_coarse)

    flanks, near = call(
        mid_kernel,
        [array(FLANKS + PAIR, LANES), array(2 * PLANE + HALF + MASKS, LANES)],
        SCALAR + vmem(5),
        vmem(2),
        buffers([((2, 4 * ZC, LANES), F32)]),
        8,
        10**8,
    )(odd, own, low, high, down_w, gains)
    flanks = swapped(flanks, "narrow", 1)
    near = swapped(near, "narrow", 0)

    encoder = (enc_w, b_enc[None], down_w, gains, shifts)
    mine = call(own_kernel, arrays(state((4,), (2,), (2,))), vmem(8), vmem(8), [], 12, 2 * 10**9)(
        own, low, high, *encoder
    )
    some = encoder + (coarse_w, b_coarse[None], w_up, voxel_mask, dec_w, b_dec[None], perm, back) + tuple(mine)
    pair = array(fine_in.shape[0], 2, *fine_in.shape[2:])
    near_done, e1, ev1, u1 = call(
        near_kernel,
        [pair] + arrays(state((), (), ())[2:4] + [((2,) + LIFTED, BF16)]),
        SCALAR + vmem(22),
        vmem(4),
        buffers(state((3,), (3,), (1,)) + [((1,) + LIFTED, BF16)]),
        24,
        4 * 10**9,
    )(near_right, near, *some)
    rest = pltpu.VMEM((fine_in.shape[0], 6) + fine_in.shape[2:], BF16)
    return call(
        far_kernel,
        [array(*fine_in.shape)],
        SCALAR + vmem(27),
        hbm(1),
        buffers(state((3,), (3,), (2,)) + [((3,) + LIFTED, BF16)]) + [rest, pltpu.SemaphoreType.DMA((4,))],
        24,
        5 * 10**9,
    )(near_right, middle, flanks, *some, near_done, e1, ev1, u1)[0]


def solution(mesh):
    field = P(None, "narrow", "wide", None)
    return jax.shard_map(
        on_device,
        mesh=mesh,
        in_specs=(field, P("narrow", "wide", None)) + (P(),) * 10,
        out_specs=field,
        check_vma=False,
    )
```

```python
import math

import jax
import jax.numpy as jnp
from jax import lax
from jax.experimental import pallas as pl
from jax.experimental.pallas import tpu as pltpu
from jax.sharding import PartitionSpec as P


F32 = jnp.float32
BF16 = jnp.bfloat16
LANES = 128
ZC = 40
Z = 80
CH = 32
BITS = (0, 1)


def nn(a, b):
    return lax.dot_general(a, b, (((1,), (0,)), ((), ())), preferred_element_type=F32)


def nt(a, b):
    return lax.dot_general(a, b, (((1,), (1,)), ((), ())), preferred_element_type=F32)


def iota(shape, dim):
    return lax.broadcasted_iota(jnp.int32, shape, dim)


PAIR = 2 * ZC
OWN = 16 * PAIR
SIDE = 8 * PAIR
SIDE_MASK = SIDE + 4 * ZC
SIDE_ROWS = SIDE_MASK + ZC
MIDDLE = 10 * PAIR
FLANKS = 13 * PAIR


def one_where(truth):
    return truth.astype(F32).astype(BF16)


def unpick(rows, cols):
    row = iota((rows, cols), 0)
    return one_where(jnp.where(row < ZC, 2 * row, 2 * row - (Z - 1)) == iota((rows, cols), 1))


def low_b(rows):
    return (iota((rows, LANES), 1) & 32) == 0


def stacked(*parts):
    return jnp.concatenate(parts, axis=0)


def beside(*parts):
    return jnp.concatenate(parts, axis=1)


def pack_kernel(x_hbm, m_hbm, own_ref, up_ref, dn_ref, x_ref, m_ref, sems):
    copies = [pltpu.make_async_copy(m_hbm, m_ref, sems.at[4])]
    for cx in range(4):
        copies.append(pltpu.make_async_copy(x_hbm.at[:, pl.ds(2 * cx, 2)], x_ref.at[:, pl.ds(2 * cx, 2)], sems.at[cx]))
    for copy in copies:
        copy.start()
    sel = unpick(Z, Z)
    src = iota((512, LANES), 0)
    y = src & 7
    goal = ((y >> 1) << 7) + ((src >> 8) << 6) + ((y & 1) << 5) + ((src >> 3) & 31) - iota((512, LANES), 1)
    perm = [one_where(goal == LANES * i) for i in range(4)]
    copies[0].wait()
    mask = (m_ref[...] > 0).astype(F32).reshape(64, Z).astype(BF16)
    cols = nt(sel, mask)
    cols = beside(cols[:ZC], cols[ZC:]).astype(BF16)
    own_ref[OWN : OWN + ZC] = cols
    up_ref[SIDE_MASK:SIDE_ROWS] = cols
    dn_ref[SIDE_MASK:SIDE_ROWS] = cols
    sides = [[], []]
    for cx in range(4):
        copies[1 + cx].wait()
        for a in BITS:
            x = 2 * cx + a
            tile = x_ref[:, x].astype(F32)
            tile = jnp.where(m_ref[x][None] > 0, tile, 0.0)
            sides[a].append(nt(sel, tile.reshape(8 * CH, Z).astype(BF16)).astype(BF16))
    both = beside(stacked(*sides[0]), stacked(*sides[1]))
    cols = [nn(both, perm[cy]) for cy in range(4)]
    ups, downs = [], []
    for cx in range(4):
        col = [v[Z * cx : Z * cx + Z] for v in cols]
        for cz in BITS:
            z = slice(ZC * cz, ZC * cz + ZC)
            first = stacked(col[0][z], col[1][z]).astype(BF16)
            second = stacked(col[2][z], col[3][z]).astype(BF16)
            own_ref[pl.ds((4 * cx + 2 * cz) * PAIR, PAIR)] = first
            own_ref[pl.ds((4 * cx + 2 * cz + 1) * PAIR, PAIR)] = second
            dn_ref[pl.ds((2 * cx + cz) * PAIR, PAIR)] = first
            up_ref[pl.ds((2 * cx + cz) * PAIR, PAIR)] = second
        ups.append(jnp.where(low_b(ZC), pltpu.roll(col[1][ZC:], LANES - 32, 1), col[1][:ZC]))
        downs.append(jnp.where(low_b(ZC), col[2][:ZC], pltpu.roll(col[2][ZC:], 32, 1)))
        if cx % 2 == 1:
            at = pl.ds(SIDE + (cx // 2) * PAIR, PAIR)
            up_ref[at] = stacked(*ups[-2:]).astype(BF16)
            dn_ref[at] = stacked(*downs[-2:]).astype(BF16)


def part(x, size):
    return pl.ds(pl.multiple_of(x * size, size), size)


def folded(pieces, right):
    lane_a = iota(pieces[0].shape, 1) >> 6
    even, odd = (v.astype(F32) for v in pieces)
    return jnp.where(lane_a == right, even, pltpu.roll(odd, 64, 1)).astype(BF16)


def edge_kernel(odd_ref, own_ref, far_ref, near_ref):
    for out_ref, right in ((far_ref, odd_ref[0]), (near_ref, 1 - odd_ref[0])):
        for i, x in enumerate((3 * right, 1 + right)):
            out_ref[4 * PAIR * i : 4 * PAIR * (i + 1)] = own_ref[part(x, 4 * PAIR)]
        x = 2 - right
        pieces = [own_ref[pl.ds(pl.multiple_of((4 * x + 2 * cz) * PAIR, PAIR), 2 * PAIR)] for cz in BITS]
        out_ref[8 * PAIR : 10 * PAIR] = folded(pieces, right)
        out_ref[MIDDLE : MIDDLE + ZC] = own_ref[OWN : OWN + ZC]


def mid_kernel(odd_ref, low_ref, high_ref, tie_ref, tie2_ref, far_ref, near_ref, ends_ref):
    ends_ref[0] = low_ref[SIDE:SIDE_MASK].astype(F32)
    ends_ref[1] = high_ref[SIDE:SIDE_MASK].astype(F32)

    def ends(x):
        at = part(x, ZC)
        return stacked(ends_ref[0, at], ends_ref[1, at]).astype(BF16)

    for out_ref, right in ((far_ref, odd_ref[0]), (near_ref, 1 - odd_ref[0])):
        for i, x in enumerate((3 * right, 1 + right)):
            at = 5 * PAIR * i
            out_ref[at : at + 2 * PAIR] = low_ref[part(x, 2 * PAIR)]
            out_ref[at + 2 * PAIR : at + 4 * PAIR] = high_ref[part(x, 2 * PAIR)]
            out_ref[at + 4 * PAIR : at + 5 * PAIR] = ends(x)
        x, at = 2 - right, 10 * PAIR
        for ref in (low_ref, high_ref):
            pieces = [ref[pl.ds(pl.multiple_of((2 * x + cz) * PAIR, PAIR), PAIR)] for cz in BITS]
            out_ref[at : at + PAIR] = folded(pieces, right)
            at = at + PAIR
        out_ref[at : at + PAIR] = ends(x)
        masks = [low_ref[SIDE_MASK:SIDE_ROWS], high_ref[SIDE_MASK:SIDE_ROWS]]
        out_ref[FLANKS : FLANKS + PAIR] = stacked(*[m.astype(F32) for m in masks]).astype(BF16)


def tap_of(out_bit, in_bit, far):
    if far:
        return 2 * (1 - in_bit) if out_bit != in_bit else None
    return in_bit - out_bit + 1


def placed(w_ref, rows, taps, group):
    total = jnp.zeros((CH, LANES), F32)
    for g, tap in enumerate(taps):
        if tap is not None:
            total = jnp.where(group == g, w_ref[rows : rows + CH, LANES * tap : LANES * tap + LANES], total)
    return total


def block(w_ref, rows, group, far_x, far_y, a_in, b_in, cz_in, shifted, cz_out):
    if shifted:
        tz = None
        if cz_out == 0 and cz_in == 1:
            tz = 0
        if cz_out == 1 and cz_in == 0:
            tz = 2
    else:
        tz = cz_in - cz_out + 1
    taps = []
    for a_out in BITS:
        for b_out in BITS:
            tx = tap_of(a_out, a_in, far_x)
            ty = tap_of(b_out, b_in, far_y)
            taps.append(None if tx is None or ty is None or tz is None else 9 * tx + 3 * ty + tz)
    return placed(w_ref, rows, taps, group)


KINDS = ((0, 0), (1, 0), (0, 1), (1, 1))


def weights_kernel(
    we_ref, wd_ref, wn_ref, wc_ref, oe_ref, od_ref, on_ref, op_ref, ob_ref, oc_ref, re_ref, rd_ref, te_ref, td_ref
):
    for tap in range(27):
        for g in range(4):
            at = LANES * tap + CH * g
            re_ref[at : at + CH] = we_ref[tap]
            rd_ref[at : at + CH] = wd_ref[tap]
    one = (iota((CH, CH), 0) == iota((CH, CH), 1)).astype(F32).astype(BF16)
    te_ref[...] = nt(one, re_ref[...])
    one = (iota((2 * CH, 2 * CH), 0) == iota((2 * CH, 2 * CH), 1)).astype(F32).astype(BF16)
    td_ref[...] = nt(one, rd_ref[...])
    one = one_where(iota((LANES, LANES), 0) == iota((LANES, LANES), 1))
    for i in range(9):
        oc_ref[LANES * i : LANES * i + LANES] = nt(one, wc_ref[3 * i : 3 * i + 3].reshape(384, LANES)).astype(BF16)
    group = iota((CH, LANES), 1) >> 5
    for w_ref, o_ref in ((te_ref, oe_ref), (td_ref, od_ref)):
        for t, (fx, fy) in enumerate(KINDS):
            for cz in BITS:
                for a in BITS:
                    for b in BITS:
                        base = 256 * t + 128 * cz + 64 * a + 32 * b
                        for s in BITS:
                            for co in BITS:
                                v = block(w_ref, 0, group, fx, fy, a, b, cz, s, co)
                                o_ref[base : base + CH, 256 * s + 128 * co : 256 * s + 128 * co + LANES] = v.astype(BF16)
    for t, (fx, fy) in enumerate(KINDS):
        for a in BITS:
            for b in BITS:
                base = 1024 + 128 * t + 64 * a + 32 * b
                for s in BITS:
                    for co in BITS:
                        v = block(td_ref, CH, group, fx, fy, a, b, 0, s, co)
                        v = v + block(td_ref, CH, group, fx, fy, a, b, 1, s, co)
                        od_ref[base : base + CH, 256 * s + 128 * co : 256 * s + 128 * co + LANES] = v.astype(BF16)
    k = iota((8 * CH, LANES), 0)
    goal = (((k >> 5) & 1) << 7) + ((k >> 6) << 5) + (k & 31) - iota((8 * CH, LANES), 1)
    perm = jnp.concatenate([(goal == LANES * i).astype(F32).astype(BF16) for i in BITS], axis=1)
    on_ref[...] = nn(wn_ref[...], perm).astype(BF16)
    src = iota((512, LANES), 0)
    goal = (((src >> 6) & 1) << 8) + ((src & 31) << 3) + ((src >> 7) << 1) + ((src >> 5) & 1) - iota((512, LANES), 1)
    op_ref[...] = beside(*[one_where(goal == LANES * i) for i in range(4)])
    column = iota((Z, LANES), 1)
    goal = jnp.where(column < ZC, 2 * column, jnp.where(column < Z, 2 * column - (Z - 1), -1))
    ob_ref[...] = one_where(goal == iota((Z, LANES), 0))


def moved(t, amount, edge):
    rows = t.shape[0]
    return jnp.where(edge, 0.0, pltpu.roll(t, amount % rows, 0))


def depth_of(rows):
    return iota((rows, LANES), 0) % ZC


def quad(bias):
    return beside(bias, bias, bias, bias)


def put_plane(a_ref, v_ref, layers, ends):
    y0, y9 = ends[:ZC].astype(F32), ends[ZC:].astype(F32)
    for cz in BITS:
        a_ref[cz] = layers[cz].astype(BF16)
        f = layers[cz].astype(F32)
        if cz == 1:
            y0, y9 = pltpu.roll(y0, 32, 1), pltpu.roll(y9, LANES - 32, 1)
        f = stacked(y0, f, y9)
        v_ref[cz] = jnp.where(low_b(320), f[PAIR:], f[:320]).astype(BF16)


def load_own(own_ref, low_ref, high_ref, a_ref, v_ref):
    low_ends = low_ref[SIDE:SIDE_MASK].astype(F32)
    high_ends = high_ref[SIDE:SIDE_MASK].astype(F32)
    for x in range(4):
        layers = []
        for cz in BITS:
            at = (2 * x + cz) * PAIR
            mine = (4 * x + 2 * cz) * PAIR
            layers.append(
                stacked(low_ref[at : at + PAIR], own_ref[mine : mine + 2 * PAIR], high_ref[at : at + PAIR])
            )
        z = slice(ZC * x, ZC * x + ZC)
        put_plane(a_ref.at[x], v_ref.at[x], layers, stacked(low_ends[z], high_ends[z]))


def load_side(mid_ref, flank_ref, a, v, k_ref):
    for i in range(2):
        mine, at = 4 * PAIR * i, 5 * PAIR * i
        layers = []
        for cz in BITS:
            low, high = at + PAIR * cz, at + PAIR * (2 + cz)
            own = mine + 2 * PAIR * cz
            layers.append(
                stacked(flank_ref[low : low + PAIR], mid_ref[own : own + 2 * PAIR], flank_ref[high : high + PAIR])
            )
        put_plane(a[i], v[i], layers, flank_ref[at + 4 * PAIR : at + 5 * PAIR].astype(F32))
    at = 10 * PAIR
    both = stacked(
        flank_ref[at : at + PAIR], mid_ref[8 * PAIR : 10 * PAIR], flank_ref[at + PAIR : at + 2 * PAIR]
    ).astype(F32)
    put_plane(a[2], v[2], [both, pltpu.roll(both, 64, 1)], flank_ref[at + 2 * PAIR : at + 3 * PAIR].astype(F32))
    masks = flank_ref[FLANKS : FLANKS + PAIR].astype(F32)
    load_masks([masks[:ZC], mid_ref[MIDDLE : MIDDLE + ZC], masks[ZC:]], k_ref)


def load_masks(parts, k_ref):
    for by, k in enumerate(parts):
        k = k.astype(F32)
        m = jnp.maximum(k, pltpu.roll(k, LANES - 1, 1))
        m = jnp.maximum(m, pltpu.roll(m, LANES - 8, 1))
        m = jnp.maximum(m, pltpu.roll(m, LANES - 64, 1))
        k_ref[0, by, 0:ZC] = k
        k_ref[1, by, 0:ZC] = m


def spread(k, index):
    return stacked(*[jnp.take_along_axis(k[8 * i : 8 * i + 8], index, axis=1, mode="promise_in_bounds") for i in range(5)])


def silu(v):
    half = 0.5 * v
    return half + half * jnp.tanh(half)


def joined_x(planes, p, part, right, rows):
    count = rows.stop - rows.start
    takes_next = one_where((1 - (iota((count, LANES), 1) >> 6)) == right) > 0.5
    return jnp.where(takes_next, planes[p + 1][part, rows], planes[p - 1][part, rows])


def spans(planes, p, parts, right, rows):
    return [planes[p][part, rows] for part in parts] + [joined_x(planes, p, part, right, rows) for part in parts]


def encode_dot(p, right, a, v, we_ref):
    every = slice(0, 320)
    return nn(beside(*spans(a, p, BITS, right, every), *spans(v, p, BITS, right, every)), we_ref[...])


def encode_finish(o, lx, k_ref, e_ref, ev_ref, be, wn_ref):
    z8 = depth_of(320)
    first, last = z8 == 0, z8 == ZC - 1
    lane = iota((8, LANES), 1)
    lane_at = 8 * (lane >> 6) + ((lane >> 5) & 1) + 16 * lx
    pre = (
        o[:, 0:128] + moved(o[:, 256:384], 1, first) + be,
        o[:, 128:256] + moved(o[:, 384:512], -1, last) + be,
    )
    enc = []
    for cz in BITS:
        active = []
        for yi in range(1, 9):
            by, ly = (yi + 1) >> 2, (yi + 1) & 3
            active.append(spread(k_ref[0, by, 0:ZC], lane_at + (64 * cz + 2 * ly)))
        e = jnp.where(stacked(*active) > 0.5, silu(pre[cz]), 0.0)
        enc.append(e.astype(BF16))
        if e_ref is None:
            continue
        e_ref[cz] = enc[cz]
        ev_ref[cz, 0:160] = jnp.where(low_b(160), e[120:280], e[40:200]).astype(BF16)
    return nt(beside(*enc), wn_ref[...])


def strided_finish(lifted, lx, k_ref, c_ref, d_ref, o_ref, gain, shift):
    where = iota((8, LANES), 1) * 0 + 16 * lx
    on = []
    for yi in range(1, 9):
        by, ly = (yi + 1) >> 2, (yi + 1) & 3
        on.append(spread(k_ref[1, by, 0:ZC], where + 2 * ly))
    on = stacked(*on)
    c = jnp.where(on > 0.5, silu(lifted * gain + shift), 0.0)
    c_ref[...] = c.astype(BF16)
    d_ref[0:240] = c[40:280].astype(BF16)
    o_ref[0:240] = on[40:280]


def coarse_dot(q, right, c, d, wc_ref):
    lhs, rhs = [], []
    for i in range(3):
        lhs += [c[q - 1 + i][0:240], d[q - 1 + i][0:240], c[q - 1 + i][80:320]]
        first = 768 * (1 - right) + 384 * i * (2 * right - 1)
        rhs.append(wc_ref[pl.ds(pl.multiple_of(first, 384), 384)])
    return nn(beside(*lhs), stacked(*rhs))


def coarse_finish(p, o_ref, u_ref, bc, wu_ref):
    z6 = depth_of(240)
    first, last = z6 == 0, z6 == ZC - 1
    s = p[:, 128:256] + moved(p[:, 0:128], 1, first) + moved(p[:, 256:384], -1, last) + bc
    act = jnp.where(o_ref[0:240] > 0.5, silu(s), 0.0).astype(BF16)
    u = nt(act, stacked(*([wu_ref[...]] * 4)))
    u_ref[0, 0:160] = u[40:200].astype(BF16)
    u_ref[1, 0:160] = jnp.where(low_b(160), u[80:240], u[0:160]).astype(BF16)


def decode_dot(p, right, e, ev, u, wd_ref):
    mid, every = slice(80, 240), slice(0, 160)
    lhs = spans(e, p, BITS, right, mid) + spans(ev, p, BITS, right, every)
    for v in BITS:
        lhs += spans(u, p, (v,), right, every)
    return nn(beside(*lhs), wd_ref[...])


def decode_finish(o, xo, bd, perm, back, m_ref, out_ref, at, send=None):
    z4 = depth_of(160)
    first, last = z4 == 0, z4 == ZC - 1
    d0 = o[:, 0:128] + moved(o[:, 256:384], 1, first) + bd
    d1 = o[:, 128:256] + moved(o[:, 384:512], -1, last) + bd
    d = [beside(*[v[ZC * y : ZC * y + ZC] for y in range(4)]) for v in (d0, d1)]
    d = stacked(*d, jnp.zeros((LANES - Z, 512), F32)).astype(BF16)
    d = nn(nn(back, d).astype(BF16), perm)
    d = stacked(d, jnp.zeros((LANES - Z, 512), F32))
    for a in BITS:
        t = jnp.transpose(d[:, 256 * a : 256 * a + 256])[:, :Z].reshape(CH, 8, Z)
        out_ref[:, at + a] = jnp.where(m_ref[2 * xo + a][None] > 0, t, 0.0).astype(BF16)
        if send is not None:
            send(at + a, 2 * xo + a)


def own_kernel(
    own_ref, low_ref, high_ref, we_ref, be_ref, wn_ref, gain_ref, shift_ref, a_ref, v_ref, e_ref, ev_ref, c_ref, d_ref,
    o_ref, k_ref
):
    load_own(own_ref, low_ref, high_ref, a_ref, v_ref)
    load_masks((low_ref[SIDE_MASK:SIDE_ROWS], own_ref[OWN : OWN + ZC], high_ref[SIDE_MASK:SIDE_ROWS]), k_ref)
    be = quad(be_ref[...])
    a, v = ([ref.at[x] for x in range(4)] for ref in (a_ref, v_ref))
    dots = [encode_dot(1 + i, 1, a, v, we_ref) for i in range(2)]
    lifted = [encode_finish(dots[i], 1 + i, k_ref, e_ref.at[i], ev_ref.at[i], be, wn_ref) for i in range(2)]
    for i in range(2):
        strided_finish(
            lifted[i], 1 + i, k_ref, c_ref.at[i], d_ref.at[i], o_ref.at[i], gain_ref[...], shift_ref[...]
        )


def own_planes(right, own):
    two = [right * (1 + 2 * i) + 1 - i for i in range(2)]
    one = [right * (2 * i - 1) + 1 - i for i in range(2)]
    a, v = ([ref.at[at] for at in two] for ref in own[0:2])
    e, ev, c, d, o = ([ref.at[at] for at in one] for ref in own[2:7])
    return a, v, e, ev, c, d, o


class Stages:
    def __init__(self, right, weights, misc, planes, side_k, own_k, emit):
        self.right, self.planes, self.emit = right, planes, emit
        self.we, be, self.wn, gain, shift, self.wc, bc, self.wu = weights
        self.m, self.wd, bd, perm, back = misc
        self.be, self.bd = quad(be[...]), quad(bd[...])
        self.gain, self.shift, self.bc = gain[...], shift[...], bc[...]
        self.perm, self.back = perm[...], back[...]
        self.k = (own_k, side_k, side_k)
        self.lx = (3 * right, 3 - 3 * right, 2 - right)

    def e_dot(self, i):
        return encode_dot(1 + i, self.right, self.planes[0], self.planes[1], self.we)

    def e_finish(self, i, dot):
        e, ev = self.planes[2], self.planes[3]
        at = (e[3 + i], ev[3 + i]) if i < 2 else (None, None)
        return encode_finish(dot, self.lx[i], self.k[i], *at, self.be, self.wn)

    def s_finish(self, i, lifted):
        c, d, o = self.planes[4:7]
        strided_finish(lifted, self.lx[i], self.k[i], c[2 + i], d[2 + i], o[2 + i], self.gain, self.shift)

    def c_dot(self, i):
        return coarse_dot(1 + i, self.right, self.planes[4], self.planes[5], self.wc)

    def c_finish(self, i, dot):
        coarse_finish(dot, self.planes[6][1 + i], self.planes[7][2 + i], self.bc, self.wu)

    def d_dot(self, i):
        return decode_dot(1 + i, self.right, self.planes[2], self.planes[3], self.planes[7], self.wd)

    def d_finish(self, i, dot):
        self.emit(i, dot, self.bd, self.perm, self.back, self.m)


def near_kernel(right_ref, middle_ref, flanks_ref, *refs):
    weights, misc, own = refs[:8], refs[8:13], refs[13:21]
    done_ref, e1_ref, ev1_ref, u1_ref = refs[21:25]
    a_ref, v_ref, e_ref, ev_ref, c_ref, d_ref, o_ref, k_ref, u_ref = refs[25:]
    right = right_ref[0]
    a, v, e, ev, c, d, o = own_planes(right, own)
    a, v, c, d, o = (x + [r.at[i] for i in range(3)] for x, r in zip((a, v, c, d, o), (a_ref, v_ref, c_ref, d_ref, o_ref)))
    e, ev = [None] + e + [e1_ref, e_ref.at[0]], [None] + ev + [ev1_ref, ev_ref.at[0]]
    u = [None, None, u1_ref.at[0], u1_ref.at[1], u_ref.at[0]]
    load_side(middle_ref, flanks_ref, a[2:], v[2:], k_ref)

    def emit(i, dot, bd, perm, back, m_ref):
        decode_finish(dot, 3 * right, bd, perm, back, m_ref, done_ref, 0)

    w = Stages(right, weights, misc, (a, v, e, ev, c, d, o, u), k_ref, own[7], emit)
    e0 = w.e_dot(0)
    e1 = w.e_dot(1)
    l0 = w.e_finish(0, e0)
    e2 = w.e_dot(2)
    w.s_finish(0, l0)
    l1 = w.e_finish(1, e1)
    c0 = w.c_dot(0)
    w.s_finish(1, l1)
    l2 = w.e_finish(2, e2)
    w.c_finish(0, c0)
    c1 = w.c_dot(1)
    w.s_finish(2, l2)
    w.c_finish(1, c1)
    c2 = w.c_dot(2)
    w.c_finish(2, c2)
    w.d_finish(2, w.d_dot(2))


def far_place(right, i):
    return right * (2 * i - 1) + 2 - i


def far_kernel(right_ref, middle_ref, flanks_ref, *refs):
    weights, misc, own = refs[:8], refs[8:13], refs[13:21]
    near_done_ref, e1_ref, ev1_ref, u1_ref, out_hbm = refs[21:26]
    a_ref, v_ref, e_ref, ev_ref, c_ref, d_ref, o_ref, k_ref, u_ref, out_ref, sems = refs[26:]
    left = right_ref[0]
    right = 1 - left
    copies = [pltpu.make_async_copy(near_done_ref, out_hbm.at[:, pl.ds(6 * left, 2)], sems.at[6])]
    copies[0].start()
    a, v, e, ev, c, d, o = own_planes(right, own)
    a, v, c, d, o = (x + [r.at[i] for i in range(3)] for x, r in zip((a, v, c, d, o), (a_ref, v_ref, c_ref, d_ref, o_ref)))
    e = [e1_ref] + e + [e_ref.at[0], e_ref.at[1]]
    ev = [ev1_ref] + ev + [ev_ref.at[0], ev_ref.at[1]]
    u = [u1_ref.at[1], u1_ref.at[0]] + [u_ref.at[i] for i in range(3)]
    load_side(middle_ref, flanks_ref, a[2:], v[2:], k_ref)

    def send(source, place):
        copies.append(
            pltpu.make_async_copy(out_ref.at[:, pl.ds(source, 1)], out_hbm.at[:, pl.ds(place, 1)], sems.at[source])
        )
        copies[-1].start()

    def emit(i, dot, bd, perm, back, m_ref):
        decode_finish(dot, far_place(right, i), bd, perm, back, m_ref, out_ref, 2 * i, send)

    w = Stages(right, weights, misc, (a, v, e, ev, c, d, o, u), k_ref, own[7], emit)
    e0 = w.e_dot(0)
    e1 = w.e_dot(1)
    l0 = w.e_finish(0, e0)
    e2 = w.e_dot(2)
    w.s_finish(0, l0)
    l1 = w.e_finish(1, e1)
    c0 = w.c_dot(0)
    w.s_finish(1, l1)
    l2 = w.e_finish(2, e2)
    w.c_finish(0, c0)
    c1 = w.c_dot(1)
    w.s_finish(2, l2)
    d0 = w.d_dot(0)
    w.c_finish(1, c1)
    c2 = w.c_dot(2)
    w.d_finish(0, d0)
    d1 = w.d_dot(1)
    w.c_finish(2, c2)
    d2 = w.d_dot(2)
    w.d_finish(1, d1)
    w.d_finish(2, d2)
    for copy in copies:
        copy.wait()


def vmem(n):
    return [pl.BlockSpec(memory_space=pltpu.VMEM)] * n


def hbm(n):
    return [pl.BlockSpec(memory_space=pltpu.HBM)] * n


def call(kernel, outs, ins, out_specs, scratch, mib, flops):
    return pl.pallas_call(
        kernel,
        out_shape=outs,
        in_specs=ins,
        out_specs=out_specs,
        scratch_shapes=scratch,
        compiler_params=pltpu.CompilerParams(vmem_limit_bytes=mib << 20),
        cost_estimate=pl.CostEstimate(flops=flops, bytes_accessed=10**6, transcendentals=0),
    )


def array(*shape, kind=BF16):
    return jax.ShapeDtypeStruct(shape, kind)


def buffers(shapes):
    return [pltpu.VMEM(s, d) for s, d in shapes]


def shifted(value, axis, step):
    peers = lax.axis_size(axis)
    return lax.ppermute(value, axis, [(i, i + step) for i in range(peers) if 0 <= i + step < peers])


def swapped(value, axis, first):
    peers = lax.axis_size(axis)
    pairs = []
    for i in range(first, peers - 1, 2):
        pairs += [(i, i + 1), (i + 1, i)]
    return lax.ppermute(value, axis, pairs)


def time_features(timestep, embed_width):
    halves = embed_width // 2
    freqs = jnp.exp(-math.log(10000.0) * jnp.arange(halves, dtype=F32) / halves)
    angles = timestep[0].astype(F32) * freqs
    return jnp.concatenate([jnp.sin(angles), jnp.cos(angles)]).astype(BF16)


SCALAR = [pl.BlockSpec(memory_space=pltpu.SMEM)]


def state(own, planes, encoded):
    return [
        (own + (2, 320, LANES), BF16),
        (own + (2, 320, LANES), BF16),
        (encoded + (2, 320, LANES), BF16),
        (encoded + (2, 192, LANES), BF16),
        (planes + (320, LANES), BF16),
        (planes + (256, LANES), BF16),
        (planes + (256, LANES), F32),
        ((2, 3, 64, LANES), F32),
    ]


LIFTED = (2, 192, LANES)


def arrays(shapes):
    return [array(*shape, kind=kind) for shape, kind in shapes]


def on_device(
    fine_in, voxel_mask, timestep, w_enc, b_enc, w_down, w_time, w_coarse, b_coarse, w_up, w_dec, b_dec
):
    own, up, down = call(
        pack_kernel,
        [array(OWN + ZC, LANES), array(SIDE_ROWS, LANES), array(SIDE_ROWS, LANES)],
        hbm(2),
        vmem(3),
        [pltpu.VMEM(fine_in.shape, BF16), pltpu.VMEM(voxel_mask.shape, jnp.int32), pltpu.SemaphoreType.DMA((5,))],
        12,
        10**9,
    )(pltpu.with_memory_space_constraint(fine_in, pltpu.HBM), pltpu.with_memory_space_constraint(voxel_mask, pltpu.HBM))
    low = shifted(up, "wide", 1)
    high = shifted(down, "wide", -1)

    odd = lax.axis_index("narrow").astype(jnp.int32)[None] & 1
    near_right = 1 - odd
    message = array(MIDDLE + ZC, LANES)
    middle, middle_near = call(edge_kernel, [message, message], SCALAR + vmem(1), vmem(2), [], 8, 10**8)(odd, own)
    middle = swapped(middle, "narrow", 1)
    middle_near = swapped(middle_near, "narrow", 0)

    embedded = time_features(timestep, w_time.shape[0])
    film = jnp.dot(embedded[None], w_time, preferred_element_type=F32)
    chans = w_down.shape[0]
    gains = 1.0 + film[:, :chans]
    shifts = film[:, chans:]
    taps = 27 * LANES
    enc_w, dec_w, down_w, perm, back, coarse_w = call(
        weights_kernel,
        [array(1024, 512), array(1536, 512), array(128, 256), array(512, 512), array(Z, LANES)]
        + [array(9 * LANES, 384)],
        vmem(4),
        vmem(6),
        buffers([((taps, 32), BF16), ((taps, 64), BF16), ((32, taps), F32), ((64, taps), F32)]),
        16,
        4 * 10**9,
    )(w_enc, w_dec, w_down, w_coarse)

    message = array(FLANKS + PAIR, LANES)
    flanks, near = call(
        mid_kernel, [message, message], SCALAR + vmem(4), vmem(2), buffers([((2, 4 * ZC, LANES), F32)]), 8, 10**8
    )(odd, low, high, down_w, gains)
    flanks = swapped(flanks, "narrow", 1)
    near = swapped(near, "narrow", 0)

    encoder = (enc_w, b_enc[None], down_w, gains, shifts)
    mine = call(own_kernel, arrays(state((4,), (2,), (2,))), vmem(8), vmem(8), [], 12, 2 * 10**9)(
        own, low, high, *encoder
    )
    some = encoder + (coarse_w, b_coarse[None], w_up, voxel_mask, dec_w, b_dec[None], perm, back) + tuple(mine)
    pair = array(fine_in.shape[0], 2, *fine_in.shape[2:])
    near_done, e1, ev1, u1 = call(
        near_kernel,
        [pair] + arrays(state((), (), ())[2:4] + [((2,) + LIFTED, BF16)]),
        SCALAR + vmem(23),
        vmem(4),
        buffers(state((3,), (3,), (1,)) + [((1,) + LIFTED, BF16)]),
        24,
        4 * 10**9,
    )(near_right, middle_near, near, *some)
    rest = pltpu.VMEM((fine_in.shape[0], 6) + fine_in.shape[2:], BF16)
    return call(
        far_kernel,
        [array(*fine_in.shape)],
        SCALAR + vmem(27),
        hbm(1),
        buffers(state((3,), (3,), (2,)) + [((3,) + LIFTED, BF16)]) + [rest, pltpu.SemaphoreType.DMA((7,))],
        24,
        5 * 10**9,
    )(near_right, middle, flanks, *some, near_done, e1, ev1, u1)[0]


def solution(mesh):
    field = P(None, "narrow", "wide", None)
    return jax.shard_map(
        on_device,
        mesh=mesh,
        in_specs=(field, P("narrow", "wide", None)) + (P(),) * 10,
        out_specs=field,
        check_vma=False,
    )
```

```python
import math

import jax
import jax.numpy as jnp
from jax import lax
from jax.experimental import pallas as pl
from jax.experimental.pallas import tpu as pltpu
from jax.sharding import PartitionSpec as P


F32 = jnp.float32
BF16 = jnp.bfloat16
LANES = 128
ZC = 40
Z = 80
CH = 32
BITS = (0, 1)


def nn(a, b):
    return lax.dot_general(a, b, (((1,), (0,)), ((), ())), preferred_element_type=F32)


def nt(a, b):
    return lax.dot_general(a, b, (((1,), (1,)), ((), ())), preferred_element_type=F32)


def iota(shape, dim):
    return lax.broadcasted_iota(jnp.int32, shape, dim)


PAIR = 2 * ZC
OWN = 16 * PAIR
SIDE = 8 * PAIR
SIDE_MASK = SIDE + 4 * ZC
SIDE_ROWS = SIDE_MASK + ZC
PLANE = 9 * PAIR
HALF = 5 * PAIR
MASKS = 3 * ZC
MIDDLE = 10 * PAIR
FLANKS = 13 * PAIR


def one_where(truth):
    return truth.astype(F32).astype(BF16)


def unpick(rows, cols):
    row = iota((rows, cols), 0)
    return one_where(jnp.where(row < ZC, 2 * row, 2 * row - (Z - 1)) == iota((rows, cols), 1))


def low_b(rows):
    return (iota((rows, LANES), 1) & 32) == 0


def stacked(*parts):
    return jnp.concatenate(parts, axis=0)


def beside(*parts):
    return jnp.concatenate(parts, axis=1)


def pack_kernel(x_hbm, m_hbm, own_ref, up_ref, dn_ref, x_ref, m_ref, sems):
    copies = [pltpu.make_async_copy(m_hbm, m_ref, sems.at[4])]
    for cx in range(4):
        copies.append(pltpu.make_async_copy(x_hbm.at[:, pl.ds(2 * cx, 2)], x_ref.at[:, pl.ds(2 * cx, 2)], sems.at[cx]))
    for copy in copies:
        copy.start()
    sel = unpick(Z, Z)
    src = iota((512, LANES), 0)
    y = src & 7
    goal = ((y >> 1) << 7) + ((src >> 8) << 6) + ((y & 1) << 5) + ((src >> 3) & 31) - iota((512, LANES), 1)
    perm = [one_where(goal == LANES * i) for i in range(4)]
    copies[0].wait()
    mask = (m_ref[...] > 0).astype(F32).reshape(64, Z).astype(BF16)
    cols = nt(sel, mask)
    cols = beside(cols[:ZC], cols[ZC:]).astype(BF16)
    own_ref[OWN : OWN + ZC] = cols
    up_ref[SIDE_MASK:SIDE_ROWS] = cols
    dn_ref[SIDE_MASK:SIDE_ROWS] = cols
    sides = [[], []]
    for cx in range(4):
        copies[1 + cx].wait()
        for a in BITS:
            x = 2 * cx + a
            tile = x_ref[:, x].astype(F32)
            tile = jnp.where(m_ref[x][None] > 0, tile, 0.0)
            sides[a].append(nt(sel, tile.reshape(8 * CH, Z).astype(BF16)).astype(BF16))
    both = beside(stacked(*sides[0]), stacked(*sides[1]))
    cols = [nn(both, perm[cy]) for cy in range(4)]
    ups, downs = [], []
    for cx in range(4):
        col = [v[Z * cx : Z * cx + Z] for v in cols]
        for cz in BITS:
            z = slice(ZC * cz, ZC * cz + ZC)
            first = stacked(col[0][z], col[1][z]).astype(BF16)
            second = stacked(col[2][z], col[3][z]).astype(BF16)
            own_ref[pl.ds((4 * cx + 2 * cz) * PAIR, PAIR)] = first
            own_ref[pl.ds((4 * cx + 2 * cz + 1) * PAIR, PAIR)] = second
            dn_ref[pl.ds((2 * cx + cz) * PAIR, PAIR)] = first
            up_ref[pl.ds((2 * cx + cz) * PAIR, PAIR)] = second
        ups.append(jnp.where(low_b(ZC), pltpu.roll(col[1][ZC:], LANES - 32, 1), col[1][:ZC]))
        downs.append(jnp.where(low_b(ZC), col[2][:ZC], pltpu.roll(col[2][ZC:], 32, 1)))
        if cx % 2 == 1:
            at = pl.ds(SIDE + (cx // 2) * PAIR, PAIR)
            up_ref[at] = stacked(*ups[-2:]).astype(BF16)
            dn_ref[at] = stacked(*downs[-2:]).astype(BF16)


def part(x, size):
    return pl.ds(pl.multiple_of(x * size, size), size)


def folded(pieces, right):
    lane_a = iota(pieces[0].shape, 1) >> 6
    even, odd = (v.astype(F32) for v in pieces)
    return jnp.where(lane_a == right, even, pltpu.roll(odd, 64, 1)).astype(BF16)


def edge_kernel(odd_ref, own_ref, out_ref):
    right = odd_ref[0]
    for i, x in enumerate((3 * right, 1 + right)):
        out_ref[4 * PAIR * i : 4 * PAIR * (i + 1)] = own_ref[part(x, 4 * PAIR)]
    x = 2 - right
    pieces = [own_ref[pl.ds(pl.multiple_of((4 * x + 2 * cz) * PAIR, PAIR), 2 * PAIR)] for cz in BITS]
    out_ref[8 * PAIR : 10 * PAIR] = folded(pieces, right)
    out_ref[MIDDLE : MIDDLE + ZC] = own_ref[OWN : OWN + ZC]


def mid_kernel(odd_ref, own_ref, low_ref, high_ref, tie_ref, tie2_ref, far_ref, near_ref, ends_ref):
    ends_ref[0] = low_ref[SIDE:SIDE_MASK].astype(F32)
    ends_ref[1] = high_ref[SIDE:SIDE_MASK].astype(F32)

    def layer(x, cz):
        return (
            low_ref[pl.ds(pl.multiple_of(x * 2 * PAIR + cz * PAIR, PAIR), PAIR)],
            own_ref[pl.ds(pl.multiple_of(x * 4 * PAIR + 2 * cz * PAIR, PAIR), 2 * PAIR)],
            high_ref[pl.ds(pl.multiple_of(x * 2 * PAIR + cz * PAIR, PAIR), PAIR)],
        )

    def ends(x):
        at = part(x, ZC)
        return stacked(ends_ref[0, at], ends_ref[1, at]).astype(BF16)

    right = 1 - odd_ref[0]
    for i, x in enumerate((3 * right, 1 + right)):
        at = i * PLANE
        for cz in BITS:
            low, own, high = layer(x, cz)
            near_ref[at : at + PAIR] = low
            near_ref[at + PAIR : at + 3 * PAIR] = own
            near_ref[at + 3 * PAIR : at + 4 * PAIR] = high
            at = at + 4 * PAIR
        near_ref[at : at + PAIR] = ends(x)
    x, at = 2 - right, 2 * PLANE
    low, own, high = zip(*[layer(x, cz) for cz in BITS])
    near_ref[at : at + PAIR] = folded(low, right)
    near_ref[at + PAIR : at + 3 * PAIR] = folded(own, right)
    near_ref[at + 3 * PAIR : at + 4 * PAIR] = folded(high, right)
    near_ref[at + 4 * PAIR : at + HALF] = ends(x)
    masks = [low_ref[SIDE_MASK:SIDE_ROWS], own_ref[OWN : OWN + ZC], high_ref[SIDE_MASK:SIDE_ROWS]]
    near_ref[at + HALF : at + HALF + MASKS] = stacked(*[m.astype(F32) for m in masks]).astype(BF16)
    right = odd_ref[0]
    for i, x in enumerate((3 * right, 1 + right)):
        at = 5 * PAIR * i
        far_ref[at : at + 2 * PAIR] = low_ref[part(x, 2 * PAIR)]
        far_ref[at + 2 * PAIR : at + 4 * PAIR] = high_ref[part(x, 2 * PAIR)]
        far_ref[at + 4 * PAIR : at + 5 * PAIR] = ends(x)
    x, at = 2 - right, 10 * PAIR
    low, own, high = zip(*[layer(x, cz) for cz in BITS])
    far_ref[at : at + PAIR] = folded(low, right)
    far_ref[at + PAIR : at + 2 * PAIR] = folded(high, right)
    far_ref[at + 2 * PAIR : at + 3 * PAIR] = ends(x)
    masks = [low_ref[SIDE_MASK:SIDE_ROWS], high_ref[SIDE_MASK:SIDE_ROWS]]
    far_ref[FLANKS : FLANKS + PAIR] = stacked(*[m.astype(F32) for m in masks]).astype(BF16)


def tap_of(out_bit, in_bit, far):
    if far:
        return 2 * (1 - in_bit) if out_bit != in_bit else None
    return in_bit - out_bit + 1


def placed(w_ref, rows, taps, group):
    total = jnp.zeros((CH, LANES), F32)
    for g, tap in enumerate(taps):
        if tap is not None:
            total = jnp.where(group == g, w_ref[rows : rows + CH, LANES * tap : LANES * tap + LANES], total)
    return total


def block(w_ref, rows, group, far_x, far_y, a_in, b_in, cz_in, shifted, cz_out):
    if shifted:
        tz = None
        if cz_out == 0 and cz_in == 1:
            tz = 0
        if cz_out == 1 and cz_in == 0:
            tz = 2
    else:
        tz = cz_in - cz_out + 1
    taps = []
    for a_out in BITS:
        for b_out in BITS:
            tx = tap_of(a_out, a_in, far_x)
            ty = tap_of(b_out, b_in, far_y)
            taps.append(None if tx is None or ty is None or tz is None else 9 * tx + 3 * ty + tz)
    return placed(w_ref, rows, taps, group)


KINDS = ((0, 0), (1, 0), (0, 1), (1, 1))


def weights_kernel(
    we_ref, wd_ref, wn_ref, wc_ref, oe_ref, od_ref, on_ref, op_ref, ob_ref, oc_ref, re_ref, rd_ref, te_ref, td_ref
):
    for tap in range(27):
        for g in range(4):
            at = LANES * tap + CH * g
            re_ref[at : at + CH] = we_ref[tap]
            rd_ref[at : at + CH] = wd_ref[tap]
    one = (iota((CH, CH), 0) == iota((CH, CH), 1)).astype(F32).astype(BF16)
    te_ref[...] = nt(one, re_ref[...])
    one = (iota((2 * CH, 2 * CH), 0) == iota((2 * CH, 2 * CH), 1)).astype(F32).astype(BF16)
    td_ref[...] = nt(one, rd_ref[...])
    one = one_where(iota((LANES, LANES), 0) == iota((LANES, LANES), 1))
    for i in range(9):
        oc_ref[LANES * i : LANES * i + LANES] = nt(one, wc_ref[3 * i : 3 * i + 3].reshape(384, LANES)).astype(BF16)
    group = iota((CH, LANES), 1) >> 5
    for w_ref, o_ref in ((te_ref, oe_ref), (td_ref, od_ref)):
        for t, (fx, fy) in enumerate(KINDS):
            for cz in BITS:
                for a in BITS:
                    for b in BITS:
                        base = 256 * t + 128 * cz + 64 * a + 32 * b
                        for s in BITS:
                            for co in BITS:
                                v = block(w_ref, 0, group, fx, fy, a, b, cz, s, co)
                                o_ref[base : base + CH, 256 * s + 128 * co : 256 * s + 128 * co + LANES] = v.astype(BF16)
    for t, (fx, fy) in enumerate(KINDS):
        for a in BITS:
            for b in BITS:
                base = 1024 + 128 * t + 64 * a + 32 * b
                for s in BITS:
                    for co in BITS:
                        v = block(td_ref, CH, group, fx, fy, a, b, 0, s, co)
                        v = v + block(td_ref, CH, group, fx, fy, a, b, 1, s, co)
                        od_ref[base : base + CH, 256 * s + 128 * co : 256 * s + 128 * co + LANES] = v.astype(BF16)
    k = iota((8 * CH, LANES), 0)
    goal = (((k >> 5) & 1) << 7) + ((k >> 6) << 5) + (k & 31) - iota((8 * CH, LANES), 1)
    perm = jnp.concatenate([(goal == LANES * i).astype(F32).astype(BF16) for i in BITS], axis=1)
    on_ref[...] = nn(wn_ref[...], perm).astype(BF16)
    src = iota((512, LANES), 0)
    goal = (((src >> 6) & 1) << 8) + ((src & 31) << 3) + ((src >> 7) << 1) + ((src >> 5) & 1) - iota((512, LANES), 1)
    op_ref[...] = beside(*[one_where(goal == LANES * i) for i in range(4)])
    column = iota((Z, LANES), 1)
    goal = jnp.where(column < ZC, 2 * column, jnp.where(column < Z, 2 * column - (Z - 1), -1))
    ob_ref[...] = one_where(goal == iota((Z, LANES), 0))


def moved(t, amount, edge):
    rows = t.shape[0]
    return jnp.where(edge, 0.0, pltpu.roll(t, amount % rows, 0))


def depth_of(rows):
    return iota((rows, LANES), 0) % ZC


def quad(bias):
    return beside(bias, bias, bias, bias)


def put_plane(a_ref, v_ref, layers, ends):
    y0, y9 = ends[:ZC].astype(F32), ends[ZC:].astype(F32)
    for cz in BITS:
        a_ref[cz] = layers[cz].astype(BF16)
        f = layers[cz].astype(F32)
        if cz == 1:
            y0, y9 = pltpu.roll(y0, 32, 1), pltpu.roll(y9, LANES - 32, 1)
        f = stacked(y0, f, y9)
        v_ref[cz] = jnp.where(low_b(320), f[PAIR:], f[:320]).astype(BF16)


def load_own(own_ref, low_ref, high_ref, a_ref, v_ref):
    low_ends = low_ref[SIDE:SIDE_MASK].astype(F32)
    high_ends = high_ref[SIDE:SIDE_MASK].astype(F32)
    for x in range(4):
        layers = []
        for cz in BITS:
            at = (2 * x + cz) * PAIR
            mine = (4 * x + 2 * cz) * PAIR
            layers.append(
                stacked(low_ref[at : at + PAIR], own_ref[mine : mine + 2 * PAIR], high_ref[at : at + PAIR])
            )
        z = slice(ZC * x, ZC * x + ZC)
        put_plane(a_ref.at[x], v_ref.at[x], layers, stacked(low_ends[z], high_ends[z]))


def load_full(ref, at, a_ref, v_ref):
    layers = [ref[at + 320 * cz : at + 320 * cz + 320] for cz in BITS]
    put_plane(a_ref, v_ref, layers, ref[at + 640 : at + PLANE].astype(F32))


def load_half(ref, at, a_ref, v_ref):
    both = ref[at : at + 320].astype(F32)
    put_plane(a_ref, v_ref, [both, pltpu.roll(both, 64, 1)], ref[at + 320 : at + HALF].astype(F32))


def load_far(mid_ref, flank_ref, a, v, k_ref):
    for i in range(2):
        mine, at = 4 * PAIR * i, 5 * PAIR * i
        layers = []
        for cz in BITS:
            low, high = at + PAIR * cz, at + PAIR * (2 + cz)
            own = mine + 2 * PAIR * cz
            layers.append(
                stacked(flank_ref[low : low + PAIR], mid_ref[own : own + 2 * PAIR], flank_ref[high : high + PAIR])
            )
        put_plane(a[i], v[i], layers, flank_ref[at + 4 * PAIR : at + 5 * PAIR].astype(F32))
    at = 10 * PAIR
    both = stacked(
        flank_ref[at : at + PAIR], mid_ref[8 * PAIR : 10 * PAIR], flank_ref[at + PAIR : at + 2 * PAIR]
    ).astype(F32)
    put_plane(a[2], v[2], [both, pltpu.roll(both, 64, 1)], flank_ref[at + 2 * PAIR : at + 3 * PAIR].astype(F32))
    masks = flank_ref[FLANKS : FLANKS + PAIR].astype(F32)
    load_masks([masks[:ZC], mid_ref[MIDDLE : MIDDLE + ZC], masks[ZC:]], k_ref)


def load_masks(parts, k_ref):
    for by, k in enumerate(parts):
        k = k.astype(F32)
        m = jnp.maximum(k, pltpu.roll(k, LANES - 1, 1))
        m = jnp.maximum(m, pltpu.roll(m, LANES - 8, 1))
        m = jnp.maximum(m, pltpu.roll(m, LANES - 64, 1))
        k_ref[0, by, 0:ZC] = k
        k_ref[1, by, 0:ZC] = m


def load_side_masks(ref, at, k_ref):
    masks = ref[at : at + MASKS].astype(F32)
    load_masks([masks[ZC * i : ZC * i + ZC] for i in range(3)], k_ref)


def spread(k, index):
    return stacked(*[jnp.take_along_axis(k[8 * i : 8 * i + 8], index, axis=1, mode="promise_in_bounds") for i in range(5)])


def silu(v):
    half = 0.5 * v
    return half + half * jnp.tanh(half)


def joined_x(planes, p, part, right, rows):
    count = rows.stop - rows.start
    takes_next = one_where((1 - (iota((count, LANES), 1) >> 6)) == right) > 0.5
    return jnp.where(takes_next, planes[p + 1][part, rows], planes[p - 1][part, rows])


def spans(planes, p, parts, right, rows):
    return [planes[p][part, rows] for part in parts] + [joined_x(planes, p, part, right, rows) for part in parts]


def encode_dot(p, right, a, v, we_ref):
    every = slice(0, 320)
    return nn(beside(*spans(a, p, BITS, right, every), *spans(v, p, BITS, right, every)), we_ref[...])


def encode_finish(o, lx, k_ref, e_ref, ev_ref, be, wn_ref):
    z8 = depth_of(320)
    first, last = z8 == 0, z8 == ZC - 1
    lane = iota((8, LANES), 1)
    lane_at = 8 * (lane >> 6) + ((lane >> 5) & 1) + 16 * lx
    pre = (
        o[:, 0:128] + moved(o[:, 256:384], 1, first) + be,
        o[:, 128:256] + moved(o[:, 384:512], -1, last) + be,
    )
    enc = []
    for cz in BITS:
        active = []
        for yi in range(1, 9):
            by, ly = (yi + 1) >> 2, (yi + 1) & 3
            active.append(spread(k_ref[0, by, 0:ZC], lane_at + (64 * cz + 2 * ly)))
        e = jnp.where(stacked(*active) > 0.5, silu(pre[cz]), 0.0)
        enc.append(e.astype(BF16))
        if e_ref is None:
            continue
        e_ref[cz] = enc[cz]
        ev_ref[cz, 0:160] = jnp.where(low_b(160), e[120:280], e[40:200]).astype(BF16)
    return nt(beside(*enc), wn_ref[...])


def strided_finish(lifted, lx, k_ref, c_ref, d_ref, o_ref, gain, shift):
    where = iota((8, LANES), 1) * 0 + 16 * lx
    on = []
    for yi in range(1, 9):
        by, ly = (yi + 1) >> 2, (yi + 1) & 3
        on.append(spread(k_ref[1, by, 0:ZC], where + 2 * ly))
    on = stacked(*on)
    c = jnp.where(on > 0.5, silu(lifted * gain + shift), 0.0)
    c_ref[...] = c.astype(BF16)
    d_ref[0:240] = c[40:280].astype(BF16)
    o_ref[0:240] = on[40:280]


def coarse_dot(q, right, c, d, wc_ref):
    lhs, rhs = [], []
    for i in range(3):
        lhs += [c[q - 1 + i][0:240], d[q - 1 + i][0:240], c[q - 1 + i][80:320]]
        first = 768 * (1 - right) + 384 * i * (2 * right - 1)
        rhs.append(wc_ref[pl.ds(pl.multiple_of(first, 384), 384)])
    return nn(beside(*lhs), stacked(*rhs))


def coarse_finish(p, o_ref, u_ref, bc, wu_ref):
    z6 = depth_of(240)
    first, last = z6 == 0, z6 == ZC - 1
    s = p[:, 128:256] + moved(p[:, 0:128], 1, first) + moved(p[:, 256:384], -1, last) + bc
    act = jnp.where(o_ref[0:240] > 0.5, silu(s), 0.0).astype(BF16)
    u = nt(act, stacked(*([wu_ref[...]] * 4)))
    u_ref[0, 0:160] = u[40:200].astype(BF16)
    u_ref[1, 0:160] = jnp.where(low_b(160), u[80:240], u[0:160]).astype(BF16)


def decode_dot(p, right, e, ev, u, wd_ref):
    mid, every = slice(80, 240), slice(0, 160)
    lhs = spans(e, p, BITS, right, mid) + spans(ev, p, BITS, right, every)
    for v in BITS:
        lhs += spans(u, p, (v,), right, every)
    return nn(beside(*lhs), wd_ref[...])


def decode_finish(o, xo, bd, perm, back, m_ref, out_ref, at, send=None):
    z4 = depth_of(160)
    first, last = z4 == 0, z4 == ZC - 1
    d0 = o[:, 0:128] + moved(o[:, 256:384], 1, first) + bd
    d1 = o[:, 128:256] + moved(o[:, 384:512], -1, last) + bd
    d = [beside(*[v[ZC * y : ZC * y + ZC] for y in range(4)]) for v in (d0, d1)]
    d = stacked(*d, jnp.zeros((LANES - Z, 512), F32)).astype(BF16)
    d = nn(nn(back, d).astype(BF16), perm)
    d = stacked(d, jnp.zeros((LANES - Z, 512), F32))
    for a in BITS:
        t = jnp.transpose(d[:, 256 * a : 256 * a + 256])[:, :Z].reshape(CH, 8, Z)
        out_ref[:, at + a] = jnp.where(m_ref[2 * xo + a][None] > 0, t, 0.0).astype(BF16)
        if send is not None:
            send(at + a, 2 * xo + a)


def own_kernel(
    own_ref, low_ref, high_ref, we_ref, be_ref, wn_ref, gain_ref, shift_ref, a_ref, v_ref, e_ref, ev_ref, c_ref, d_ref,
    o_ref, k_ref
):
    load_own(own_ref, low_ref, high_ref, a_ref, v_ref)
    load_masks((low_ref[SIDE_MASK:SIDE_ROWS], own_ref[OWN : OWN + ZC], high_ref[SIDE_MASK:SIDE_ROWS]), k_ref)
    be = quad(be_ref[...])
    a, v = ([ref.at[x] for x in range(4)] for ref in (a_ref, v_ref))
    dots = [encode_dot(1 + i, 1, a, v, we_ref) for i in range(2)]
    lifted = [encode_finish(dots[i], 1 + i, k_ref, e_ref.at[i], ev_ref.at[i], be, wn_ref) for i in range(2)]
    for i in range(2):
        strided_finish(
            lifted[i], 1 + i, k_ref, c_ref.at[i], d_ref.at[i], o_ref.at[i], gain_ref[...], shift_ref[...]
        )


def own_planes(right, own):
    two = [right * (1 + 2 * i) + 1 - i for i in range(2)]
    one = [right * (2 * i - 1) + 1 - i for i in range(2)]
    a, v = ([ref.at[at] for at in two] for ref in own[0:2])
    e, ev, c, d, o = ([ref.at[at] for at in one] for ref in own[2:7])
    return a, v, e, ev, c, d, o


class Stages:
    def __init__(self, right, weights, misc, planes, side_k, own_k, emit):
        self.right, self.planes, self.emit = right, planes, emit
        self.we, be, self.wn, gain, shift, self.wc, bc, self.wu = weights
        self.m, self.wd, bd, perm, back = misc
        self.be, self.bd = quad(be[...]), quad(bd[...])
        self.gain, self.shift, self.bc = gain[...], shift[...], bc[...]
        self.perm, self.back = perm[...], back[...]
        self.k = (own_k, side_k, side_k)
        self.lx = (3 * right, 3 - 3 * right, 2 - right)

    def e_dot(self, i):
        return encode_dot(1 + i, self.right, self.planes[0], self.planes[1], self.we)

    def e_finish(self, i, dot):
        e, ev = self.planes[2], self.planes[3]
        at = (e[3 + i], ev[3 + i]) if i < 2 else (None, None)
        return encode_finish(dot, self.lx[i], self.k[i], *at, self.be, self.wn)

    def s_finish(self, i, lifted):
        c, d, o = self.planes[4:7]
        strided_finish(lifted, self.lx[i], self.k[i], c[2 + i], d[2 + i], o[2 + i], self.gain, self.shift)

    def c_dot(self, i):
        return coarse_dot(1 + i, self.right, self.planes[4], self.planes[5], self.wc)

    def c_finish(self, i, dot):
        coarse_finish(dot, self.planes[6][1 + i], self.planes[7][2 + i], self.bc, self.wu)

    def d_dot(self, i):
        return decode_dot(1 + i, self.right, self.planes[2], self.planes[3], self.planes[7], self.wd)

    def d_finish(self, i, dot):
        self.emit(i, dot, self.bd, self.perm, self.back, self.m)


def near_kernel(right_ref, side_ref, *refs):
    weights, misc, own = refs[:8], refs[8:13], refs[13:21]
    done_ref, e1_ref, ev1_ref, u1_ref = refs[21:25]
    a_ref, v_ref, e_ref, ev_ref, c_ref, d_ref, o_ref, k_ref, u_ref = refs[25:]
    right = right_ref[0]
    a, v, e, ev, c, d, o = own_planes(right, own)
    a, v, c, d, o = (x + [r.at[i] for i in range(3)] for x, r in zip((a, v, c, d, o), (a_ref, v_ref, c_ref, d_ref, o_ref)))
    e, ev = [None] + e + [e1_ref, e_ref.at[0]], [None] + ev + [ev1_ref, ev_ref.at[0]]
    u = [None, None, u1_ref.at[0], u1_ref.at[1], u_ref.at[0]]
    for i in range(2):
        load_full(side_ref, i * PLANE, a[2 + i], v[2 + i])
    load_half(side_ref, 2 * PLANE, a[4], v[4])
    load_side_masks(side_ref, 2 * PLANE + HALF, k_ref)

    def emit(i, dot, bd, perm, back, m_ref):
        decode_finish(dot, 3 * right, bd, perm, back, m_ref, done_ref, 0)

    w = Stages(right, weights, misc, (a, v, e, ev, c, d, o, u), k_ref, own[7], emit)
    e0 = w.e_dot(0)
    e1 = w.e_dot(1)
    l0 = w.e_finish(0, e0)
    e2 = w.e_dot(2)
    w.s_finish(0, l0)
    l1 = w.e_finish(1, e1)
    c0 = w.c_dot(0)
    w.s_finish(1, l1)
    l2 = w.e_finish(2, e2)
    w.c_finish(0, c0)
    c1 = w.c_dot(1)
    w.s_finish(2, l2)
    w.c_finish(1, c1)
    c2 = w.c_dot(2)
    w.c_finish(2, c2)
    w.d_finish(2, w.d_dot(2))


def far_place(right, i):
    return right * (2 * i - 1) + 2 - i


def far_kernel(right_ref, middle_ref, flanks_ref, *refs):
    weights, misc, own = refs[:8], refs[8:13], refs[13:21]
    near_done_ref, e1_ref, ev1_ref, u1_ref, out_hbm = refs[21:26]
    a_ref, v_ref, e_ref, ev_ref, c_ref, d_ref, o_ref, k_ref, u_ref, out_ref, sems = refs[26:]
    left = right_ref[0]
    right = 1 - left
    copies = [pltpu.make_async_copy(near_done_ref, out_hbm.at[:, pl.ds(6 * left, 2)], sems.at[6])]
    copies[0].start()
    a, v, e, ev, c, d, o = own_planes(right, own)
    a, v, c, d, o = (x + [r.at[i] for i in range(3)] for x, r in zip((a, v, c, d, o), (a_ref, v_ref, c_ref, d_ref, o_ref)))
    e = [e1_ref] + e + [e_ref.at[0], e_ref.at[1]]
    ev = [ev1_ref] + ev + [ev_ref.at[0], ev_ref.at[1]]
    u = [u1_ref.at[1], u1_ref.at[0]] + [u_ref.at[i] for i in range(3)]
    load_far(middle_ref, flanks_ref, a[2:], v[2:], k_ref)

    def send(source, place):
        copies.append(
            pltpu.make_async_copy(out_ref.at[:, pl.ds(source, 1)], out_hbm.at[:, pl.ds(place, 1)], sems.at[source])
        )
        copies[-1].start()

    def emit(i, dot, bd, perm, back, m_ref):
        decode_finish(dot, far_place(right, i), bd, perm, back, m_ref, out_ref, 2 * i, send)

    w = Stages(right, weights, misc, (a, v, e, ev, c, d, o, u), k_ref, own[7], emit)
    e0 = w.e_dot(0)
    e1 = w.e_dot(1)
    l0 = w.e_finish(0, e0)
    e2 = w.e_dot(2)
    w.s_finish(0, l0)
    l1 = w.e_finish(1, e1)
    c0 = w.c_dot(0)
    w.s_finish(1, l1)
    l2 = w.e_finish(2, e2)
    w.c_finish(0, c0)
    c1 = w.c_dot(1)
    w.s_finish(2, l2)
    d0 = w.d_dot(0)
    w.c_finish(1, c1)
    c2 = w.c_dot(2)
    w.d_finish(0, d0)
    d1 = w.d_dot(1)
    w.c_finish(2, c2)
    d2 = w.d_dot(2)
    w.d_finish(1, d1)
    w.d_finish(2, d2)
    for copy in copies:
        copy.wait()


def vmem(n):
    return [pl.BlockSpec(memory_space=pltpu.VMEM)] * n


def hbm(n):
    return [pl.BlockSpec(memory_space=pltpu.HBM)] * n


def call(kernel, outs, ins, out_specs, scratch, mib, flops):
    return pl.pallas_call(
        kernel,
        out_shape=outs,
        in_specs=ins,
        out_specs=out_specs,
        scratch_shapes=scratch,
        compiler_params=pltpu.CompilerParams(vmem_limit_bytes=mib << 20),
        cost_estimate=pl.CostEstimate(flops=flops, bytes_accessed=10**6, transcendentals=0),
    )


def array(*shape, kind=BF16):
    return jax.ShapeDtypeStruct(shape, kind)


def buffers(shapes):
    return [pltpu.VMEM(s, d) for s, d in shapes]


def shifted(value, axis, step):
    peers = lax.axis_size(axis)
    return lax.ppermute(value, axis, [(i, i + step) for i in range(peers) if 0 <= i + step < peers])


def swapped(value, axis, first):
    peers = lax.axis_size(axis)
    pairs = []
    for i in range(first, peers - 1, 2):
        pairs += [(i, i + 1), (i + 1, i)]
    return lax.ppermute(value, axis, pairs)


def time_features(timestep, embed_width):
    halves = embed_width // 2
    freqs = jnp.exp(-math.log(10000.0) * jnp.arange(halves, dtype=F32) / halves)
    angles = timestep[0].astype(F32) * freqs
    return jnp.concatenate([jnp.sin(angles), jnp.cos(angles)]).astype(BF16)


SCALAR = [pl.BlockSpec(memory_space=pltpu.SMEM)]


def state(own, planes, encoded):
    return [
        (own + (2, 320, LANES), BF16),
        (own + (2, 320, LANES), BF16),
        (encoded + (2, 320, LANES), BF16),
        (encoded + (2, 192, LANES), BF16),
        (planes + (320, LANES), BF16),
        (planes + (256, LANES), BF16),
        (planes + (256, LANES), F32),
        ((2, 3, 64, LANES), F32),
    ]


LIFTED = (2, 192, LANES)


def arrays(shapes):
    return [array(*shape, kind=kind) for shape, kind in shapes]


def on_device(
    fine_in, voxel_mask, timestep, w_enc, b_enc, w_down, w_time, w_coarse, b_coarse, w_up, w_dec, b_dec
):
    own, up, down = call(
        pack_kernel,
        [array(OWN + ZC, LANES), array(SIDE_ROWS, LANES), array(SIDE_ROWS, LANES)],
        hbm(2),
        vmem(3),
        [pltpu.VMEM(fine_in.shape, BF16), pltpu.VMEM(voxel_mask.shape, jnp.int32), pltpu.SemaphoreType.DMA((5,))],
        12,
        10**9,
    )(pltpu.with_memory_space_constraint(fine_in, pltpu.HBM), pltpu.with_memory_space_constraint(voxel_mask, pltpu.HBM))
    low = shifted(up, "wide", 1)
    high = shifted(down, "wide", -1)

    odd = lax.axis_index("narrow").astype(jnp.int32)[None] & 1
    near_right = 1 - odd
    middle = call(edge_kernel, [array(MIDDLE + ZC, LANES)], SCALAR + vmem(1), vmem(1), [], 8, 10**8)(odd, own)[0]
    middle = swapped(middle, "narrow", 1)

    embedded = time_features(timestep, w_time.shape[0])
    film = jnp.dot(embedded[None], w_time, preferred_element_type=F32)
    chans = w_down.shape[0]
    gains = 1.0 + film[:, :chans]
    shifts = film[:, chans:]
    taps = 27 * LANES
    enc_w, dec_w, down_w, perm, back, coarse_w = call(
        weights_kernel,
        [array(1024, 512), array(1536, 512), array(128, 256), array(512, 512), array(Z, LANES)]
        + [array(9 * LANES, 384)],
        vmem(4),
        vmem(6),
        buffers([((taps, 32), BF16), ((taps, 64), BF16), ((32, taps), F32), ((64, taps), F32)]),
        16,
        4 * 10**9,
    )(w_enc, w_dec, w_down, w_coarse)

    flanks, near = call(
        mid_kernel,
        [array(FLANKS + PAIR, LANES), array(2 * PLANE + HALF + MASKS, LANES)],
        SCALAR + vmem(5),
        vmem(2),
        buffers([((2, 4 * ZC, LANES), F32)]),
        8,
        10**8,
    )(odd, own, low, high, down_w, gains)
    flanks = swapped(flanks, "narrow", 1)
    near = swapped(near, "narrow", 0)

    encoder = (enc_w, b_enc[None], down_w, gains, shifts)
    mine = call(own_kernel, arrays(state((4,), (2,), (2,))), vmem(8), vmem(8), [], 12, 2 * 10**9)(
        own, low, high, *encoder
    )
    some = encoder + (coarse_w, b_coarse[None], w_up, voxel_mask, dec_w, b_dec[None], perm, back) + tuple(mine)
    pair = array(fine_in.shape[0], 2, *fine_in.shape[2:])
    near_done, e1, ev1, u1 = call(
        near_kernel,
        [pair] + arrays(state((), (), ())[2:4] + [((2,) + LIFTED, BF16)]),
        SCALAR + vmem(22),
        vmem(4),
        buffers(state((3,), (3,), (1,)) + [((1,) + LIFTED, BF16)]),
        24,
        4 * 10**9,
    )(near_right, near, *some)
    rest = pltpu.VMEM((fine_in.shape[0], 6) + fine_in.shape[2:], BF16)
    return call(
        far_kernel,
        [array(*fine_in.shape)],
        SCALAR + vmem(27),
        hbm(1),
        buffers(state((3,), (3,), (2,)) + [((3,) + LIFTED, BF16)]) + [rest, pltpu.SemaphoreType.DMA((7,))],
        24,
        5 * 10**9,
    )(near_right, middle, flanks, *some, near_done, e1, ev1, u1)[0]


def solution(mesh):
    field = P(None, "narrow", "wide", None)
    return jax.shard_map(
        on_device,
        mesh=mesh,
        in_specs=(field, P("narrow", "wide", None)) + (P(),) * 10,
        out_specs=field,
        check_vma=False,
    )
```

```python
import math

import jax
import jax.numpy as jnp
from jax import lax
from jax.experimental import pallas as pl
from jax.experimental.pallas import tpu as pltpu
from jax.sharding import PartitionSpec as P


F32 = jnp.float32
BF16 = jnp.bfloat16
LANES = 128
ZC = 40
Z = 80
CH = 32
BITS = (0, 1)


def nn(a, b):
    return lax.dot_general(a, b, (((1,), (0,)), ((), ())), preferred_element_type=F32)


def nt(a, b):
    return lax.dot_general(a, b, (((1,), (1,)), ((), ())), preferred_element_type=F32)


def iota(shape, dim):
    return lax.broadcasted_iota(jnp.int32, shape, dim)


PAIR = 2 * ZC
OWN = 16 * PAIR
SIDE = 8 * PAIR
SIDE_MASK = SIDE + 4 * ZC
SIDE_ROWS = SIDE_MASK + ZC
PLANE = 9 * PAIR
HALF = 5 * PAIR
MASKS = 3 * ZC
MIDDLE = 10 * PAIR
FLANKS = 13 * PAIR


def one_where(truth):
    return truth.astype(F32).astype(BF16)


def unpick(rows, cols):
    row = iota((rows, cols), 0)
    return one_where(jnp.where(row < ZC, 2 * row, 2 * row - (Z - 1)) == iota((rows, cols), 1))


def low_b(rows):
    return (iota((rows, LANES), 1) & 32) == 0


def stacked(*parts):
    return jnp.concatenate(parts, axis=0)


def beside(*parts):
    return jnp.concatenate(parts, axis=1)


def pack_kernel(x_hbm, m_hbm, own_ref, up_ref, dn_ref, x_ref, m_ref, sems):
    copies = [pltpu.make_async_copy(m_hbm, m_ref, sems.at[4])]
    for cx in range(4):
        copies.append(pltpu.make_async_copy(x_hbm.at[:, pl.ds(2 * cx, 2)], x_ref.at[:, pl.ds(2 * cx, 2)], sems.at[cx]))
    for copy in copies:
        copy.start()
    sel = unpick(Z, Z)
    src = iota((512, LANES), 0)
    y = src & 7
    goal = ((y >> 1) << 7) + ((src >> 8) << 6) + ((y & 1) << 5) + ((src >> 3) & 31) - iota((512, LANES), 1)
    perm = [one_where(goal == LANES * i) for i in range(4)]
    copies[0].wait()
    mask = (m_ref[...] > 0).astype(F32).reshape(64, Z).astype(BF16)
    cols = nt(sel, mask)
    cols = beside(cols[:ZC], cols[ZC:]).astype(BF16)
    own_ref[OWN : OWN + ZC] = cols
    up_ref[SIDE_MASK:SIDE_ROWS] = cols
    dn_ref[SIDE_MASK:SIDE_ROWS] = cols
    sides = [[], []]
    for cx in range(4):
        copies[1 + cx].wait()
        for a in BITS:
            x = 2 * cx + a
            tile = x_ref[:, x].astype(F32)
            tile = jnp.where(m_ref[x][None] > 0, tile, 0.0)
            sides[a].append(nt(sel, tile.reshape(8 * CH, Z).astype(BF16)).astype(BF16))
    both = beside(stacked(*sides[0]), stacked(*sides[1]))
    cols = [nn(both, perm[cy]) for cy in range(4)]
    ups, downs = [], []
    for cx in range(4):
        col = [v[Z * cx : Z * cx + Z] for v in cols]
        for cz in BITS:
            z = slice(ZC * cz, ZC * cz + ZC)
            first = stacked(col[0][z], col[1][z]).astype(BF16)
            second = stacked(col[2][z], col[3][z]).astype(BF16)
            own_ref[pl.ds((4 * cx + 2 * cz) * PAIR, PAIR)] = first
            own_ref[pl.ds((4 * cx + 2 * cz + 1) * PAIR, PAIR)] = second
            dn_ref[pl.ds((2 * cx + cz) * PAIR, PAIR)] = first
            up_ref[pl.ds((2 * cx + cz) * PAIR, PAIR)] = second
        ups.append(jnp.where(low_b(ZC), pltpu.roll(col[1][ZC:], LANES - 32, 1), col[1][:ZC]))
        downs.append(jnp.where(low_b(ZC), col[2][:ZC], pltpu.roll(col[2][ZC:], 32, 1)))
        if cx % 2 == 1:
            at = pl.ds(SIDE + (cx // 2) * PAIR, PAIR)
            up_ref[at] = stacked(*ups[-2:]).astype(BF16)
            dn_ref[at] = stacked(*downs[-2:]).astype(BF16)


def part(x, size):
    return pl.ds(pl.multiple_of(x * size, size), size)


def folded(pieces, right):
    lane_a = iota(pieces[0].shape, 1) >> 6
    even, odd = (v.astype(F32) for v in pieces)
    return jnp.where(lane_a == right, even, pltpu.roll(odd, 64, 1)).astype(BF16)


def edge_kernel(odd_ref, own_ref, out_ref):
    right = odd_ref[0]
    for i, x in enumerate((3 * right, 1 + right)):
        out_ref[4 * PAIR * i : 4 * PAIR * (i + 1)] = own_ref[part(x, 4 * PAIR)]
    x = 2 - right
    pieces = [own_ref[pl.ds(pl.multiple_of((4 * x + 2 * cz) * PAIR, PAIR), 2 * PAIR)] for cz in BITS]
    out_ref[8 * PAIR : 10 * PAIR] = folded(pieces, right)
    out_ref[MIDDLE : MIDDLE + ZC] = own_ref[OWN : OWN + ZC]


def mid_kernel(odd_ref, own_ref, low_ref, high_ref, tie_ref, tie2_ref, far_ref, near_ref, ends_ref):
    ends_ref[0] = low_ref[SIDE:SIDE_MASK].astype(F32)
    ends_ref[1] = high_ref[SIDE:SIDE_MASK].astype(F32)

    def layer(x, cz):
        return (
            low_ref[pl.ds(pl.multiple_of(x * 2 * PAIR + cz * PAIR, PAIR), PAIR)],
            own_ref[pl.ds(pl.multiple_of(x * 4 * PAIR + 2 * cz * PAIR, PAIR), 2 * PAIR)],
            high_ref[pl.ds(pl.multiple_of(x * 2 * PAIR + cz * PAIR, PAIR), PAIR)],
        )

    def ends(x):
        at = part(x, ZC)
        return stacked(ends_ref[0, at], ends_ref[1, at]).astype(BF16)

    right = 1 - odd_ref[0]
    for i, x in enumerate((3 * right, 1 + right)):
        at = i * PLANE
        for cz in BITS:
            low, own, high = layer(x, cz)
            near_ref[at : at + PAIR] = low
            near_ref[at + PAIR : at + 3 * PAIR] = own
            near_ref[at + 3 * PAIR : at + 4 * PAIR] = high
            at = at + 4 * PAIR
        near_ref[at : at + PAIR] = ends(x)
    x, at = 2 - right, 2 * PLANE
    low, own, high = zip(*[layer(x, cz) for cz in BITS])
    near_ref[at : at + PAIR] = folded(low, right)
    near_ref[at + PAIR : at + 3 * PAIR] = folded(own, right)
    near_ref[at + 3 * PAIR : at + 4 * PAIR] = folded(high, right)
    near_ref[at + 4 * PAIR : at + HALF] = ends(x)
    masks = [low_ref[SIDE_MASK:SIDE_ROWS], own_ref[OWN : OWN + ZC], high_ref[SIDE_MASK:SIDE_ROWS]]
    near_ref[at + HALF : at + HALF + MASKS] = stacked(*[m.astype(F32) for m in masks]).astype(BF16)
    right = odd_ref[0]
    for i, x in enumerate((3 * right, 1 + right)):
        at = 5 * PAIR * i
        far_ref[at : at + 2 * PAIR] = low_ref[part(x, 2 * PAIR)]
        far_ref[at + 2 * PAIR : at + 4 * PAIR] = high_ref[part(x, 2 * PAIR)]
        far_ref[at + 4 * PAIR : at + 5 * PAIR] = ends(x)
    x, at = 2 - right, 10 * PAIR
    low, own, high = zip(*[layer(x, cz) for cz in BITS])
    far_ref[at : at + PAIR] = folded(low, right)
    far_ref[at + PAIR : at + 2 * PAIR] = folded(high, right)
    far_ref[at + 2 * PAIR : at + 3 * PAIR] = ends(x)
    masks = [low_ref[SIDE_MASK:SIDE_ROWS], high_ref[SIDE_MASK:SIDE_ROWS]]
    far_ref[FLANKS : FLANKS + PAIR] = stacked(*[m.astype(F32) for m in masks]).astype(BF16)


def tap_of(out_bit, in_bit, far):
    if far:
        return 2 * (1 - in_bit) if out_bit != in_bit else None
    return in_bit - out_bit + 1


def placed(w_ref, rows, taps, masks):
    full = None not in taps
    total = None if full else jnp.zeros((CH, LANES), BF16)
    for g, tap in enumerate(taps):
        if tap is not None:
            value = w_ref[rows : rows + CH, LANES * tap : LANES * tap + LANES]
            total = value if total is None else jnp.where(masks[g], value, total)
    return total


def block(w_ref, rows, group, far_x, far_y, a_in, b_in, cz_in, shifted, cz_out):
    if shifted:
        tz = None
        if cz_out == 0 and cz_in == 1:
            tz = 0
        if cz_out == 1 and cz_in == 0:
            tz = 2
    else:
        tz = cz_in - cz_out + 1
    taps = []
    for a_out in BITS:
        for b_out in BITS:
            tx = tap_of(a_out, a_in, far_x)
            ty = tap_of(b_out, b_in, far_y)
            taps.append(None if tx is None or ty is None or tz is None else 9 * tx + 3 * ty + tz)
    return placed(w_ref, rows, taps, group)


KINDS = ((0, 0), (1, 0), (0, 1), (1, 1))


def weights_kernel(
    time_ref, wt_ref, we_ref, wd_ref, wn_ref, wc_ref, og_ref, os_ref, oe_ref, od_ref, on_ref, op_ref, ob_ref, oc_ref,
    re_ref, rd_ref, te_ref, td_ref
):
    lane = iota((16, LANES), 1)
    angles = time_ref[...].astype(F32) * jnp.exp(-math.log(10000.0) * (lane & 63).astype(F32) / 64.0)
    embedded = jnp.where(lane < 64, jnp.sin(angles), jnp.cos(angles)).astype(BF16)
    film = nn(embedded, wt_ref[...])
    og_ref[...] = 1.0 + film[0:1, :LANES]
    os_ref[...] = film[0:1, LANES:]
    for tap in range(27):
        for g in range(4):
            at = LANES * tap + CH * g
            re_ref[at : at + CH] = we_ref[tap]
            rd_ref[at : at + CH] = wd_ref[tap]
    one = (iota((CH, CH), 0) == iota((CH, CH), 1)).astype(F32).astype(BF16)
    te_ref[...] = nt(one, re_ref[...]).astype(BF16)
    one = (iota((2 * CH, 2 * CH), 0) == iota((2 * CH, 2 * CH), 1)).astype(F32).astype(BF16)
    td_ref[...] = nt(one, rd_ref[...]).astype(BF16)
    one = one_where(iota((LANES, LANES), 0) == iota((LANES, LANES), 1))
    for i in range(9):
        oc_ref[LANES * i : LANES * i + LANES] = nt(one, wc_ref[3 * i : 3 * i + 3].reshape(384, LANES)).astype(BF16)
    group = [one_where((iota((CH, LANES), 1) >> 5) == g) > 0.5 for g in range(4)]
    for w_ref, o_ref in ((te_ref, oe_ref), (td_ref, od_ref)):
        for t, (fx, fy) in enumerate(KINDS):
            for cz in BITS:
                for a in BITS:
                    for b in BITS:
                        base = 256 * t + 128 * cz + 64 * a + 32 * b
                        for s in BITS:
                            for co in BITS:
                                v = block(w_ref, 0, group, fx, fy, a, b, cz, s, co)
                                o_ref[base : base + CH, 256 * s + 128 * co : 256 * s + 128 * co + LANES] = v
    for t, (fx, fy) in enumerate(KINDS):
        for a in BITS:
            for b in BITS:
                base = 1024 + 128 * t + 64 * a + 32 * b
                for s in BITS:
                    for co in BITS:
                        v = block(td_ref, CH, group, fx, fy, a, b, 0, s, co).astype(F32)
                        v = v + block(td_ref, CH, group, fx, fy, a, b, 1, s, co).astype(F32)
                        od_ref[base : base + CH, 256 * s + 128 * co : 256 * s + 128 * co + LANES] = v.astype(BF16)
    k = iota((8 * CH, LANES), 0)
    goal = (((k >> 5) & 1) << 7) + ((k >> 6) << 5) + (k & 31) - iota((8 * CH, LANES), 1)
    perm = jnp.concatenate([(goal == LANES * i).astype(F32).astype(BF16) for i in BITS], axis=1)
    on_ref[...] = nn(wn_ref[...], perm).astype(BF16)
    src = iota((512, LANES), 0)
    goal = (((src >> 6) & 1) << 8) + ((src & 31) << 3) + ((src >> 7) << 1) + ((src >> 5) & 1) - iota((512, LANES), 1)
    op_ref[...] = beside(*[one_where(goal == LANES * i) for i in range(4)])
    column = iota((Z, LANES), 1)
    goal = jnp.where(column < ZC, 2 * column, jnp.where(column < Z, 2 * column - (Z - 1), -1))
    ob_ref[...] = one_where(goal == iota((Z, LANES), 0))


def moved(t, amount, edge):
    rows = t.shape[0]
    return jnp.where(edge, 0.0, pltpu.roll(t, amount % rows, 0))


def depth_of(rows):
    return iota((rows, LANES), 0) % ZC


def quad(bias):
    return beside(bias, bias, bias, bias)


def put_plane(a_ref, v_ref, layers, ends):
    y0, y9 = ends[:ZC].astype(F32), ends[ZC:].astype(F32)
    for cz in BITS:
        a_ref[cz] = layers[cz].astype(BF16)
        f = layers[cz].astype(F32)
        if cz == 1:
            y0, y9 = pltpu.roll(y0, 32, 1), pltpu.roll(y9, LANES - 32, 1)
        f = stacked(y0, f, y9)
        v_ref[cz] = jnp.where(low_b(320), f[PAIR:], f[:320]).astype(BF16)


def load_own(own_ref, low_ref, high_ref, a_ref, v_ref):
    low_ends = low_ref[SIDE:SIDE_MASK].astype(F32)
    high_ends = high_ref[SIDE:SIDE_MASK].astype(F32)
    for x in range(4):
        layers = []
        for cz in BITS:
            at = (2 * x + cz) * PAIR
            mine = (4 * x + 2 * cz) * PAIR
            layers.append(
                stacked(low_ref[at : at + PAIR], own_ref[mine : mine + 2 * PAIR], high_ref[at : at + PAIR])
            )
        z = slice(ZC * x, ZC * x + ZC)
        put_plane(a_ref.at[x], v_ref.at[x], layers, stacked(low_ends[z], high_ends[z]))


def load_full(ref, at, a_ref, v_ref):
    layers = [ref[at + 320 * cz : at + 320 * cz + 320] for cz in BITS]
    put_plane(a_ref, v_ref, layers, ref[at + 640 : at + PLANE].astype(F32))


def load_half(ref, at, a_ref, v_ref):
    both = ref[at : at + 320].astype(F32)
    put_plane(a_ref, v_ref, [both, pltpu.roll(both, 64, 1)], ref[at + 320 : at + HALF].astype(F32))


def load_far(mid_ref, flank_ref, a, v, k_ref):
    for i in range(2):
        mine, at = 4 * PAIR * i, 5 * PAIR * i
        layers = []
        for cz in BITS:
            low, high = at + PAIR * cz, at + PAIR * (2 + cz)
            own = mine + 2 * PAIR * cz
            layers.append(
                stacked(flank_ref[low : low + PAIR], mid_ref[own : own + 2 * PAIR], flank_ref[high : high + PAIR])
            )
        put_plane(a[i], v[i], layers, flank_ref[at + 4 * PAIR : at + 5 * PAIR].astype(F32))
    at = 10 * PAIR
    both = stacked(
        flank_ref[at : at + PAIR], mid_ref[8 * PAIR : 10 * PAIR], flank_ref[at + PAIR : at + 2 * PAIR]
    ).astype(F32)
    put_plane(a[2], v[2], [both, pltpu.roll(both, 64, 1)], flank_ref[at + 2 * PAIR : at + 3 * PAIR].astype(F32))
    masks = flank_ref[FLANKS : FLANKS + PAIR].astype(F32)
    load_masks([masks[:ZC], mid_ref[MIDDLE : MIDDLE + ZC], masks[ZC:]], k_ref)


def load_masks(parts, k_ref):
    for by, k in enumerate(parts):
        k = k.astype(F32)
        m = jnp.maximum(k, pltpu.roll(k, LANES - 1, 1))
        m = jnp.maximum(m, pltpu.roll(m, LANES - 8, 1))
        m = jnp.maximum(m, pltpu.roll(m, LANES - 64, 1))
        k_ref[0, by, 0:ZC] = k
        k_ref[1, by, 0:ZC] = m


def load_side_masks(ref, at, k_ref):
    masks = ref[at : at + MASKS].astype(F32)
    load_masks([masks[ZC * i : ZC * i + ZC] for i in range(3)], k_ref)


def spread(k, index):
    return stacked(*[jnp.take_along_axis(k[8 * i : 8 * i + 8], index, axis=1, mode="promise_in_bounds") for i in range(5)])


def silu(v):
    half = 0.5 * v
    return half + half * jnp.tanh(half)


def joined_x(planes, p, part, right, rows):
    count = rows.stop - rows.start
    takes_next = one_where((1 - (iota((count, LANES), 1) >> 6)) == right) > 0.5
    return jnp.where(takes_next, planes[p + 1][part, rows], planes[p - 1][part, rows])


def spans(planes, p, parts, right, rows):
    return [planes[p][part, rows] for part in parts] + [joined_x(planes, p, part, right, rows) for part in parts]


def encode_dot(p, right, a, v, we_ref):
    every = slice(0, 320)
    return nn(beside(*spans(a, p, BITS, right, every), *spans(v, p, BITS, right, every)), we_ref[...])


def encode_finish(o, lx, k_ref, e_ref, ev_ref, be, wn_ref):
    z8 = depth_of(320)
    first, last = z8 == 0, z8 == ZC - 1
    lane = iota((8, LANES), 1)
    lane_at = 8 * (lane >> 6) + ((lane >> 5) & 1) + 16 * lx
    pre = (
        o[:, 0:128] + moved(o[:, 256:384], 1, first) + be,
        o[:, 128:256] + moved(o[:, 384:512], -1, last) + be,
    )
    enc = []
    for cz in BITS:
        active = []
        for yi in range(1, 9):
            by, ly = (yi + 1) >> 2, (yi + 1) & 3
            active.append(spread(k_ref[0, by, 0:ZC], lane_at + (64 * cz + 2 * ly)))
        e = jnp.where(stacked(*active) > 0.5, silu(pre[cz]), 0.0)
        enc.append(e.astype(BF16))
        if e_ref is None:
            continue
        e_ref[cz] = enc[cz]
        ev_ref[cz, 0:160] = jnp.where(low_b(160), e[120:280], e[40:200]).astype(BF16)
    return nt(beside(*enc), wn_ref[...])


def strided_finish(lifted, lx, k_ref, c_ref, d_ref, o_ref, gain, shift):
    where = iota((8, LANES), 1) * 0 + 16 * lx
    on = []
    for yi in range(1, 9):
        by, ly = (yi + 1) >> 2, (yi + 1) & 3
        on.append(spread(k_ref[1, by, 0:ZC], where + 2 * ly))
    on = stacked(*on)
    c = jnp.where(on > 0.5, silu(lifted * gain + shift), 0.0)
    c_ref[...] = c.astype(BF16)
    d_ref[0:240] = c[40:280].astype(BF16)
    o_ref[0:240] = on[40:280]


def coarse_dot(q, right, c, d, wc_ref):
    lhs, rhs = [], []
    for i in range(3):
        lhs += [c[q - 1 + i][0:240], d[q - 1 + i][0:240], c[q - 1 + i][80:320]]
        first = 768 * (1 - right) + 384 * i * (2 * right - 1)
        rhs.append(wc_ref[pl.ds(pl.multiple_of(first, 384), 384)])
    return nn(beside(*lhs), stacked(*rhs))


def coarse_finish(p, o_ref, u_ref, bc, wu_ref):
    z6 = depth_of(240)
    first, last = z6 == 0, z6 == ZC - 1
    s = p[:, 128:256] + moved(p[:, 0:128], 1, first) + moved(p[:, 256:384], -1, last) + bc
    act = jnp.where(o_ref[0:240] > 0.5, silu(s), 0.0).astype(BF16)
    u = nt(act, stacked(*([wu_ref[...]] * 4)))
    u_ref[0, 0:160] = u[40:200].astype(BF16)
    u_ref[1, 0:160] = jnp.where(low_b(160), u[80:240], u[0:160]).astype(BF16)


def decode_dot(p, right, e, ev, u, wd_ref):
    mid, every = slice(80, 240), slice(0, 160)
    lhs = spans(e, p, BITS, right, mid) + spans(ev, p, BITS, right, every)
    for v in BITS:
        lhs += spans(u, p, (v,), right, every)
    return nn(beside(*lhs), wd_ref[...])


def decode_finish(o, xo, bd, perm, back, m_ref, out_ref, at, send=None):
    z4 = depth_of(160)
    first, last = z4 == 0, z4 == ZC - 1
    d0 = o[:, 0:128] + moved(o[:, 256:384], 1, first) + bd
    d1 = o[:, 128:256] + moved(o[:, 384:512], -1, last) + bd
    d = [beside(*[v[ZC * y : ZC * y + ZC] for y in range(4)]) for v in (d0, d1)]
    d = stacked(*d, jnp.zeros((LANES - Z, 512), F32)).astype(BF16)
    d = nn(nn(back, d).astype(BF16), perm)
    d = stacked(d, jnp.zeros((LANES - Z, 512), F32))
    for a in BITS:
        t = jnp.transpose(d[:, 256 * a : 256 * a + 256])[:, :Z].reshape(CH, 8, Z)
        out_ref[:, at + a] = jnp.where(m_ref[2 * xo + a][None] > 0, t, 0.0).astype(BF16)
        if send is not None:
            send(at + a, 2 * xo + a)


def own_kernel(
    own_ref, low_ref, high_ref, we_ref, be_ref, wn_ref, gain_ref, shift_ref, a_ref, v_ref, e_ref, ev_ref, c_ref, d_ref,
    o_ref, k_ref
):
    load_own(own_ref, low_ref, high_ref, a_ref, v_ref)
    load_masks((low_ref[SIDE_MASK:SIDE_ROWS], own_ref[OWN : OWN + ZC], high_ref[SIDE_MASK:SIDE_ROWS]), k_ref)
    be = quad(be_ref[...])
    a, v = ([ref.at[x] for x in range(4)] for ref in (a_ref, v_ref))
    dots = [encode_dot(1 + i, 1, a, v, we_ref) for i in range(2)]
    lifted = [encode_finish(dots[i], 1 + i, k_ref, e_ref.at[i], ev_ref.at[i], be, wn_ref) for i in range(2)]
    for i in range(2):
        strided_finish(
            lifted[i], 1 + i, k_ref, c_ref.at[i], d_ref.at[i], o_ref.at[i], gain_ref[...], shift_ref[...]
        )


def own_planes(right, own):
    two = [right * (1 + 2 * i) + 1 - i for i in range(2)]
    one = [right * (2 * i - 1) + 1 - i for i in range(2)]
    a, v = ([ref.at[at] for at in two] for ref in own[0:2])
    e, ev, c, d, o = ([ref.at[at] for at in one] for ref in own[2:7])
    return a, v, e, ev, c, d, o


class Stages:
    def __init__(self, right, weights, misc, planes, side_k, own_k, emit):
        self.right, self.planes, self.emit = right, planes, emit
        self.we, be, self.wn, gain, shift, self.wc, bc, self.wu = weights
        self.m, self.wd, bd, perm, back = misc
        self.be, self.bd = quad(be[...]), quad(bd[...])
        self.gain, self.shift, self.bc = gain[...], shift[...], bc[...]
        self.perm, self.back = perm[...], back[...]
        self.k = (own_k, side_k, side_k)
        self.lx = (3 * right, 3 - 3 * right, 2 - right)

    def e_dot(self, i):
        return encode_dot(1 + i, self.right, self.planes[0], self.planes[1], self.we)

    def e_finish(self, i, dot):
        e, ev = self.planes[2], self.planes[3]
        at = (e[3 + i], ev[3 + i]) if i < 2 else (None, None)
        return encode_finish(dot, self.lx[i], self.k[i], *at, self.be, self.wn)

    def s_finish(self, i, lifted):
        c, d, o = self.planes[4:7]
        strided_finish(lifted, self.lx[i], self.k[i], c[2 + i], d[2 + i], o[2 + i], self.gain, self.shift)

    def c_dot(self, i):
        return coarse_dot(1 + i, self.right, self.planes[4], self.planes[5], self.wc)

    def c_finish(self, i, dot):
        coarse_finish(dot, self.planes[6][1 + i], self.planes[7][2 + i], self.bc, self.wu)

    def d_dot(self, i):
        return decode_dot(1 + i, self.right, self.planes[2], self.planes[3], self.planes[7], self.wd)

    def d_finish(self, i, dot):
        self.emit(i, dot, self.bd, self.perm, self.back, self.m)


def near_kernel(right_ref, side_ref, *refs):
    weights, misc, own = refs[:8], refs[8:13], refs[13:21]
    done_ref, e1_ref, ev1_ref, u1_ref = refs[21:25]
    a_ref, v_ref, e_ref, ev_ref, c_ref, d_ref, o_ref, k_ref, u_ref = refs[25:]
    right = right_ref[0]
    a, v, e, ev, c, d, o = own_planes(right, own)
    a, v, c, d, o = (x + [r.at[i] for i in range(3)] for x, r in zip((a, v, c, d, o), (a_ref, v_ref, c_ref, d_ref, o_ref)))
    e, ev = [None] + e + [e1_ref, e_ref.at[0]], [None] + ev + [ev1_ref, ev_ref.at[0]]
    u = [None, None, u1_ref.at[0], u1_ref.at[1], u_ref.at[0]]
    for i in range(2):
        load_full(side_ref, i * PLANE, a[2 + i], v[2 + i])
    load_half(side_ref, 2 * PLANE, a[4], v[4])
    load_side_masks(side_ref, 2 * PLANE + HALF, k_ref)

    def emit(i, dot, bd, perm, back, m_ref):
        decode_finish(dot, 3 * right, bd, perm, back, m_ref, done_ref, 0)

    w = Stages(right, weights, misc, (a, v, e, ev, c, d, o, u), k_ref, own[7], emit)
    e0 = w.e_dot(0)
    e1 = w.e_dot(1)
    l0 = w.e_finish(0, e0)
    e2 = w.e_dot(2)
    w.s_finish(0, l0)
    l1 = w.e_finish(1, e1)
    c0 = w.c_dot(0)
    w.s_finish(1, l1)
    l2 = w.e_finish(2, e2)
    w.c_finish(0, c0)
    c1 = w.c_dot(1)
    w.s_finish(2, l2)
    w.c_finish(1, c1)
    c2 = w.c_dot(2)
    w.c_finish(2, c2)
    w.d_finish(2, w.d_dot(2))


def far_place(right, i):
    return right * (2 * i - 1) + 2 - i


def far_kernel(right_ref, middle_ref, flanks_ref, *refs):
    weights, misc, own = refs[:8], refs[8:13], refs[13:21]
    near_done_ref, e1_ref, ev1_ref, u1_ref, out_hbm = refs[21:26]
    a_ref, v_ref, e_ref, ev_ref, c_ref, d_ref, o_ref, k_ref, u_ref, out_ref, sems = refs[26:]
    left = right_ref[0]
    right = 1 - left
    copies = [pltpu.make_async_copy(near_done_ref, out_hbm.at[:, pl.ds(6 * left, 2)], sems.at[6])]
    copies[0].start()
    a, v, e, ev, c, d, o = own_planes(right, own)
    a, v, c, d, o = (x + [r.at[i] for i in range(3)] for x, r in zip((a, v, c, d, o), (a_ref, v_ref, c_ref, d_ref, o_ref)))
    e = [e1_ref] + e + [e_ref.at[0], e_ref.at[1]]
    ev = [ev1_ref] + ev + [ev_ref.at[0], ev_ref.at[1]]
    u = [u1_ref.at[1], u1_ref.at[0]] + [u_ref.at[i] for i in range(3)]
    load_far(middle_ref, flanks_ref, a[2:], v[2:], k_ref)

    def send(source, place):
        copies.append(
            pltpu.make_async_copy(out_ref.at[:, pl.ds(source, 1)], out_hbm.at[:, pl.ds(place, 1)], sems.at[source])
        )
        copies[-1].start()

    def emit(i, dot, bd, perm, back, m_ref):
        decode_finish(dot, far_place(right, i), bd, perm, back, m_ref, out_ref, 2 * i, send)

    w = Stages(right, weights, misc, (a, v, e, ev, c, d, o, u), k_ref, own[7], emit)
    e0 = w.e_dot(0)
    e1 = w.e_dot(1)
    l0 = w.e_finish(0, e0)
    e2 = w.e_dot(2)
    w.s_finish(0, l0)
    l1 = w.e_finish(1, e1)
    c0 = w.c_dot(0)
    w.s_finish(1, l1)
    l2 = w.e_finish(2, e2)
    w.c_finish(0, c0)
    c1 = w.c_dot(1)
    w.s_finish(2, l2)
    d0 = w.d_dot(0)
    w.c_finish(1, c1)
    c2 = w.c_dot(2)
    w.d_finish(0, d0)
    d1 = w.d_dot(1)
    w.c_finish(2, c2)
    d2 = w.d_dot(2)
    w.d_finish(1, d1)
    w.d_finish(2, d2)
    for copy in copies:
        copy.wait()


def vmem(n):
    return [pl.BlockSpec(memory_space=pltpu.VMEM)] * n


def hbm(n):
    return [pl.BlockSpec(memory_space=pltpu.HBM)] * n


def call(kernel, outs, ins, out_specs, scratch, mib, flops):
    return pl.pallas_call(
        kernel,
        out_shape=outs,
        in_specs=ins,
        out_specs=out_specs,
        scratch_shapes=scratch,
        compiler_params=pltpu.CompilerParams(vmem_limit_bytes=mib << 20),
        cost_estimate=pl.CostEstimate(flops=flops, bytes_accessed=10**6, transcendentals=0),
    )


def array(*shape, kind=BF16):
    return jax.ShapeDtypeStruct(shape, kind)


def buffers(shapes):
    return [pltpu.VMEM(s, d) for s, d in shapes]


def shifted(value, axis, step):
    peers = lax.axis_size(axis)
    return lax.ppermute(value, axis, [(i, i + step) for i in range(peers) if 0 <= i + step < peers])


def swapped(value, axis, first):
    peers = lax.axis_size(axis)
    pairs = []
    for i in range(first, peers - 1, 2):
        pairs += [(i, i + 1), (i + 1, i)]
    return lax.ppermute(value, axis, pairs)


SCALAR = [pl.BlockSpec(memory_space=pltpu.SMEM)]


def state(own, planes, encoded):
    return [
        (own + (2, 320, LANES), BF16),
        (own + (2, 320, LANES), BF16),
        (encoded + (2, 320, LANES), BF16),
        (encoded + (2, 192, LANES), BF16),
        (planes + (320, LANES), BF16),
        (planes + (256, LANES), BF16),
        (planes + (256, LANES), F32),
        ((2, 3, 64, LANES), F32),
    ]


LIFTED = (2, 192, LANES)


def arrays(shapes):
    return [array(*shape, kind=kind) for shape, kind in shapes]


def on_device(
    fine_in, voxel_mask, timestep, w_enc, b_enc, w_down, w_time, w_coarse, b_coarse, w_up, w_dec, b_dec
):
    own, up, down = call(
        pack_kernel,
        [array(OWN + ZC, LANES), array(SIDE_ROWS, LANES), array(SIDE_ROWS, LANES)],
        hbm(2),
        vmem(3),
        [pltpu.VMEM(fine_in.shape, BF16), pltpu.VMEM(voxel_mask.shape, jnp.int32), pltpu.SemaphoreType.DMA((5,))],
        12,
        10**9,
    )(pltpu.with_memory_space_constraint(fine_in, pltpu.HBM), pltpu.with_memory_space_constraint(voxel_mask, pltpu.HBM))
    low = shifted(up, "wide", 1)
    high = shifted(down, "wide", -1)

    odd = lax.axis_index("narrow").astype(jnp.int32)[None] & 1
    near_right = 1 - odd
    middle = call(edge_kernel, [array(MIDDLE + ZC, LANES)], SCALAR + vmem(1), vmem(1), [], 8, 10**8)(odd, own)[0]
    middle = swapped(middle, "narrow", 1)

    taps = 27 * LANES
    gains, shifts, enc_w, dec_w, down_w, perm, back, coarse_w = call(
        weights_kernel,
        [array(1, LANES, kind=F32), array(1, LANES, kind=F32)]
        + [array(1024, 512), array(1536, 512), array(128, 256), array(512, 512), array(Z, LANES)]
        + [array(9 * LANES, 384)],
        vmem(6),
        vmem(8),
        buffers([((taps, 32), BF16), ((taps, 64), BF16), ((32, taps), BF16), ((64, taps), BF16)]),
        16,
        4 * 10**9,
    )(timestep[None], w_time, w_enc, w_dec, w_down, w_coarse)

    flanks, near = call(
        mid_kernel,
        [array(FLANKS + PAIR, LANES), array(2 * PLANE + HALF + MASKS, LANES)],
        SCALAR + vmem(5),
        vmem(2),
        buffers([((2, 4 * ZC, LANES), F32)]),
        8,
        10**8,
    )(odd, own, low, high, down_w, gains)
    flanks = swapped(flanks, "narrow", 1)
    near = swapped(near, "narrow", 0)

    encoder = (enc_w, b_enc[None], down_w, gains, shifts)
    mine = call(own_kernel, arrays(state((4,), (2,), (2,))), vmem(8), vmem(8), [], 12, 2 * 10**9)(
        own, low, high, *encoder
    )
    some = encoder + (coarse_w, b_coarse[None], w_up, voxel_mask, dec_w, b_dec[None], perm, back) + tuple(mine)
    pair = array(fine_in.shape[0], 2, *fine_in.shape[2:])
    near_done, e1, ev1, u1 = call(
        near_kernel,
        [pair] + arrays(state((), (), ())[2:4] + [((2,) + LIFTED, BF16)]),
        SCALAR + vmem(22),
        vmem(4),
        buffers(state((3,), (3,), (1,)) + [((1,) + LIFTED, BF16)]),
        24,
        4 * 10**9,
    )(near_right, near, *some)
    rest = pltpu.VMEM((fine_in.shape[0], 6) + fine_in.shape[2:], BF16)
    return call(
        far_kernel,
        [array(*fine_in.shape)],
        SCALAR + vmem(27),
        hbm(1),
        buffers(state((3,), (3,), (2,)) + [((3,) + LIFTED, BF16)]) + [rest, pltpu.SemaphoreType.DMA((7,))],
        24,
        5 * 10**9,
    )(near_right, middle, flanks, *some, near_done, e1, ev1, u1)[0]


def solution(mesh):
    field = P(None, "narrow", "wide", None)
    return jax.shard_map(
        on_device,
        mesh=mesh,
        in_specs=(field, P("narrow", "wide", None)) + (P(),) * 10,
        out_specs=field,
        check_vma=False,
    )
```

```python
import math

import jax
import jax.numpy as jnp
from jax import lax
from jax.experimental import pallas as pl
from jax.experimental.pallas import tpu as pltpu
from jax.sharding import PartitionSpec as P


F32 = jnp.float32
BF16 = jnp.bfloat16
LANES = 128
ZC = 40
Z = 80
CH = 32
BITS = (0, 1)


def nn(a, b):
    return lax.dot_general(a, b, (((1,), (0,)), ((), ())), preferred_element_type=F32)


def nt(a, b):
    return lax.dot_general(a, b, (((1,), (1,)), ((), ())), preferred_element_type=F32)


def iota(shape, dim):
    return lax.broadcasted_iota(jnp.int32, shape, dim)


PAIR = 2 * ZC
OWN = 16 * PAIR
SIDE = 8 * PAIR
SIDE_MASK = SIDE + 4 * ZC
SIDE_ROWS = SIDE_MASK + ZC
PLANE = 9 * PAIR
HALF = 5 * PAIR
MASKS = 3 * ZC
MIDDLE = 10 * PAIR
FLANKS = 13 * PAIR


def one_where(truth):
    return truth.astype(F32).astype(BF16)


def unpick(rows, cols):
    row = iota((rows, cols), 0)
    return one_where(jnp.where(row < ZC, 2 * row, 2 * row - (Z - 1)) == iota((rows, cols), 1))


def low_b(rows):
    return (iota((rows, LANES), 1) & 32) == 0


def stacked(*parts):
    return jnp.concatenate(parts, axis=0)


def beside(*parts):
    return jnp.concatenate(parts, axis=1)


def pack_kernel(x_hbm, m_hbm, own_ref, up_ref, dn_ref, x_ref, m_ref, sems):
    copies = [pltpu.make_async_copy(m_hbm, m_ref, sems.at[4])]
    for cx in range(4):
        copies.append(pltpu.make_async_copy(x_hbm.at[:, pl.ds(2 * cx, 2)], x_ref.at[:, pl.ds(2 * cx, 2)], sems.at[cx]))
    for copy in copies:
        copy.start()
    sel = unpick(Z, Z)
    src = iota((512, LANES), 0)
    y = src & 7
    goal = ((y >> 1) << 7) + ((src >> 8) << 6) + ((y & 1) << 5) + ((src >> 3) & 31) - iota((512, LANES), 1)
    perm = [one_where(goal == LANES * i) for i in range(4)]
    copies[0].wait()
    mask = (m_ref[...] > 0).astype(F32).reshape(64, Z).astype(BF16)
    cols = nt(sel, mask)
    cols = beside(cols[:ZC], cols[ZC:]).astype(BF16)
    own_ref[OWN : OWN + ZC] = cols
    up_ref[SIDE_MASK:SIDE_ROWS] = cols
    dn_ref[SIDE_MASK:SIDE_ROWS] = cols
    cols = [[] for _ in range(4)]
    for pair in range(2):
        sides = [[], []]
        for cx in (2 * pair, 2 * pair + 1):
            copies[1 + cx].wait()
            for a in BITS:
                x = 2 * cx + a
                tile = x_ref[:, x].astype(F32)
                tile = jnp.where(m_ref[x][None] > 0, tile, 0.0)
                sides[a].append(nt(sel, tile.reshape(8 * CH, Z).astype(BF16)).astype(BF16))
        both = beside(stacked(*sides[0]), stacked(*sides[1]))
        for cy in range(4):
            v = nn(both, perm[cy])
            cols[cy] += [v[:Z], v[Z:]]
    ups, downs = [], []
    for cx in range(4):
        col = [v[cx] for v in cols]
        for cz in BITS:
            z = slice(ZC * cz, ZC * cz + ZC)
            first = stacked(col[0][z], col[1][z]).astype(BF16)
            second = stacked(col[2][z], col[3][z]).astype(BF16)
            own_ref[pl.ds((4 * cx + 2 * cz) * PAIR, PAIR)] = first
            own_ref[pl.ds((4 * cx + 2 * cz + 1) * PAIR, PAIR)] = second
            dn_ref[pl.ds((2 * cx + cz) * PAIR, PAIR)] = first
            up_ref[pl.ds((2 * cx + cz) * PAIR, PAIR)] = second
        ups.append(jnp.where(low_b(ZC), pltpu.roll(col[1][ZC:], LANES - 32, 1), col[1][:ZC]))
        downs.append(jnp.where(low_b(ZC), col[2][:ZC], pltpu.roll(col[2][ZC:], 32, 1)))
        if cx % 2 == 1:
            at = pl.ds(SIDE + (cx // 2) * PAIR, PAIR)
            up_ref[at] = stacked(*ups[-2:]).astype(BF16)
            dn_ref[at] = stacked(*downs[-2:]).astype(BF16)


def part(x, size):
    return pl.ds(pl.multiple_of(x * size, size), size)


def folded(pieces, right):
    lane_a = iota(pieces[0].shape, 1) >> 6
    even, odd = (v.astype(F32) for v in pieces)
    return jnp.where(lane_a == right, even, pltpu.roll(odd, 64, 1)).astype(BF16)


def edge_kernel(odd_ref, own_ref, out_ref):
    right = odd_ref[0]
    for i, x in enumerate((3 * right, 1 + right)):
        out_ref[4 * PAIR * i : 4 * PAIR * (i + 1)] = own_ref[part(x, 4 * PAIR)]
    x = 2 - right
    pieces = [own_ref[pl.ds(pl.multiple_of((4 * x + 2 * cz) * PAIR, PAIR), 2 * PAIR)] for cz in BITS]
    out_ref[8 * PAIR : 10 * PAIR] = folded(pieces, right)
    out_ref[MIDDLE : MIDDLE + ZC] = own_ref[OWN : OWN + ZC]


def mid_kernel(odd_ref, own_ref, low_ref, high_ref, tie_ref, tie2_ref, far_ref, near_ref, ends_ref):
    ends_ref[0] = low_ref[SIDE:SIDE_MASK].astype(F32)
    ends_ref[1] = high_ref[SIDE:SIDE_MASK].astype(F32)

    def layer(x, cz):
        return (
            low_ref[pl.ds(pl.multiple_of(x * 2 * PAIR + cz * PAIR, PAIR), PAIR)],
            own_ref[pl.ds(pl.multiple_of(x * 4 * PAIR + 2 * cz * PAIR, PAIR), 2 * PAIR)],
            high_ref[pl.ds(pl.multiple_of(x * 2 * PAIR + cz * PAIR, PAIR), PAIR)],
        )

    def ends(x):
        at = part(x, ZC)
        return stacked(ends_ref[0, at], ends_ref[1, at]).astype(BF16)

    right = 1 - odd_ref[0]
    for i, x in enumerate((3 * right, 1 + right)):
        at = i * PLANE
        for cz in BITS:
            low, own, high = layer(x, cz)
            near_ref[at : at + PAIR] = low
            near_ref[at + PAIR : at + 3 * PAIR] = own
            near_ref[at + 3 * PAIR : at + 4 * PAIR] = high
            at = at + 4 * PAIR
        near_ref[at : at + PAIR] = ends(x)
    x, at = 2 - right, 2 * PLANE
    low, own, high = zip(*[layer(x, cz) for cz in BITS])
    near_ref[at : at + PAIR] = folded(low, right)
    near_ref[at + PAIR : at + 3 * PAIR] = folded(own, right)
    near_ref[at + 3 * PAIR : at + 4 * PAIR] = folded(high, right)
    near_ref[at + 4 * PAIR : at + HALF] = ends(x)
    masks = [low_ref[SIDE_MASK:SIDE_ROWS], own_ref[OWN : OWN + ZC], high_ref[SIDE_MASK:SIDE_ROWS]]
    near_ref[at + HALF : at + HALF + MASKS] = stacked(*[m.astype(F32) for m in masks]).astype(BF16)
    right = odd_ref[0]
    for i, x in enumerate((3 * right, 1 + right)):
        at = 5 * PAIR * i
        far_ref[at : at + 2 * PAIR] = low_ref[part(x, 2 * PAIR)]
        far_ref[at + 2 * PAIR : at + 4 * PAIR] = high_ref[part(x, 2 * PAIR)]
        far_ref[at + 4 * PAIR : at + 5 * PAIR] = ends(x)
    x, at = 2 - right, 10 * PAIR
    low, own, high = zip(*[layer(x, cz) for cz in BITS])
    far_ref[at : at + PAIR] = folded(low, right)
    far_ref[at + PAIR : at + 2 * PAIR] = folded(high, right)
    far_ref[at + 2 * PAIR : at + 3 * PAIR] = ends(x)
    masks = [low_ref[SIDE_MASK:SIDE_ROWS], high_ref[SIDE_MASK:SIDE_ROWS]]
    far_ref[FLANKS : FLANKS + PAIR] = stacked(*[m.astype(F32) for m in masks]).astype(BF16)


def tap_of(out_bit, in_bit, far):
    if far:
        return 2 * (1 - in_bit) if out_bit != in_bit else None
    return in_bit - out_bit + 1


def placed(w_ref, rows, taps, masks):
    full = None not in taps
    total = None if full else jnp.zeros((CH, LANES), BF16)
    for g, tap in enumerate(taps):
        if tap is not None:
            value = w_ref[rows : rows + CH, LANES * tap : LANES * tap + LANES]
            total = value if total is None else jnp.where(masks[g], value, total)
    return total


def block(w_ref, rows, group, far_x, far_y, a_in, b_in, cz_in, shifted, cz_out):
    if shifted:
        tz = None
        if cz_out == 0 and cz_in == 1:
            tz = 0
        if cz_out == 1 and cz_in == 0:
            tz = 2
    else:
        tz = cz_in - cz_out + 1
    taps = []
    for a_out in BITS:
        for b_out in BITS:
            tx = tap_of(a_out, a_in, far_x)
            ty = tap_of(b_out, b_in, far_y)
            taps.append(None if tx is None or ty is None or tz is None else 9 * tx + 3 * ty + tz)
    return placed(w_ref, rows, taps, group)


KINDS = ((0, 0), (1, 0), (0, 1), (1, 1))


def weights_kernel(
    time_ref, wt_ref, we_ref, wd_ref, wn_ref, wc_ref, og_ref, os_ref, oe_ref, od_ref, on_ref, op_ref, ob_ref, oc_ref,
    re_ref, rd_ref, te_ref, td_ref
):
    lane = iota((16, LANES), 1)
    angles = time_ref[...].astype(F32) * jnp.exp(-math.log(10000.0) * (lane & 63).astype(F32) / 64.0)
    embedded = jnp.where(lane < 64, jnp.sin(angles), jnp.cos(angles)).astype(BF16)
    film = nn(embedded, wt_ref[...])
    og_ref[...] = 1.0 + film[0:1, :LANES]
    os_ref[...] = film[0:1, LANES:]
    for tap in range(27):
        for g in range(4):
            at = LANES * tap + CH * g
            re_ref[at : at + CH] = we_ref[tap]
            rd_ref[at : at + CH] = wd_ref[tap]
    one = (iota((CH, CH), 0) == iota((CH, CH), 1)).astype(F32).astype(BF16)
    te_ref[...] = nt(one, re_ref[...]).astype(BF16)
    one = (iota((2 * CH, 2 * CH), 0) == iota((2 * CH, 2 * CH), 1)).astype(F32).astype(BF16)
    td_ref[...] = nt(one, rd_ref[...]).astype(BF16)
    one = one_where(iota((LANES, LANES), 0) == iota((LANES, LANES), 1))
    for i in range(9):
        oc_ref[LANES * i : LANES * i + LANES] = nt(one, wc_ref[3 * i : 3 * i + 3].reshape(384, LANES)).astype(BF16)
    group = [one_where((iota((CH, LANES), 1) >> 5) == g) > 0.5 for g in range(4)]
    for w_ref, o_ref in ((te_ref, oe_ref), (td_ref, od_ref)):
        for t, (fx, fy) in enumerate(KINDS):
            for cz in BITS:
                for a in BITS:
                    for b in BITS:
                        base = 256 * t + 128 * cz + 64 * a + 32 * b
                        for s in BITS:
                            for co in BITS:
                                v = block(w_ref, 0, group, fx, fy, a, b, cz, s, co)
                                o_ref[base : base + CH, 256 * s + 128 * co : 256 * s + 128 * co + LANES] = v
    for t, (fx, fy) in enumerate(KINDS):
        for a in BITS:
            for b in BITS:
                base = 1024 + 128 * t + 64 * a + 32 * b
                for s in BITS:
                    for co in BITS:
                        v = block(td_ref, CH, group, fx, fy, a, b, 0, s, co).astype(F32)
                        v = v + block(td_ref, CH, group, fx, fy, a, b, 1, s, co).astype(F32)
                        od_ref[base : base + CH, 256 * s + 128 * co : 256 * s + 128 * co + LANES] = v.astype(BF16)
    k = iota((8 * CH, LANES), 0)
    goal = (((k >> 5) & 1) << 7) + ((k >> 6) << 5) + (k & 31) - iota((8 * CH, LANES), 1)
    perm = jnp.concatenate([(goal == LANES * i).astype(F32).astype(BF16) for i in BITS], axis=1)
    on_ref[...] = nn(wn_ref[...], perm).astype(BF16)
    src = iota((512, LANES), 0)
    goal = (((src >> 6) & 1) << 8) + ((src & 31) << 3) + ((src >> 7) << 1) + ((src >> 5) & 1) - iota((512, LANES), 1)
    op_ref[...] = beside(*[one_where(goal == LANES * i) for i in range(4)])
    column = iota((Z, LANES), 1)
    goal = jnp.where(column < ZC, 2 * column, jnp.where(column < Z, 2 * column - (Z - 1), -1))
    ob_ref[...] = one_where(goal == iota((Z, LANES), 0))


def moved(t, amount, edge):
    rows = t.shape[0]
    return jnp.where(edge, 0.0, pltpu.roll(t, amount % rows, 0))


def depth_of(rows):
    return iota((rows, LANES), 0) % ZC


def quad(bias):
    return beside(bias, bias, bias, bias)


def put_plane(a_ref, v_ref, layers, ends):
    y0, y9 = ends[:ZC].astype(F32), ends[ZC:].astype(F32)
    for cz in BITS:
        a_ref[cz] = layers[cz].astype(BF16)
        f = layers[cz].astype(F32)
        if cz == 1:
            y0, y9 = pltpu.roll(y0, 32, 1), pltpu.roll(y9, LANES - 32, 1)
        f = stacked(y0, f, y9)
        v_ref[cz] = jnp.where(low_b(320), f[PAIR:], f[:320]).astype(BF16)


def load_own(own_ref, low_ref, high_ref, a_ref, v_ref):
    low_ends = low_ref[SIDE:SIDE_MASK].astype(F32)
    high_ends = high_ref[SIDE:SIDE_MASK].astype(F32)
    for x in range(4):
        layers = []
        for cz in BITS:
            at = (2 * x + cz) * PAIR
            mine = (4 * x + 2 * cz) * PAIR
            layers.append(
                stacked(low_ref[at : at + PAIR], own_ref[mine : mine + 2 * PAIR], high_ref[at : at + PAIR])
            )
        z = slice(ZC * x, ZC * x + ZC)
        put_plane(a_ref.at[x], v_ref.at[x], layers, stacked(low_ends[z], high_ends[z]))


def load_full(ref, at, a_ref, v_ref):
    layers = [ref[at + 320 * cz : at + 320 * cz + 320] for cz in BITS]
    put_plane(a_ref, v_ref, layers, ref[at + 640 : at + PLANE].astype(F32))


def load_half(ref, at, a_ref, v_ref):
    both = ref[at : at + 320].astype(F32)
    put_plane(a_ref, v_ref, [both, pltpu.roll(both, 64, 1)], ref[at + 320 : at + HALF].astype(F32))


def load_far(mid_ref, flank_ref, a, v, k_ref):
    for i in range(2):
        mine, at = 4 * PAIR * i, 5 * PAIR * i
        layers = []
        for cz in BITS:
            low, high = at + PAIR * cz, at + PAIR * (2 + cz)
            own = mine + 2 * PAIR * cz
            layers.append(
                stacked(flank_ref[low : low + PAIR], mid_ref[own : own + 2 * PAIR], flank_ref[high : high + PAIR])
            )
        put_plane(a[i], v[i], layers, flank_ref[at + 4 * PAIR : at + 5 * PAIR].astype(F32))
    at = 10 * PAIR
    both = stacked(
        flank_ref[at : at + PAIR], mid_ref[8 * PAIR : 10 * PAIR], flank_ref[at + PAIR : at + 2 * PAIR]
    ).astype(F32)
    put_plane(a[2], v[2], [both, pltpu.roll(both, 64, 1)], flank_ref[at + 2 * PAIR : at + 3 * PAIR].astype(F32))
    masks = flank_ref[FLANKS : FLANKS + PAIR].astype(F32)
    load_masks([masks[:ZC], mid_ref[MIDDLE : MIDDLE + ZC], masks[ZC:]], k_ref)


def load_masks(parts, k_ref):
    for by, k in enumerate(parts):
        k = k.astype(F32)
        m = jnp.maximum(k, pltpu.roll(k, LANES - 1, 1))
        m = jnp.maximum(m, pltpu.roll(m, LANES - 8, 1))
        m = jnp.maximum(m, pltpu.roll(m, LANES - 64, 1))
        k_ref[0, by, 0:ZC] = k
        k_ref[1, by, 0:ZC] = m


def load_side_masks(ref, at, k_ref):
    masks = ref[at : at + MASKS].astype(F32)
    load_masks([masks[ZC * i : ZC * i + ZC] for i in range(3)], k_ref)


def spread(k, index):
    return stacked(*[jnp.take_along_axis(k[8 * i : 8 * i + 8], index, axis=1, mode="promise_in_bounds") for i in range(5)])


def silu(v):
    half = 0.5 * v
    return half + half * jnp.tanh(half)


def joined_x(planes, p, part, right, rows):
    count = rows.stop - rows.start
    takes_next = one_where((1 - (iota((count, LANES), 1) >> 6)) == right) > 0.5
    return jnp.where(takes_next, planes[p + 1][part, rows], planes[p - 1][part, rows])


def spans(planes, p, parts, right, rows):
    return [planes[p][part, rows] for part in parts] + [joined_x(planes, p, part, right, rows) for part in parts]


def encode_dot(p, right, a, v, we_ref):
    every = slice(0, 320)
    return nn(beside(*spans(a, p, BITS, right, every), *spans(v, p, BITS, right, every)), we_ref[...])


def encode_finish(o, lx, k_ref, e_ref, ev_ref, be, wn_ref):
    z8 = depth_of(320)
    first, last = z8 == 0, z8 == ZC - 1
    lane = iota((8, LANES), 1)
    lane_at = 8 * (lane >> 6) + ((lane >> 5) & 1) + 16 * lx
    pre = (
        o[:, 0:128] + moved(o[:, 256:384], 1, first) + be,
        o[:, 128:256] + moved(o[:, 384:512], -1, last) + be,
    )
    enc = []
    for cz in BITS:
        active = []
        for yi in range(1, 9):
            by, ly = (yi + 1) >> 2, (yi + 1) & 3
            active.append(spread(k_ref[0, by, 0:ZC], lane_at + (64 * cz + 2 * ly)))
        e = jnp.where(stacked(*active) > 0.5, silu(pre[cz]), 0.0)
        enc.append(e.astype(BF16))
        if e_ref is None:
            continue
        e_ref[cz] = enc[cz]
        ev_ref[cz, 0:160] = jnp.where(low_b(160), e[120:280], e[40:200]).astype(BF16)
    return nt(beside(*enc), wn_ref[...])


def strided_finish(lifted, lx, k_ref, c_ref, d_ref, o_ref, gain, shift):
    where = iota((8, LANES), 1) * 0 + 16 * lx
    on = []
    for yi in range(1, 9):
        by, ly = (yi + 1) >> 2, (yi + 1) & 3
        on.append(spread(k_ref[1, by, 0:ZC], where + 2 * ly))
    on = stacked(*on)
    c = jnp.where(on > 0.5, silu(lifted * gain + shift), 0.0)
    c_ref[...] = c.astype(BF16)
    d_ref[0:240] = c[40:280].astype(BF16)
    o_ref[0:240] = on[40:280]


def coarse_dot(q, right, c, d, wc_ref):
    lhs, rhs = [], []
    for i in range(3):
        lhs += [c[q - 1 + i][0:240], d[q - 1 + i][0:240], c[q - 1 + i][80:320]]
        first = 768 * (1 - right) + 384 * i * (2 * right - 1)
        rhs.append(wc_ref[pl.ds(pl.multiple_of(first, 384), 384)])
    return nn(beside(*lhs), stacked(*rhs))


def coarse_finish(p, o_ref, u_ref, bc, wu_ref):
    z6 = depth_of(240)
    first, last = z6 == 0, z6 == ZC - 1
    s = p[:, 128:256] + moved(p[:, 0:128], 1, first) + moved(p[:, 256:384], -1, last) + bc
    act = jnp.where(o_ref[0:240] > 0.5, silu(s), 0.0).astype(BF16)
    u = nt(act, stacked(*([wu_ref[...]] * 4)))
    u_ref[0, 0:160] = u[40:200].astype(BF16)
    u_ref[1, 0:160] = jnp.where(low_b(160), u[80:240], u[0:160]).astype(BF16)


def decode_dot(p, right, e, ev, u, wd_ref):
    mid, every = slice(80, 240), slice(0, 160)
    lhs = spans(e, p, BITS, right, mid) + spans(ev, p, BITS, right, every)
    for v in BITS:
        lhs += spans(u, p, (v,), right, every)
    return nn(beside(*lhs), wd_ref[...])


def decode_finish(o, xo, bd, perm, back, m_ref, out_ref, at, send=None):
    z4 = depth_of(160)
    first, last = z4 == 0, z4 == ZC - 1
    d0 = o[:, 0:128] + moved(o[:, 256:384], 1, first) + bd
    d1 = o[:, 128:256] + moved(o[:, 384:512], -1, last) + bd
    d = [beside(*[v[ZC * y : ZC * y + ZC] for y in range(4)]) for v in (d0, d1)]
    d = stacked(*d, jnp.zeros((LANES - Z, 512), F32)).astype(BF16)
    d = nn(nn(back, d).astype(BF16), perm)
    d = stacked(d, jnp.zeros((LANES - Z, 512), F32))
    for a in BITS:
        t = jnp.transpose(d[:, 256 * a : 256 * a + 256])[:, :Z].reshape(CH, 8, Z)
        out_ref[:, at + a] = jnp.where(m_ref[2 * xo + a][None] > 0, t, 0.0).astype(BF16)
        if send is not None:
            send(at + a, 2 * xo + a)


def own_kernel(
    own_ref, low_ref, high_ref, we_ref, be_ref, wn_ref, gain_ref, shift_ref, a_ref, v_ref, e_ref, ev_ref, c_ref, d_ref,
    o_ref, k_ref
):
    load_own(own_ref, low_ref, high_ref, a_ref, v_ref)
    load_masks((low_ref[SIDE_MASK:SIDE_ROWS], own_ref[OWN : OWN + ZC], high_ref[SIDE_MASK:SIDE_ROWS]), k_ref)
    be = quad(be_ref[...])
    a, v = ([ref.at[x] for x in range(4)] for ref in (a_ref, v_ref))
    dots = [encode_dot(1 + i, 1, a, v, we_ref) for i in range(2)]
    lifted = [encode_finish(dots[i], 1 + i, k_ref, e_ref.at[i], ev_ref.at[i], be, wn_ref) for i in range(2)]
    for i in range(2):
        strided_finish(
            lifted[i], 1 + i, k_ref, c_ref.at[i], d_ref.at[i], o_ref.at[i], gain_ref[...], shift_ref[...]
        )


def own_planes(right, own):
    two = [right * (1 + 2 * i) + 1 - i for i in range(2)]
    one = [right * (2 * i - 1) + 1 - i for i in range(2)]
    a, v = ([ref.at[at] for at in two] for ref in own[0:2])
    e, ev, c, d, o = ([ref.at[at] for at in one] for ref in own[2:7])
    return a, v, e, ev, c, d, o


class Stages:
    def __init__(self, right, weights, misc, planes, side_k, own_k, emit):
        self.right, self.planes, self.emit = right, planes, emit
        self.we, be, self.wn, gain, shift, self.wc, bc, self.wu = weights
        self.m, self.wd, bd, perm, back = misc
        self.be, self.bd = quad(be[...]), quad(bd[...])
        self.gain, self.shift, self.bc = gain[...], shift[...], bc[...]
        self.perm, self.back = perm[...], back[...]
        self.k = (own_k, side_k, side_k)
        self.lx = (3 * right, 3 - 3 * right, 2 - right)

    def e_dot(self, i):
        return encode_dot(1 + i, self.right, self.planes[0], self.planes[1], self.we)

    def e_finish(self, i, dot):
        e, ev = self.planes[2], self.planes[3]
        at = (e[3 + i], ev[3 + i]) if i < 2 else (None, None)
        return encode_finish(dot, self.lx[i], self.k[i], *at, self.be, self.wn)

    def s_finish(self, i, lifted):
        c, d, o = self.planes[4:7]
        strided_finish(lifted, self.lx[i], self.k[i], c[2 + i], d[2 + i], o[2 + i], self.gain, self.shift)

    def c_dot(self, i):
        return coarse_dot(1 + i, self.right, self.planes[4], self.planes[5], self.wc)

    def c_finish(self, i, dot):
        coarse_finish(dot, self.planes[6][1 + i], self.planes[7][2 + i], self.bc, self.wu)

    def d_dot(self, i):
        return decode_dot(1 + i, self.right, self.planes[2], self.planes[3], self.planes[7], self.wd)

    def d_finish(self, i, dot):
        self.emit(i, dot, self.bd, self.perm, self.back, self.m)


def near_kernel(right_ref, side_ref, *refs):
    weights, misc, own = refs[:8], refs[8:13], refs[13:21]
    done_ref, e1_ref, ev1_ref, u1_ref = refs[21:25]
    a_ref, v_ref, e_ref, ev_ref, c_ref, d_ref, o_ref, k_ref, u_ref = refs[25:]
    right = right_ref[0]
    a, v, e, ev, c, d, o = own_planes(right, own)
    a, v, c, d, o = (x + [r.at[i] for i in range(3)] for x, r in zip((a, v, c, d, o), (a_ref, v_ref, c_ref, d_ref, o_ref)))
    e, ev = [None] + e + [e1_ref, e_ref.at[0]], [None] + ev + [ev1_ref, ev_ref.at[0]]
    u = [None, None, u1_ref.at[0], u1_ref.at[1], u_ref.at[0]]
    for i in range(2):
        load_full(side_ref, i * PLANE, a[2 + i], v[2 + i])
    load_half(side_ref, 2 * PLANE, a[4], v[4])
    load_side_masks(side_ref, 2 * PLANE + HALF, k_ref)

    def emit(i, dot, bd, perm, back, m_ref):
        decode_finish(dot, 3 * right, bd, perm, back, m_ref, done_ref, 0)

    w = Stages(right, weights, misc, (a, v, e, ev, c, d, o, u), k_ref, own[7], emit)
    e0 = w.e_dot(0)
    e1 = w.e_dot(1)
    l0 = w.e_finish(0, e0)
    e2 = w.e_dot(2)
    w.s_finish(0, l0)
    l1 = w.e_finish(1, e1)
    c0 = w.c_dot(0)
    w.s_finish(1, l1)
    l2 = w.e_finish(2, e2)
    w.c_finish(0, c0)
    c1 = w.c_dot(1)
    w.s_finish(2, l2)
    w.c_finish(1, c1)
    c2 = w.c_dot(2)
    w.c_finish(2, c2)
    w.d_finish(2, w.d_dot(2))


def far_place(right, i):
    return right * (2 * i - 1) + 2 - i


def far_kernel(right_ref, middle_ref, flanks_ref, *refs):
    weights, misc, own = refs[:8], refs[8:13], refs[13:21]
    near_done_ref, e1_ref, ev1_ref, u1_ref, out_hbm = refs[21:26]
    a_ref, v_ref, e_ref, ev_ref, c_ref, d_ref, o_ref, k_ref, u_ref, out_ref, sems = refs[26:]
    left = right_ref[0]
    right = 1 - left
    copies = [pltpu.make_async_copy(near_done_ref, out_hbm.at[:, pl.ds(6 * left, 2)], sems.at[6])]
    copies[0].start()
    a, v, e, ev, c, d, o = own_planes(right, own)
    a, v, c, d, o = (x + [r.at[i] for i in range(3)] for x, r in zip((a, v, c, d, o), (a_ref, v_ref, c_ref, d_ref, o_ref)))
    e = [e1_ref] + e + [e_ref.at[0], e_ref.at[1]]
    ev = [ev1_ref] + ev + [ev_ref.at[0], ev_ref.at[1]]
    u = [u1_ref.at[1], u1_ref.at[0]] + [u_ref.at[i] for i in range(3)]
    load_far(middle_ref, flanks_ref, a[2:], v[2:], k_ref)

    def send(source, place):
        copies.append(
            pltpu.make_async_copy(out_ref.at[:, pl.ds(source, 1)], out_hbm.at[:, pl.ds(place, 1)], sems.at[source])
        )
        copies[-1].start()

    def emit(i, dot, bd, perm, back, m_ref):
        decode_finish(dot, far_place(right, i), bd, perm, back, m_ref, out_ref, 2 * i, send)

    w = Stages(right, weights, misc, (a, v, e, ev, c, d, o, u), k_ref, own[7], emit)
    e0 = w.e_dot(0)
    e1 = w.e_dot(1)
    l0 = w.e_finish(0, e0)
    e2 = w.e_dot(2)
    w.s_finish(0, l0)
    l1 = w.e_finish(1, e1)
    c0 = w.c_dot(0)
    w.s_finish(1, l1)
    l2 = w.e_finish(2, e2)
    w.c_finish(0, c0)
    c1 = w.c_dot(1)
    w.s_finish(2, l2)
    d0 = w.d_dot(0)
    w.c_finish(1, c1)
    c2 = w.c_dot(2)
    w.d_finish(0, d0)
    d1 = w.d_dot(1)
    w.c_finish(2, c2)
    d2 = w.d_dot(2)
    w.d_finish(1, d1)
    w.d_finish(2, d2)
    for copy in copies:
        copy.wait()


def vmem(n):
    return [pl.BlockSpec(memory_space=pltpu.VMEM)] * n


def hbm(n):
    return [pl.BlockSpec(memory_space=pltpu.HBM)] * n


def call(kernel, outs, ins, out_specs, scratch, mib, flops):
    return pl.pallas_call(
        kernel,
        out_shape=outs,
        in_specs=ins,
        out_specs=out_specs,
        scratch_shapes=scratch,
        compiler_params=pltpu.CompilerParams(vmem_limit_bytes=mib << 20),
        cost_estimate=pl.CostEstimate(flops=flops, bytes_accessed=10**6, transcendentals=0),
    )


def array(*shape, kind=BF16):
    return jax.ShapeDtypeStruct(shape, kind)


def buffers(shapes):
    return [pltpu.VMEM(s, d) for s, d in shapes]


def shifted(value, axis, step):
    peers = lax.axis_size(axis)
    return lax.ppermute(value, axis, [(i, i + step) for i in range(peers) if 0 <= i + step < peers])


def swapped(value, axis, first):
    peers = lax.axis_size(axis)
    pairs = []
    for i in range(first, peers - 1, 2):
        pairs += [(i, i + 1), (i + 1, i)]
    return lax.ppermute(value, axis, pairs)


SCALAR = [pl.BlockSpec(memory_space=pltpu.SMEM)]


def state(own, planes, encoded):
    return [
        (own + (2, 320, LANES), BF16),
        (own + (2, 320, LANES), BF16),
        (encoded + (2, 320, LANES), BF16),
        (encoded + (2, 192, LANES), BF16),
        (planes + (320, LANES), BF16),
        (planes + (256, LANES), BF16),
        (planes + (256, LANES), F32),
        ((2, 3, 64, LANES), F32),
    ]


LIFTED = (2, 192, LANES)


def arrays(shapes):
    return [array(*shape, kind=kind) for shape, kind in shapes]


def on_device(
    fine_in, voxel_mask, timestep, w_enc, b_enc, w_down, w_time, w_coarse, b_coarse, w_up, w_dec, b_dec
):
    own, up, down = call(
        pack_kernel,
        [array(OWN + ZC, LANES), array(SIDE_ROWS, LANES), array(SIDE_ROWS, LANES)],
        hbm(2),
        vmem(3),
        [pltpu.VMEM(fine_in.shape, BF16), pltpu.VMEM(voxel_mask.shape, jnp.int32), pltpu.SemaphoreType.DMA((5,))],
        12,
        10**9,
    )(pltpu.with_memory_space_constraint(fine_in, pltpu.HBM), pltpu.with_memory_space_constraint(voxel_mask, pltpu.HBM))
    low = shifted(up, "wide", 1)
    high = shifted(down, "wide", -1)

    odd = lax.axis_index("narrow").astype(jnp.int32)[None] & 1
    near_right = 1 - odd
    middle = call(edge_kernel, [array(MIDDLE + ZC, LANES)], SCALAR + vmem(1), vmem(1), [], 8, 10**8)(odd, own)[0]
    middle = swapped(middle, "narrow", 1)

    taps = 27 * LANES
    gains, shifts, enc_w, dec_w, down_w, perm, back, coarse_w = call(
        weights_kernel,
        [array(1, LANES, kind=F32), array(1, LANES, kind=F32)]
        + [array(1024, 512), array(1536, 512), array(128, 256), array(512, 512), array(Z, LANES)]
        + [array(9 * LANES, 384)],
        vmem(6),
        vmem(8),
        buffers([((taps, 32), BF16), ((taps, 64), BF16), ((32, taps), BF16), ((64, taps), BF16)]),
        16,
        4 * 10**9,
    )(timestep[None], w_time, w_enc, w_dec, w_down, w_coarse)

    flanks, near = call(
        mid_kernel,
        [array(FLANKS + PAIR, LANES), array(2 * PLANE + HALF + MASKS, LANES)],
        SCALAR + vmem(5),
        vmem(2),
        buffers([((2, 4 * ZC, LANES), F32)]),
        8,
        10**8,
    )(odd, own, low, high, down_w, gains)
    flanks = swapped(flanks, "narrow", 1)
    near = swapped(near, "narrow", 0)

    encoder = (enc_w, b_enc[None], down_w, gains, shifts)
    mine = call(own_kernel, arrays(state((4,), (2,), (2,))), vmem(8), vmem(8), [], 12, 2 * 10**9)(
        own, low, high, *encoder
    )
    some = encoder + (coarse_w, b_coarse[None], w_up, voxel_mask, dec_w, b_dec[None], perm, back) + tuple(mine)
    pair = array(fine_in.shape[0], 2, *fine_in.shape[2:])
    near_done, e1, ev1, u1 = call(
        near_kernel,
        [pair] + arrays(state((), (), ())[2:4] + [((2,) + LIFTED, BF16)]),
        SCALAR + vmem(22),
        vmem(4),
        buffers(state((3,), (3,), (1,)) + [((1,) + LIFTED, BF16)]),
        24,
        4 * 10**9,
    )(near_right, near, *some)
    rest = pltpu.VMEM((fine_in.shape[0], 6) + fine_in.shape[2:], BF16)
    return call(
        far_kernel,
        [array(*fine_in.shape)],
        SCALAR + vmem(27),
        hbm(1),
        buffers(state((3,), (3,), (2,)) + [((3,) + LIFTED, BF16)]) + [rest, pltpu.SemaphoreType.DMA((7,))],
        24,
        5 * 10**9,
    )(near_right, middle, flanks, *some, near_done, e1, ev1, u1)[0]


def solution(mesh):
    field = P(None, "narrow", "wide", None)
    return jax.shard_map(
        on_device,
        mesh=mesh,
        in_specs=(field, P("narrow", "wide", None)) + (P(),) * 10,
        out_specs=field,
        check_vma=False,
    )
```
